32 devices in a mesh: dp: 2 (over x), col: 4 (over z), row: 4 (over y, core).
Axes of the slice: x: 2, y: 2, z: 4, core: 2. Of those that a mesh axis runs over, the one named last changes fastest.
Arguments:
- hidden: bfloat16 [128, 3584], P('dp', 'row'), parts along dimension 0
- norm_gain: float32 [3584], P('row')
- w_head: bfloat16 [3584, 152064], P('row', 'col')
Outputs:
- output 1: float32 [128, 152064], P('dp', ('col', 'row')), parts along dimension 0
- output 2: float32 [128], P('dp'), parts along dimension 0
There are 2 independent parts. The reference program is written for one: setup_inputs(seed, part) draws one part's arguments, and reference() takes and returns one part's arrays. A program takes and returns all parts, laid end to end along the dimension named above; an argument that names none is the same for every part.
All inputs are finite; a program needn't handle non-finite values.
Results may differ from the reference program's by a relative error of at most 0.001.
Values sent between devices are 32-bit elements.
A program may use at most 1 GiB of HBM per device.

```python
import jax
import jax.numpy as jnp
from jax import lax

BATCH = 64
HIDDEN = 3584
VOCAB = 152064
EPS = 1e-5


def setup_inputs(seed: int = 0, part: int = 0) -> dict:
    key = jax.random.key(seed)
    part_key = jax.random.fold_in(key, part)
    key_tok, key_feat = jax.random.split(part_key, 2)
    key_gain, key_weight = jax.random.split(key, 2)
    position = jnp.arange(HIDDEN, dtype=jnp.float32) / HIDDEN
    feat_scale = (0.4 + 1.2 * position) * jax.random.uniform(key_feat, (HIDDEN,), jnp.float32, 0.8, 1.2)
    hidden = jax.random.normal(key_tok, (BATCH, HIDDEN), jnp.float32) * feat_scale
    gain = 2.4 / (0.4 + 1.2 * position) * jax.random.uniform(key_gain, (HIDDEN,), jnp.float32, 0.7, 1.3)
    weight = jax.random.normal(key_weight, (HIDDEN, VOCAB), jnp.float32) * HIDDEN ** -0.5
    return {"hidden": hidden.astype(jnp.bfloat16), "norm_gain": gain, "w_head": weight.astype(jnp.bfloat16)}


def reference(hidden, norm_gain, w_head):
    wide_hidden = hidden.astype(jnp.float32)
    mean_sq = jnp.mean(wide_hidden * wide_hidden, axis=-1, keepdims=True)
    normed = (wide_hidden * lax.rsqrt(mean_sq + EPS) * norm_gain).astype(jnp.bfloat16)
    logits = jnp.dot(normed, w_head, preferred_element_type=jnp.float32)
    log_norm = jax.nn.logsumexp(logits, axis=-1)
    return logits - log_norm[:, None], log_norm
```

```python
import jax
import jax.numpy as jnp
from jax import lax
from jax.experimental import pallas as pl
from jax.experimental.pallas import tpu as pltpu
from jax.sharding import PartitionSpec as P

EPS = 1e-5
MESH = pl.DeviceIdType.MESH
LANES = 128
TILES = 3
CHUNK = TILES * LANES
SLOTS = 12


def head_kernel(
    count, width, hidden_size,
    h_ref, g_ref, w_ref, z_ref, lse_ref,
    wa, wb, x_ref, qbuf, rbuf, pbuf, lbuf, rin, lin, yin, nst, fst, m_ref, s_ref, carry,
    wa_sem, wb_sem, nsend, nrecv, qsend, psend, ysend, rrecv, lrecv, yrecv, fsend, frecv,
):
    rows = h_ref.shape[0]
    feats = h_ref.shape[1]
    stride = (width // LANES) * LANES
    rest = width - stride
    col = lax.axis_index("col")
    row = lax.axis_index("row")
    core = lax.rem(row, 2)
    mate = row + 1 - 2 * core
    across = lax.rem(row + 2, 4)
    far = 3 - row
    shift = row * rest

    def fetch(stream, t):
        if stream == 0:
            first, second, buf, sem = far, mate, wa, wa_sem
        else:
            first, second, buf, sem = across, row, wb, wb_sem
        part = first + (second - first) * (t // count)
        start = pl.multiple_of(stride * part + CHUNK * lax.rem(t, count), LANES)
        slot = lax.rem(t, SLOTS)
        return pltpu.make_async_copy(w_ref.at[:, pl.ds(start, CHUNK)], buf.at[slot], sem.at[slot])

    for t in range(SLOTS):
        fetch(0, t).start()
        fetch(1, t).start()

    barrier = pltpu.get_barrier_semaphore()
    for dc in range(4):
        for dr in range(4):
            if dc or dr:
                pl.semaphore_signal(
                    barrier, inc=1, device_id_type=MESH,
                    device_id={"col": lax.rem(col + dc, 4), "row": lax.rem(row + dr, 4)},
                )

    lane = lax.broadcasted_iota(jnp.int32, (rows, LANES), 1)
    sq = jnp.zeros((rows, LANES), jnp.float32)
    for j in range(feats // LANES):
        part = h_ref[:, j * LANES:(j + 1) * LANES].astype(jnp.float32)
        sq = sq + part * part
    sq = jnp.transpose(jnp.concatenate([sq, sq], axis=0))
    nst[row] = jnp.sum(sq, axis=0, keepdims=True)
    pl.semaphore_wait(barrier, 15)

    def norm_copy(k):
        return pltpu.make_async_remote_copy(
            src_ref=nst.at[row], dst_ref=nst.at[row], send_sem=nsend.at[k], recv_sem=nrecv.at[row],
            device_id={"row": lax.rem(row + k, 4)}, device_id_type=MESH,
        )

    for k in range(1, 4):
        norm_copy(k).start()
    for k in range(1, 4):
        peer = lax.rem(row + k, 4)
        pltpu.make_async_remote_copy(
            src_ref=nst.at[peer], dst_ref=nst.at[peer], send_sem=nsend.at[k], recv_sem=nrecv.at[peer],
            device_id={"row": peer}, device_id_type=MESH,
        ).wait_recv()
    total = nst[0] + nst[1] + nst[2] + nst[3]
    scale = lax.rsqrt(total / hidden_size + EPS)
    scale = jnp.transpose(jnp.broadcast_to(scale, (LANES, LANES)))[:rows]
    for j in range(feats // LANES):
        cols = slice(j * LANES, (j + 1) * LANES)
        x_ref[:, cols] = (h_ref[:, cols].astype(jnp.float32) * scale * g_ref[:, cols]).astype(jnp.bfloat16)

    def product(stream, t):
        buf, sem = ((wa, wa_sem), (wb, wb_sem))[stream]
        fetch(stream, t).wait()
        slot = lax.rem(t, SLOTS)
        return jnp.dot(x_ref[...], buf[slot], preferred_element_type=jnp.float32)

    def refill(stream, t):
        @pl.when(t + SLOTS < 2 * count)
        def _():
            fetch(stream, t + SLOTS).start()

    def mate_copy(src, dst, send, recv, i):
        return pltpu.make_async_remote_copy(
            src_ref=src.at[i], dst_ref=dst.at[i], send_sem=send, recv_sem=recv.at[i],
            device_id={"row": mate}, device_id_type=MESH,
        )

    def across_copy(i):
        return pltpu.make_async_remote_copy(
            src_ref=rbuf.at[i], dst_ref=yin.at[i], send_sem=ysend, recv_sem=yrecv.at[i],
            device_id={"row": across}, device_id_type=MESH,
        )

    def far_step(i):
        qbuf[i] = product(0, i)
        mate_copy(qbuf, rin, qsend, rrecv, i).start()
        refill(0, i)

    def across_step(i):
        term = product(1, i)
        refill(1, i)
        mate_copy(qbuf, rin, qsend, rrecv, i).wait_recv()
        rbuf[i] = term + rin[i]
        across_copy(i).start()

    far_step(0)

    @pl.loop(0, count - 1)
    def _(i):
        far_step(i + 1)
        across_step(i)

    across_step(count - 1)

    @pl.loop(0, count)
    def _(i):
        pbuf[i] = product(0, count + i)
        mate_copy(pbuf, lin, psend, lrecv, i).start()
        refill(0, count + i)
        lbuf[i] = product(1, count + i)
        refill(1, count + i)

    turn = lax.rem(LANES - shift, LANES)
    keep = lane < LANES - shift

    def turned(i):
        mate_copy(pbuf, lin, psend, lrecv, i).wait_recv()
        across_copy(i).wait_recv()
        full = lbuf[i] + lin[i] + yin[i]
        return [pltpu.roll(full[:, k * LANES:(k + 1) * LANES], turn, 1) for k in range(TILES)]

    def arrive(i, first):
        rolled = turned(i)
        tiles = [jnp.where(keep, rolled[k], rolled[k + 1]) for k in range(TILES - 1)]
        at = 0
        if not first:
            tiles = [jnp.where(keep, carry[...], rolled[0])] + tiles
            at = pl.multiple_of(i * CHUNK - LANES, LANES)
        carry[...] = rolled[-1]
        z_ref[:, pl.ds(at, LANES * len(tiles))] = jnp.concatenate(tiles, axis=1)
        top = tiles[0]
        for tile in tiles[1:]:
            top = jnp.maximum(top, tile)
        if not first:
            top = jnp.maximum(top, m_ref[...])
        mass = jnp.exp(tiles[0] - top)
        for tile in tiles[1:]:
            mass = mass + jnp.exp(tile - top)
        if not first:
            mass = mass + s_ref[...] * jnp.exp(m_ref[...] - top)
        m_ref[...] = top
        s_ref[...] = mass

    arrive(0, True)

    @pl.loop(1, count)
    def _(i):
        arrive(i, False)

    last = carry[...]
    z_ref[:, stride:] = last[:, :rest]
    last = jnp.where(lane < rest, last, -jnp.inf)
    top = jnp.maximum(m_ref[...], last)
    mass = s_ref[...] * jnp.exp(m_ref[...] - top) + jnp.exp(last - top)
    top = jnp.transpose(jnp.concatenate([top, top], axis=0))
    mass = jnp.transpose(jnp.concatenate([mass, mass], axis=0))
    peak = jnp.max(top, axis=0, keepdims=True)
    mass = jnp.sum(mass * jnp.exp(top - peak), axis=0, keepdims=True)
    me = col * 4 + row
    fst[me] = jnp.where(lane[:1] < rows, peak, mass)

    def stat_copy(dc, dr):
        k = dc * 4 + dr
        return pltpu.make_async_remote_copy(
            src_ref=fst.at[me], dst_ref=fst.at[me], send_sem=fsend.at[k], recv_sem=frecv.at[me],
            device_id={"col": lax.rem(col + dc, 4), "row": lax.rem(row + dr, 4)}, device_id_type=MESH,
        )

    peers = [(dc, dr) for dc in (3, 2, 1, 0) for dr in (2, 3, 1, 0) if dc or dr]
    for dc, dr in peers:
        stat_copy(dc, dr).start()
    for dc, dr in peers:
        pc, pr = lax.rem(col + dc, 4), lax.rem(row + dr, 4)
        peer = pc * 4 + pr
        pltpu.make_async_remote_copy(
            src_ref=fst.at[peer], dst_ref=fst.at[peer], send_sem=fsend.at[dc * 4 + dr], recv_sem=frecv.at[peer],
            device_id={"col": pc, "row": pr}, device_id_type=MESH,
        ).wait_recv()
    stats = fst[...]
    swapped = pltpu.roll(stats, LANES // 2, 2)
    peak = jnp.max(stats, axis=0)
    mass = jnp.sum(swapped * jnp.exp(stats - peak), axis=0)
    lse_ref[...] = peak + jnp.log(mass)

    for k in range(1, 4):
        norm_copy(k).wait_send()
    for src, dst, send, recv in ((qbuf, rin, qsend, rrecv), (pbuf, lin, psend, lrecv)):
        pltpu.make_async_remote_copy(
            src_ref=src, dst_ref=dst, send_sem=send, recv_sem=recv.at[0],
            device_id={"row": mate}, device_id_type=MESH,
        ).wait_send()
    pltpu.make_async_remote_copy(
        src_ref=rbuf, dst_ref=yin, send_sem=ysend, recv_sem=yrecv.at[0],
        device_id={"row": across}, device_id_type=MESH,
    ).wait_send()
    for dc, dr in peers:
        stat_copy(dc, dr).wait_send()


def solution(mesh):
    def local_head(hidden, norm_gain, w_head):
        rows, feats = hidden.shape
        width = w_head.shape[1] // 4
        count = (width // LANES + 1) // TILES
        block = (count, rows, CHUNK)
        dma = pltpu.SemaphoreType.DMA

        def body(*refs):
            head_kernel(count, width, feats * 4, *refs)

        z, lse = pl.pallas_call(
            body,
            out_shape=(
                jax.ShapeDtypeStruct((rows, width), jnp.float32),
                jax.ShapeDtypeStruct((1, LANES), jnp.float32),
            ),
            in_specs=[
                pl.BlockSpec(memory_space=pltpu.VMEM),
                pl.BlockSpec(memory_space=pltpu.VMEM),
                pl.BlockSpec(memory_space=pl.ANY),
            ],
            out_specs=(pl.BlockSpec(memory_space=pltpu.VMEM), pl.BlockSpec(memory_space=pltpu.VMEM)),
            scratch_shapes=[
                pltpu.VMEM((SLOTS, feats, CHUNK), jnp.bfloat16),
                pltpu.VMEM((SLOTS, feats, CHUNK), jnp.bfloat16),
                pltpu.VMEM((rows, feats), jnp.bfloat16),
                *[pltpu.VMEM(block, jnp.float32) for _ in range(7)],
                pltpu.VMEM((4, 1, LANES), jnp.float32),
                pltpu.VMEM((16, 1, LANES), jnp.float32),
                *[pltpu.VMEM((rows, LANES), jnp.float32) for _ in range(3)],
                dma((SLOTS,)), dma((SLOTS,)), dma((4,)), dma((4,)),
                dma, dma, dma, dma((count,)), dma((count,)), dma((count,)), dma((16,)), dma((16,)),
            ],
            compiler_params=pltpu.CompilerParams(
                collective_id=0, has_side_effects=True, vmem_limit_bytes=48 * 1024 * 1024
            ),
            name="head",
        )(hidden, norm_gain.reshape(1, feats), w_head)
        log_norm = lse[0, :rows]
        return z - log_norm[:, None], log_norm

    return jax.shard_map(
        local_head,
        mesh=mesh,
        in_specs=(P("dp", "row"), P("row"), P("row", "col")),
        out_specs=(P("dp", ("col", "row")), P("dp")),
        check_vma=False,
    )
```

```python
import jax
import jax.numpy as jnp
from jax import lax
from jax.experimental import pallas as pl
from jax.experimental.pallas import tpu as pltpu
from jax.sharding import PartitionSpec as P

EPS = 1e-5
MESH = pl.DeviceIdType.MESH
LANES = 128
TILES = 3
CHUNK = TILES * LANES
SLOTS = 12


def head_kernel(
    count, width, hidden_size,
    h_hbm, g_hbm, w_ref, z_ref, lse_ref,
    h_ref, g_ref, wa, wb, x_ref, qbuf, rbuf, pbuf, lbuf, rin, lin, yin, nst, fst, m_ref, s_ref, carry,
    h_sem, g_sem, hops, wa_sem, wb_sem, nsend, nrecv, qsend, psend, ysend, rrecv, lrecv, yrecv, fsend, frecv,
):
    rows, feats = h_ref.shape
    stride = (width // LANES) * LANES
    rest = width - stride
    col = lax.axis_index("col")
    row = lax.axis_index("row")
    core = lax.rem(row, 2)
    mate = row + 1 - 2 * core
    across = lax.rem(row + 2, 4)
    far = 3 - row
    shift = row * rest

    def fetch(stream, t):
        if stream == 0:
            first, second, buf, sem = far, mate, wa, wa_sem
        else:
            first, second, buf, sem = across, row, wb, wb_sem
        part = first + (second - first) * (t // count)
        start = pl.multiple_of(stride * part + CHUNK * lax.rem(t, count), LANES)
        slot = lax.rem(t, SLOTS)
        return pltpu.make_async_copy(w_ref.at[:, pl.ds(start, CHUNK)], buf.at[slot], sem.at[slot])

    barrier = pltpu.get_barrier_semaphore()

    def tell_columns(sem):
        for step, there in ((-1, col > 0), (1, col < 3)):
            @pl.when(there)
            def _():
                pl.semaphore_signal(sem, inc=1, device_id_type=MESH, device_id={"col": col + step})

    for k in (2, 3, 1):
        pl.semaphore_signal(barrier, inc=1, device_id_type=MESH, device_id={"row": lax.rem(row + k, 4)})
    tell_columns(barrier)
    beside = (col + 2) // 3 + (5 - col) // 3

    h_copy = pltpu.make_async_copy(h_hbm, h_ref, h_sem)
    g_copy = pltpu.make_async_copy(g_hbm, g_ref, g_sem)
    h_copy.start()
    g_copy.start()
    for t in range(SLOTS):
        fetch(0, t).start()
        fetch(1, t).start()
    h_copy.wait()

    lane = lax.broadcasted_iota(jnp.int32, (rows, LANES), 1)
    sq = jnp.zeros((rows, LANES), jnp.float32)
    for j in range(feats // LANES):
        part = h_ref[:, j * LANES:(j + 1) * LANES].astype(jnp.float32)
        sq = sq + part * part
    sq = jnp.transpose(jnp.concatenate([sq, sq], axis=0))
    nst[row] = jnp.sum(sq, axis=0, keepdims=True)
    pl.semaphore_wait(barrier, 3 + beside)

    def norm_copy(k):
        return pltpu.make_async_remote_copy(
            src_ref=nst.at[row], dst_ref=nst.at[row], send_sem=nsend.at[k], recv_sem=nrecv.at[row],
            device_id={"row": lax.rem(row + k, 4)}, device_id_type=MESH,
        )

    for k in range(1, 4):
        norm_copy(k).start()
    for k in range(1, 4):
        peer = lax.rem(row + k, 4)
        pltpu.make_async_remote_copy(
            src_ref=nst.at[peer], dst_ref=nst.at[peer], send_sem=nsend.at[k], recv_sem=nrecv.at[peer],
            device_id={"row": peer}, device_id_type=MESH,
        ).wait_recv()
    tell_columns(hops.at[0])
    g_copy.wait()
    total = nst[0] + nst[1] + nst[2] + nst[3]
    scale = lax.rsqrt(total / hidden_size + EPS)
    scale = jnp.transpose(jnp.broadcast_to(scale, (LANES, LANES)))[:rows]
    for j in range(feats // LANES):
        cols = slice(j * LANES, (j + 1) * LANES)
        x_ref[:, cols] = (h_ref[:, cols].astype(jnp.float32) * scale * g_ref[cols].reshape(1, LANES)).astype(jnp.bfloat16)

    def product(stream, t):
        buf, sem = ((wa, wa_sem), (wb, wb_sem))[stream]
        fetch(stream, t).wait()
        slot = lax.rem(t, SLOTS)
        return jnp.dot(x_ref[...], buf[slot], preferred_element_type=jnp.float32)

    def refill(stream, t):
        @pl.when(t + SLOTS < 2 * count)
        def _():
            fetch(stream, t + SLOTS).start()

    def mate_copy(src, dst, send, recv, i):
        return pltpu.make_async_remote_copy(
            src_ref=src.at[i], dst_ref=dst.at[i], send_sem=send, recv_sem=recv.at[i],
            device_id={"row": mate}, device_id_type=MESH,
        )

    def across_copy(i):
        return pltpu.make_async_remote_copy(
            src_ref=rbuf.at[i], dst_ref=yin.at[i], send_sem=ysend, recv_sem=yrecv.at[i],
            device_id={"row": across}, device_id_type=MESH,
        )

    def far_step(i):
        qbuf[i] = product(0, i)
        mate_copy(qbuf, rin, qsend, rrecv, i).start()
        refill(0, i)

    def across_step(i):
        term = product(1, i)
        refill(1, i)
        mate_copy(qbuf, rin, qsend, rrecv, i).wait_recv()
        rbuf[i] = term + rin[i]
        across_copy(i).start()

    far_step(0)

    @pl.loop(0, count - 1)
    def _(i):
        far_step(i + 1)
        across_step(i)

    across_step(count - 1)
    pl.semaphore_wait(hops.at[0], beside)
    tell_columns(hops.at[1])

    @pl.loop(0, count)
    def _(i):
        pbuf[i] = product(0, count + i)
        mate_copy(pbuf, lin, psend, lrecv, i).start()
        refill(0, count + i)
        lbuf[i] = product(1, count + i)
        refill(1, count + i)

    pl.semaphore_wait(hops.at[1], beside)
    tell_columns(hops.at[2])

    turn = lax.rem(LANES - shift, LANES)
    keep = lane < LANES - shift

    def turned(i):
        mate_copy(pbuf, lin, psend, lrecv, i).wait_recv()
        across_copy(i).wait_recv()
        full = lbuf[i] + lin[i] + yin[i]
        return [pltpu.roll(full[:, k * LANES:(k + 1) * LANES], turn, 1) for k in range(TILES)]

    def arrive(i, first):
        rolled = turned(i)
        tiles = [jnp.where(keep, rolled[k], rolled[k + 1]) for k in range(TILES - 1)]
        at = 0
        if not first:
            tiles = [jnp.where(keep, carry[...], rolled[0])] + tiles
            at = pl.multiple_of(i * CHUNK - LANES, LANES)
        carry[...] = rolled[-1]
        z_ref[:, pl.ds(at, LANES * len(tiles))] = jnp.concatenate(tiles, axis=1)
        top = tiles[0]
        for tile in tiles[1:]:
            top = jnp.maximum(top, tile)
        if not first:
            top = jnp.maximum(top, m_ref[...])
        mass = jnp.exp(tiles[0] - top)
        for tile in tiles[1:]:
            mass = mass + jnp.exp(tile - top)
        if not first:
            mass = mass + s_ref[...] * jnp.exp(m_ref[...] - top)
        m_ref[...] = top
        s_ref[...] = mass

    arrive(0, True)
    pl.semaphore_wait(hops.at[2], beside)

    @pl.loop(1, count)
    def _(i):
        arrive(i, False)

    last = carry[...]
    z_ref[:, stride:] = last[:, :rest]
    last = jnp.where(lane < rest, last, -jnp.inf)
    top = jnp.maximum(m_ref[...], last)
    mass = s_ref[...] * jnp.exp(m_ref[...] - top) + jnp.exp(last - top)
    top = jnp.transpose(jnp.concatenate([top, top], axis=0))
    mass = jnp.transpose(jnp.concatenate([mass, mass], axis=0))
    peak = jnp.max(top, axis=0, keepdims=True)
    mass = jnp.sum(mass * jnp.exp(top - peak), axis=0, keepdims=True)
    me = col * 4 + row
    fst[me] = jnp.where(lane[:1] < rows, peak, mass)

    def stat_copy(dc, dr):
        k = dc * 4 + dr
        return pltpu.make_async_remote_copy(
            src_ref=fst.at[me], dst_ref=fst.at[me], send_sem=fsend.at[k], recv_sem=frecv.at[me],
            device_id={"col": lax.rem(col + dc, 4), "row": lax.rem(row + dr, 4)}, device_id_type=MESH,
        )

    peers = [(dc, dr) for dc in (3, 2, 1, 0) for dr in (2, 3, 1, 0) if dc or dr]
    for dc, dr in peers:
        stat_copy(dc, dr).start()
    for dc, dr in peers:
        pc, pr = lax.rem(col + dc, 4), lax.rem(row + dr, 4)
        peer = pc * 4 + pr
        pltpu.make_async_remote_copy(
            src_ref=fst.at[peer], dst_ref=fst.at[peer], send_sem=fsend.at[dc * 4 + dr], recv_sem=frecv.at[peer],
            device_id={"col": pc, "row": pr}, device_id_type=MESH,
        ).wait_recv()
    stats = fst[...]
    swapped = pltpu.roll(stats, LANES // 2, 2)
    peak = jnp.max(stats, axis=0)
    mass = jnp.sum(swapped * jnp.exp(stats - peak), axis=0)
    lse_ref[...] = peak + jnp.log(mass)

    for k in range(1, 4):
        norm_copy(k).wait_send()
    for src, dst, send, recv in ((qbuf, rin, qsend, rrecv), (pbuf, lin, psend, lrecv)):
        pltpu.make_async_remote_copy(
            src_ref=src, dst_ref=dst, send_sem=send, recv_sem=recv.at[0],
            device_id={"row": mate}, device_id_type=MESH,
        ).wait_send()
    pltpu.make_async_remote_copy(
        src_ref=rbuf, dst_ref=yin, send_sem=ysend, recv_sem=yrecv.at[0],
        device_id={"row": across}, device_id_type=MESH,
    ).wait_send()
    for dc, dr in peers:
        stat_copy(dc, dr).wait_send()


def solution(mesh):
    def local_head(hidden, norm_gain, w_head):
        rows, feats = hidden.shape
        width = w_head.shape[1] // 4
        count = (width // LANES + 1) // TILES
        block = (count, rows, CHUNK)
        dma = pltpu.SemaphoreType.DMA

        def body(*refs):
            head_kernel(count, width, feats * 4, *refs)

        z, lse = pl.pallas_call(
            body,
            out_shape=(
                jax.ShapeDtypeStruct((rows, width), jnp.float32),
                jax.ShapeDtypeStruct((1, LANES), jnp.float32),
            ),
            in_specs=[
                pl.BlockSpec(memory_space=pltpu.HBM),
                pl.BlockSpec(memory_space=pltpu.HBM),
                pl.BlockSpec(memory_space=pltpu.HBM),
            ],
            out_specs=(pl.BlockSpec(memory_space=pltpu.VMEM), pl.BlockSpec(memory_space=pltpu.VMEM)),
            scratch_shapes=[
                pltpu.VMEM((rows, feats), hidden.dtype),
                pltpu.VMEM((feats,), jnp.float32),
                pltpu.VMEM((SLOTS, feats, CHUNK), jnp.bfloat16),
                pltpu.VMEM((SLOTS, feats, CHUNK), jnp.bfloat16),
                pltpu.VMEM((rows, feats), jnp.bfloat16),
                *[pltpu.VMEM(block, jnp.float32) for _ in range(7)],
                pltpu.VMEM((4, 1, LANES), jnp.float32),
                pltpu.VMEM((16, 1, LANES), jnp.float32),
                *[pltpu.VMEM((rows, LANES), jnp.float32) for _ in range(3)],
                dma, dma, pltpu.SemaphoreType.REGULAR((3,)),
                dma((SLOTS,)), dma((SLOTS,)), dma((4,)), dma((4,)),
                dma, dma, dma, dma((count,)), dma((count,)), dma((count,)), dma((16,)), dma((16,)),
            ],
            compiler_params=pltpu.CompilerParams(
                collective_id=0, has_side_effects=True, vmem_limit_bytes=48 * 1024 * 1024
            ),
            name="head",
        )(pltpu.with_memory_space_constraint(hidden, pltpu.HBM), pltpu.with_memory_space_constraint(norm_gain, pltpu.HBM), w_head)
        log_norm = lse[0, :rows]
        return z - log_norm[:, None], log_norm

    return jax.shard_map(
        local_head,
        mesh=mesh,
        in_specs=(P("dp", "row"), P("row"), P("row", "col")),
        out_specs=(P("dp", ("col", "row")), P("dp")),
        check_vma=False,
    )
```

```python
import jax
import jax.numpy as jnp
from jax import lax
from jax.experimental import pallas as pl
from jax.experimental.pallas import tpu as pltpu
from jax.sharding import PartitionSpec as P

EPS = 1e-5
MESH = pl.DeviceIdType.MESH
LANES = 128
TILES = 3
CHUNK = TILES * LANES
EARLY = 2
SLOTS = 12


def head_kernel(
    count, width, hidden_size,
    h_hbm, g_hbm, w_ref, z_ref, lse_ref,
    h_ref, g_ref, wa, wb, x_ref, qbuf, rbuf, pbuf, lbuf, rin, lin, yin, nst, fst, m_ref, s_ref, carry,
    h_sem, g_sem, hops, wa_sem, wb_sem, nsend, nrecv, qsend, psend, ysend, rrecv, lrecv, yrecv, fsend, frecv,
):
    rows, feats = h_ref.shape
    stride = (width // LANES) * LANES
    rest = width - stride
    col = lax.axis_index("col")
    row = lax.axis_index("row")
    core = lax.rem(row, 2)
    mate = row + 1 - 2 * core
    across = lax.rem(row + 2, 4)
    far = 3 - row
    shift = row * rest

    def fetch(stream, t):
        if stream == 0:
            first, second, buf, sem = far, mate, wa, wa_sem
        else:
            first, second, buf, sem = across, row, wb, wb_sem
        part = first + (second - first) * (t // count)
        start = pl.multiple_of(stride * part + CHUNK * lax.rem(t, count), LANES)
        slot = lax.rem(t, SLOTS)
        return pltpu.make_async_copy(w_ref.at[:, pl.ds(start, CHUNK)], buf.at[slot], sem.at[slot])

    barrier = pltpu.get_barrier_semaphore()

    def tell_columns(sem):
        for step, there in ((-1, col > 0), (1, col < 3)):
            @pl.when(there)
            def _():
                pl.semaphore_signal(sem, inc=1, device_id_type=MESH, device_id={"col": col + step})

    for k in (2, 3, 1):
        pl.semaphore_signal(barrier, inc=1, device_id_type=MESH, device_id={"row": lax.rem(row + k, 4)})
    tell_columns(barrier)
    beside = (col + 2) // 3 + (5 - col) // 3

    h_copy = pltpu.make_async_copy(h_hbm, h_ref, h_sem)
    g_copy = pltpu.make_async_copy(g_hbm, g_ref, g_sem)
    h_copy.start()
    g_copy.start()
    h_copy.wait()
    for t in range(EARLY):
        fetch(0, t).start()
        fetch(1, t).start()

    lane = lax.broadcasted_iota(jnp.int32, (rows, LANES), 1)
    sq = jnp.zeros((rows, LANES), jnp.float32)
    for j in range(feats // LANES):
        part = h_ref[:, j * LANES:(j + 1) * LANES].astype(jnp.float32)
        sq = sq + part * part
    sq = jnp.transpose(jnp.concatenate([sq, sq], axis=0))
    nst[row] = jnp.sum(sq, axis=0, keepdims=True)
    pl.semaphore_wait(barrier, 3 + beside)

    def norm_copy(k):
        return pltpu.make_async_remote_copy(
            src_ref=nst.at[row], dst_ref=nst.at[row], send_sem=nsend.at[k], recv_sem=nrecv.at[row],
            device_id={"row": lax.rem(row + k, 4)}, device_id_type=MESH,
        )

    for k in (2, 3, 1):
        norm_copy(k).start()
    for t in range(EARLY, SLOTS):
        fetch(0, t).start()
        fetch(1, t).start()
    for k in range(1, 4):
        peer = lax.rem(row + k, 4)
        pltpu.make_async_remote_copy(
            src_ref=nst.at[peer], dst_ref=nst.at[peer], send_sem=nsend.at[k], recv_sem=nrecv.at[peer],
            device_id={"row": peer}, device_id_type=MESH,
        ).wait_recv()
    tell_columns(hops.at[0])
    g_copy.wait()
    total = nst[0] + nst[1] + nst[2] + nst[3]
    scale = lax.rsqrt(total / hidden_size + EPS)
    scale = jnp.transpose(jnp.broadcast_to(scale, (LANES, LANES)))[:rows]
    for j in range(feats // LANES):
        cols = slice(j * LANES, (j + 1) * LANES)
        x_ref[:, cols] = (h_ref[:, cols].astype(jnp.float32) * scale * g_ref[cols].reshape(1, LANES)).astype(jnp.bfloat16)

    def product(stream, t):
        buf, sem = ((wa, wa_sem), (wb, wb_sem))[stream]
        fetch(stream, t).wait()
        slot = lax.rem(t, SLOTS)
        return jnp.dot(x_ref[...], buf[slot], preferred_element_type=jnp.float32)

    def refill(stream, t):
        @pl.when(t + SLOTS < 2 * count)
        def _():
            fetch(stream, t + SLOTS).start()

    def mate_copy(src, dst, send, recv, i):
        return pltpu.make_async_remote_copy(
            src_ref=src.at[i], dst_ref=dst.at[i], send_sem=send, recv_sem=recv.at[i],
            device_id={"row": mate}, device_id_type=MESH,
        )

    def across_copy(i):
        return pltpu.make_async_remote_copy(
            src_ref=rbuf.at[i], dst_ref=yin.at[i], send_sem=ysend, recv_sem=yrecv.at[i],
            device_id={"row": across}, device_id_type=MESH,
        )

    def far_step(i):
        qbuf[i] = product(0, i)
        mate_copy(qbuf, rin, qsend, rrecv, i).start()
        refill(0, i)

    def across_step(i):
        term = product(1, i)
        refill(1, i)
        mate_copy(qbuf, rin, qsend, rrecv, i).wait_recv()
        rbuf[i] = term + rin[i]
        across_copy(i).start()

    far_step(0)

    @pl.loop(0, count - 1)
    def _(i):
        far_step(i + 1)
        across_step(i)

    across_step(count - 1)
    pl.semaphore_wait(hops.at[0], beside)
    tell_columns(hops.at[1])

    @pl.loop(0, count)
    def _(i):
        pbuf[i] = product(0, count + i)
        mate_copy(pbuf, lin, psend, lrecv, i).start()
        refill(0, count + i)
        lbuf[i] = product(1, count + i)
        refill(1, count + i)

    pl.semaphore_wait(hops.at[1], beside)
    tell_columns(hops.at[2])

    turn = lax.rem(LANES - shift, LANES)
    keep = lane < LANES - shift

    def turned(i):
        mate_copy(pbuf, lin, psend, lrecv, i).wait_recv()
        across_copy(i).wait_recv()
        full = lbuf[i] + lin[i] + yin[i]
        return [pltpu.roll(full[:, k * LANES:(k + 1) * LANES], turn, 1) for k in range(TILES)]

    def arrive(i, first):
        rolled = turned(i)
        tiles = [jnp.where(keep, rolled[k], rolled[k + 1]) for k in range(TILES - 1)]
        at = 0
        if not first:
            tiles = [jnp.where(keep, carry[...], rolled[0])] + tiles
            at = pl.multiple_of(i * CHUNK - LANES, LANES)
        carry[...] = rolled[-1]
        z_ref[:, pl.ds(at, LANES * len(tiles))] = jnp.concatenate(tiles, axis=1)
        top = tiles[0]
        for tile in tiles[1:]:
            top = jnp.maximum(top, tile)
        if not first:
            top = jnp.maximum(top, m_ref[...])
        mass = jnp.exp(tiles[0] - top)
        for tile in tiles[1:]:
            mass = mass + jnp.exp(tile - top)
        if not first:
            mass = mass + s_ref[...] * jnp.exp(m_ref[...] - top)
        m_ref[...] = top
        s_ref[...] = mass

    arrive(0, True)
    pl.semaphore_wait(hops.at[2], beside)

    @pl.loop(1, count)
    def _(i):
        arrive(i, False)

    last = carry[...]
    z_ref[:, stride:] = last[:, :rest]
    last = jnp.where(lane < rest, last, -jnp.inf)
    top = jnp.maximum(m_ref[...], last)
    mass = s_ref[...] * jnp.exp(m_ref[...] - top) + jnp.exp(last - top)
    top = jnp.transpose(jnp.concatenate([top, top], axis=0))
    mass = jnp.transpose(jnp.concatenate([mass, mass], axis=0))
    peak = jnp.max(top, axis=0, keepdims=True)
    mass = jnp.sum(mass * jnp.exp(top - peak), axis=0, keepdims=True)
    me = col * 4 + row
    fst[me] = jnp.where(lane[:1] < rows, peak, mass)

    peers = [
        (c, lax.rem(row + dr, 4))
        for c in (3 - col, lax.rem(col + 2, 4), lax.rem(5 - col, 4), col) for dr in (2, 3, 1, 0)
    ][:-1]

    def stat_copy(k, slot):
        c, r = peers[k]
        return pltpu.make_async_remote_copy(
            src_ref=fst.at[slot], dst_ref=fst.at[slot], send_sem=fsend.at[k], recv_sem=frecv.at[slot],
            device_id={"col": c, "row": r}, device_id_type=MESH,
        )

    for k in range(15):
        stat_copy(k, me).start()
    for k in reversed(range(15)):
        c, r = peers[k]
        stat_copy(k, c * 4 + r).wait_recv()
    stats = fst[...]
    swapped = pltpu.roll(stats, LANES // 2, 2)
    peak = jnp.max(stats, axis=0)
    mass = jnp.sum(swapped * jnp.exp(stats - peak), axis=0)
    lse_ref[...] = peak + jnp.log(mass)

    for k in range(1, 4):
        norm_copy(k).wait_send()
    for src, dst, send, recv in ((qbuf, rin, qsend, rrecv), (pbuf, lin, psend, lrecv)):
        pltpu.make_async_remote_copy(
            src_ref=src, dst_ref=dst, send_sem=send, recv_sem=recv.at[0],
            device_id={"row": mate}, device_id_type=MESH,
        ).wait_send()
    pltpu.make_async_remote_copy(
        src_ref=rbuf, dst_ref=yin, send_sem=ysend, recv_sem=yrecv.at[0],
        device_id={"row": across}, device_id_type=MESH,
    ).wait_send()
    for k in range(15):
        stat_copy(k, me).wait_send()


def solution(mesh):
    def local_head(hidden, norm_gain, w_head):
        rows, feats = hidden.shape
        width = w_head.shape[1] // 4
        count = (width // LANES + 1) // TILES
        block = (count, rows, CHUNK)
        dma = pltpu.SemaphoreType.DMA

        def body(*refs):
            head_kernel(count, width, feats * 4, *refs)

        z, lse = pl.pallas_call(
            body,
            out_shape=(
                jax.ShapeDtypeStruct((rows, width), jnp.float32),
                jax.ShapeDtypeStruct((1, LANES), jnp.float32),
            ),
            in_specs=[
                pl.BlockSpec(memory_space=pltpu.HBM),
                pl.BlockSpec(memory_space=pltpu.HBM),
                pl.BlockSpec(memory_space=pltpu.HBM),
            ],
            out_specs=(pl.BlockSpec(memory_space=pltpu.VMEM), pl.BlockSpec(memory_space=pltpu.VMEM)),
            scratch_shapes=[
                pltpu.VMEM((rows, feats), hidden.dtype),
                pltpu.VMEM((feats,), jnp.float32),
                pltpu.VMEM((SLOTS, feats, CHUNK), jnp.bfloat16),
                pltpu.VMEM((SLOTS, feats, CHUNK), jnp.bfloat16),
                pltpu.VMEM((rows, feats), jnp.bfloat16),
                *[pltpu.VMEM(block, jnp.float32) for _ in range(7)],
                pltpu.VMEM((4, 1, LANES), jnp.float32),
                pltpu.VMEM((16, 1, LANES), jnp.float32),
                *[pltpu.VMEM((rows, LANES), jnp.float32) for _ in range(3)],
                dma, dma, pltpu.SemaphoreType.REGULAR((3,)),
                dma((SLOTS,)), dma((SLOTS,)), dma((4,)), dma((4,)),
                dma, dma, dma, dma((count,)), dma((count,)), dma((count,)), dma((16,)), dma((16,)),
            ],
            compiler_params=pltpu.CompilerParams(
                collective_id=0, has_side_effects=True, vmem_limit_bytes=48 * 1024 * 1024
            ),
            name="head",
        )(pltpu.with_memory_space_constraint(hidden, pltpu.HBM), pltpu.with_memory_space_constraint(norm_gain, pltpu.HBM), w_head)
        log_norm = lse[0, :rows]
        return z - log_norm[:, None], log_norm

    return jax.shard_map(
        local_head,
        mesh=mesh,
        in_specs=(P("dp", "row"), P("row"), P("row", "col")),
        out_specs=(P("dp", ("col", "row")), P("dp")),
        check_vma=False,
    )
```

```python
import jax
import jax.numpy as jnp
from jax import lax
from jax.experimental import pallas as pl
from jax.experimental.pallas import tpu as pltpu
from jax.sharding import PartitionSpec as P

EPS = 1e-5
MESH = pl.DeviceIdType.MESH
LANES = 128
TILES = 3
CHUNK = TILES * LANES
EARLY = 2
SLOTS = 4


def head_kernel(
    count, width, hidden_size,
    h_hbm, g_hbm, w_ref, z_ref, lse_ref,
    h_ref, g_ref, wa, wb, x_ref, qbuf, rbuf, pbuf, lbuf, rin, lin, yin, nst, fst, m_ref, s_ref, carry,
    h_sem, g_sem, hops, wa_sem, wb_sem, nsend, nrecv, qsend, psend, ysend, rrecv, lrecv, yrecv, fsend, frecv,
):
    rows, feats = h_ref.shape
    stride = (width // LANES) * LANES
    rest = width - stride
    col = lax.axis_index("col")
    row = lax.axis_index("row")
    core = lax.rem(row, 2)
    mate = row + 1 - 2 * core
    across = lax.rem(row + 2, 4)
    far = 3 - row
    shift = row * rest

    def fetch(stream, t):
        if stream == 0:
            first, second, buf, sem = far, mate, wa, wa_sem
        else:
            first, second, buf, sem = across, row, wb, wb_sem
        part = first + (second - first) * (t // count)
        start = pl.multiple_of(stride * part + CHUNK * lax.rem(t, count), LANES)
        slot = lax.rem(t, SLOTS)
        return pltpu.make_async_copy(w_ref.at[:, pl.ds(start, CHUNK)], buf.at[slot], sem.at[slot])

    barrier = pltpu.get_barrier_semaphore()

    def tell_columns(sem):
        for step, there in ((-1, col > 0), (1, col < 3)):
            @pl.when(there)
            def _():
                pl.semaphore_signal(sem, inc=1, device_id_type=MESH, device_id={"col": col + step})

    for k in (2, 3, 1):
        pl.semaphore_signal(barrier, inc=1, device_id_type=MESH, device_id={"row": lax.rem(row + k, 4)})
    tell_columns(barrier)
    beside = (col + 2) // 3 + (5 - col) // 3

    h_copy = pltpu.make_async_copy(h_hbm, h_ref, h_sem)
    g_copy = pltpu.make_async_copy(g_hbm, g_ref, g_sem)
    h_copy.start()
    g_copy.start()
    h_copy.wait()
    for t in range(EARLY):
        fetch(0, t).start()
        fetch(1, t).start()

    lane = lax.broadcasted_iota(jnp.int32, (rows, LANES), 1)
    sq = jnp.zeros((rows, LANES), jnp.float32)
    for j in range(feats // LANES):
        part = h_ref[:, j * LANES:(j + 1) * LANES].astype(jnp.float32)
        sq = sq + part * part
    sq = jnp.transpose(jnp.concatenate([sq, sq], axis=0))
    nst[row] = jnp.sum(sq, axis=0, keepdims=True)
    pl.semaphore_wait(barrier, 3 + beside)

    def norm_copy(k):
        return pltpu.make_async_remote_copy(
            src_ref=nst.at[row], dst_ref=nst.at[row], send_sem=nsend.at[k], recv_sem=nrecv.at[row],
            device_id={"row": lax.rem(row + k, 4)}, device_id_type=MESH,
        )

    for k in (2, 3, 1):
        norm_copy(k).start()
    for t in range(EARLY, SLOTS):
        fetch(0, t).start()
        fetch(1, t).start()
    for k in range(1, 4):
        peer = lax.rem(row + k, 4)
        pltpu.make_async_remote_copy(
            src_ref=nst.at[peer], dst_ref=nst.at[peer], send_sem=nsend.at[k], recv_sem=nrecv.at[peer],
            device_id={"row": peer}, device_id_type=MESH,
        ).wait_recv()
    tell_columns(hops.at[0])
    g_copy.wait()
    total = nst[0] + nst[1] + nst[2] + nst[3]
    scale = lax.rsqrt(total / hidden_size + EPS)
    scale = jnp.transpose(jnp.broadcast_to(scale, (LANES, LANES)))[:rows]
    for j in range(feats // LANES):
        cols = slice(j * LANES, (j + 1) * LANES)
        x_ref[:, cols] = (h_ref[:, cols].astype(jnp.float32) * scale * g_ref[cols].reshape(1, LANES)).astype(jnp.bfloat16)

    def product(stream, t):
        buf, sem = ((wa, wa_sem), (wb, wb_sem))[stream]
        fetch(stream, t).wait()
        slot = lax.rem(t, SLOTS)
        return jnp.dot(x_ref[...], buf[slot], preferred_element_type=jnp.float32)

    def refill(stream, t):
        @pl.when(t + SLOTS < 2 * count)
        def _():
            fetch(stream, t + SLOTS).start()

    def mate_copy(src, dst, send, recv, i):
        return pltpu.make_async_remote_copy(
            src_ref=src.at[i], dst_ref=dst.at[i], send_sem=send, recv_sem=recv.at[i],
            device_id={"row": mate}, device_id_type=MESH,
        )

    def across_copy(i):
        return pltpu.make_async_remote_copy(
            src_ref=rbuf.at[i], dst_ref=yin.at[i], send_sem=ysend, recv_sem=yrecv.at[i],
            device_id={"row": across}, device_id_type=MESH,
        )

    def far_step(i):
        qbuf[i] = product(0, i)
        mate_copy(qbuf, rin, qsend, rrecv, i).start()
        refill(0, i)

    def across_step(i):
        term = product(1, i)
        refill(1, i)
        mate_copy(qbuf, rin, qsend, rrecv, i).wait_recv()
        rbuf[i] = term + rin[i]
        across_copy(i).start()

    far_step(0)

    @pl.loop(0, count - 1)
    def _(i):
        far_step(i + 1)
        across_step(i)

    across_step(count - 1)
    pl.semaphore_wait(hops.at[0], beside)
    tell_columns(hops.at[1])

    @pl.loop(0, count)
    def _(i):
        pbuf[i] = product(0, count + i)
        mate_copy(pbuf, lin, psend, lrecv, i).start()
        refill(0, count + i)
        lbuf[i] = product(1, count + i)
        refill(1, count + i)

    pl.semaphore_wait(hops.at[1], beside)
    tell_columns(hops.at[2])

    turn = lax.rem(LANES - shift, LANES)
    keep = lane < LANES - shift

    def turned(i):
        mate_copy(pbuf, lin, psend, lrecv, i).wait_recv()
        across_copy(i).wait_recv()
        full = lbuf[i] + lin[i] + yin[i]
        return [pltpu.roll(full[:, k * LANES:(k + 1) * LANES], turn, 1) for k in range(TILES)]

    def arrive(i, first):
        rolled = turned(i)
        tiles = [jnp.where(keep, rolled[k], rolled[k + 1]) for k in range(TILES - 1)]
        at = 0
        if not first:
            tiles = [jnp.where(keep, carry[...], rolled[0])] + tiles
            at = pl.multiple_of(i * CHUNK - LANES, LANES)
        carry[...] = rolled[-1]
        z_ref[:, pl.ds(at, LANES * len(tiles))] = jnp.concatenate(tiles, axis=1)
        top = tiles[0]
        for tile in tiles[1:]:
            top = jnp.maximum(top, tile)
        if not first:
            top = jnp.maximum(top, m_ref[...])
        mass = jnp.exp(tiles[0] - top)
        for tile in tiles[1:]:
            mass = mass + jnp.exp(tile - top)
        if not first:
            mass = mass + s_ref[...] * jnp.exp(m_ref[...] - top)
        m_ref[...] = top
        s_ref[...] = mass

    arrive(0, True)
    pl.semaphore_wait(hops.at[2], beside)

    @pl.loop(1, count)
    def _(i):
        arrive(i, False)

    last = carry[...]
    z_ref[:, stride:] = last[:, :rest]
    last = jnp.where(lane < rest, last, -jnp.inf)
    top = jnp.maximum(m_ref[...], last)
    mass = s_ref[...] * jnp.exp(m_ref[...] - top) + jnp.exp(last - top)
    top = jnp.transpose(jnp.concatenate([top, top], axis=0))
    mass = jnp.transpose(jnp.concatenate([mass, mass], axis=0))
    peak = jnp.max(top, axis=0, keepdims=True)
    mass = jnp.sum(mass * jnp.exp(top - peak), axis=0, keepdims=True)
    me = col * 4 + row
    fst[me] = jnp.where(lane[:1] < rows, peak, mass)

    peers = [
        (c, lax.rem(row + dr, 4))
        for c in (3 - col, lax.rem(col + 2, 4), lax.rem(5 - col, 4), col) for dr in (2, 3, 1, 0)
    ][:-1]

    def stat_copy(k, slot):
        c, r = peers[k]
        return pltpu.make_async_remote_copy(
            src_ref=fst.at[slot], dst_ref=fst.at[slot], send_sem=fsend.at[k], recv_sem=frecv.at[slot],
            device_id={"col": c, "row": r}, device_id_type=MESH,
        )

    for k in range(15):
        stat_copy(k, me).start()
    for k in reversed(range(15)):
        c, r = peers[k]
        stat_copy(k, c * 4 + r).wait_recv()
    stats = fst[...]
    swapped = pltpu.roll(stats, LANES // 2, 2)
    peak = jnp.max(stats, axis=0)
    mass = jnp.sum(swapped * jnp.exp(stats - peak), axis=0)
    lse_ref[...] = peak + jnp.log(mass)

    for k in range(1, 4):
        norm_copy(k).wait_send()
    for src, dst, send, recv in ((qbuf, rin, qsend, rrecv), (pbuf, lin, psend, lrecv)):
        pltpu.make_async_remote_copy(
            src_ref=src, dst_ref=dst, send_sem=send, recv_sem=recv.at[0],
            device_id={"row": mate}, device_id_type=MESH,
        ).wait_send()
    pltpu.make_async_remote_copy(
        src_ref=rbuf, dst_ref=yin, send_sem=ysend, recv_sem=yrecv.at[0],
        device_id={"row": across}, device_id_type=MESH,
    ).wait_send()
    for k in range(15):
        stat_copy(k, me).wait_send()


def solution(mesh):
    def local_head(hidden, norm_gain, w_head):
        rows, feats = hidden.shape
        width = w_head.shape[1] // 4
        count = (width // LANES + 1) // TILES
        block = (count, rows, CHUNK)
        dma = pltpu.SemaphoreType.DMA

        def body(*refs):
            head_kernel(count, width, feats * 4, *refs)

        z, lse = pl.pallas_call(
            body,
            out_shape=(
                jax.ShapeDtypeStruct((rows, width), jnp.float32),
                jax.ShapeDtypeStruct((1, LANES), jnp.float32),
            ),
            in_specs=[
                pl.BlockSpec(memory_space=pltpu.HBM),
                pl.BlockSpec(memory_space=pltpu.HBM),
                pl.BlockSpec(memory_space=pltpu.HBM),
            ],
            out_specs=(pl.BlockSpec(memory_space=pltpu.VMEM), pl.BlockSpec(memory_space=pltpu.VMEM)),
            scratch_shapes=[
                pltpu.VMEM((rows, feats), hidden.dtype),
                pltpu.VMEM((feats,), jnp.float32),
                pltpu.VMEM((SLOTS, feats, CHUNK), jnp.bfloat16),
                pltpu.VMEM((SLOTS, feats, CHUNK), jnp.bfloat16),
                pltpu.VMEM((rows, feats), jnp.bfloat16),
                *[pltpu.VMEM(block, jnp.float32) for _ in range(7)],
                pltpu.VMEM((4, 1, LANES), jnp.float32),
                pltpu.VMEM((16, 1, LANES), jnp.float32),
                *[pltpu.VMEM((rows, LANES), jnp.float32) for _ in range(3)],
                dma, dma, pltpu.SemaphoreType.REGULAR((3,)),
                dma((SLOTS,)), dma((SLOTS,)), dma((4,)), dma((4,)),
                dma, dma, dma, dma((count,)), dma((count,)), dma((count,)), dma((16,)), dma((16,)),
            ],
            compiler_params=pltpu.CompilerParams(
                collective_id=0, has_side_effects=True, vmem_limit_bytes=48 * 1024 * 1024
            ),
            name="head",
        )(pltpu.with_memory_space_constraint(hidden, pltpu.HBM), pltpu.with_memory_space_constraint(norm_gain, pltpu.HBM), w_head)
        log_norm = lse[0, :rows]
        return z - log_norm[:, None], log_norm

    return jax.shard_map(
        local_head,
        mesh=mesh,
        in_specs=(P("dp", "row"), P("row"), P("row", "col")),
        out_specs=(P("dp", ("col", "row")), P("dp")),
        check_vma=False,
    )
```

```python
import jax
import jax.numpy as jnp
from jax import lax
from jax.experimental import pallas as pl
from jax.experimental.pallas import tpu as pltpu
from jax.sharding import PartitionSpec as P

EPS = 1e-5
MESH = pl.DeviceIdType.MESH
LANES = 128
TILES = 5
CHUNK = TILES * LANES
EARLY = 2
SLOTS = 4


def head_kernel(
    count, width, hidden_size,
    h_hbm, g_hbm, w_ref, z_ref, lse_ref,
    h_ref, g_ref, wa, wb, x_ref, qbuf, rbuf, pbuf, lbuf, rin, lin, yin, nst, fst, m_ref, s_ref, carry,
    h_sem, g_sem, hops, wa_sem, wb_sem, nsend, nrecv, qsend, psend, ysend, rrecv, lrecv, yrecv, fsend, frecv,
):
    rows, feats = h_ref.shape
    stride = (width // LANES) * LANES
    rest = width - stride
    col = lax.axis_index("col")
    row = lax.axis_index("row")
    core = lax.rem(row, 2)
    mate = row + 1 - 2 * core
    across = lax.rem(row + 2, 4)
    far = 3 - row
    shift = row * rest

    def fetch(stream, t):
        if stream == 0:
            first, second, buf, sem = far, mate, wa, wa_sem
        else:
            first, second, buf, sem = across, row, wb, wb_sem
        part = first + (second - first) * (t // count)
        start = pl.multiple_of(stride * part + CHUNK * lax.rem(t, count), LANES)
        slot = lax.rem(t, SLOTS)
        return pltpu.make_async_copy(w_ref.at[:, pl.ds(start, CHUNK)], buf.at[slot], sem.at[slot])

    barrier = pltpu.get_barrier_semaphore()

    def tell_columns(sem):
        for step, there in ((-1, col > 0), (1, col < 3)):
            @pl.when(there)
            def _():
                pl.semaphore_signal(sem, inc=1, device_id_type=MESH, device_id={"col": col + step})

    for k in (2, 3, 1):
        pl.semaphore_signal(barrier, inc=1, device_id_type=MESH, device_id={"row": lax.rem(row + k, 4)})
    tell_columns(barrier)
    beside = (col + 2) // 3 + (5 - col) // 3

    h_copy = pltpu.make_async_copy(h_hbm, h_ref, h_sem)
    g_copy = pltpu.make_async_copy(g_hbm, g_ref, g_sem)
    h_copy.start()
    g_copy.start()
    h_copy.wait()
    for t in range(EARLY):
        fetch(0, t).start()
        fetch(1, t).start()

    lane = lax.broadcasted_iota(jnp.int32, (rows, LANES), 1)
    sq = jnp.zeros((rows, LANES), jnp.float32)
    for j in range(feats // LANES):
        part = h_ref[:, j * LANES:(j + 1) * LANES].astype(jnp.float32)
        sq = sq + part * part
    sq = jnp.transpose(jnp.concatenate([sq, sq], axis=0))
    nst[row] = jnp.sum(sq, axis=0, keepdims=True)
    pl.semaphore_wait(barrier, 3 + beside)

    def norm_copy(k):
        return pltpu.make_async_remote_copy(
            src_ref=nst.at[row], dst_ref=nst.at[row], send_sem=nsend.at[k], recv_sem=nrecv.at[row],
            device_id={"row": lax.rem(row + k, 4)}, device_id_type=MESH,
        )

    for k in (2, 3, 1):
        norm_copy(k).start()
    for t in range(EARLY, SLOTS):
        fetch(0, t).start()
        fetch(1, t).start()
    for k in range(1, 4):
        peer = lax.rem(row + k, 4)
        pltpu.make_async_remote_copy(
            src_ref=nst.at[peer], dst_ref=nst.at[peer], send_sem=nsend.at[k], recv_sem=nrecv.at[peer],
            device_id={"row": peer}, device_id_type=MESH,
        ).wait_recv()
    tell_columns(hops.at[0])
    g_copy.wait()
    total = nst[0] + nst[1] + nst[2] + nst[3]
    scale = lax.rsqrt(total / hidden_size + EPS)
    scale = jnp.transpose(jnp.broadcast_to(scale, (LANES, LANES)))[:rows]
    for j in range(feats // LANES):
        cols = slice(j * LANES, (j + 1) * LANES)
        x_ref[:, cols] = (h_ref[:, cols].astype(jnp.float32) * scale * g_ref[cols].reshape(1, LANES)).astype(jnp.bfloat16)

    def product(stream, t):
        buf, sem = ((wa, wa_sem), (wb, wb_sem))[stream]
        fetch(stream, t).wait()
        slot = lax.rem(t, SLOTS)
        return jnp.dot(x_ref[...], buf[slot], preferred_element_type=jnp.float32)

    def refill(stream, t):
        @pl.when(t + SLOTS < 2 * count)
        def _():
            fetch(stream, t + SLOTS).start()

    def mate_copy(src, dst, send, recv, i):
        return pltpu.make_async_remote_copy(
            src_ref=src.at[i], dst_ref=dst.at[i], send_sem=send, recv_sem=recv.at[i],
            device_id={"row": mate}, device_id_type=MESH,
        )

    def across_copy(i):
        return pltpu.make_async_remote_copy(
            src_ref=rbuf.at[i], dst_ref=yin.at[i], send_sem=ysend, recv_sem=yrecv.at[i],
            device_id={"row": across}, device_id_type=MESH,
        )

    def far_step(i):
        qbuf[i] = product(0, i)
        mate_copy(qbuf, rin, qsend, rrecv, i).start()
        refill(0, i)

    def across_step(i):
        term = product(1, i)
        refill(1, i)
        mate_copy(qbuf, rin, qsend, rrecv, i).wait_recv()
        rbuf[i] = term + rin[i]
        across_copy(i).start()

    far_step(0)

    @pl.loop(0, count - 1)
    def _(i):
        far_step(i + 1)
        across_step(i)

    across_step(count - 1)
    pl.semaphore_wait(hops.at[0], beside)
    tell_columns(hops.at[1])

    @pl.loop(0, count)
    def _(i):
        pbuf[i] = product(0, count + i)
        mate_copy(pbuf, lin, psend, lrecv, i).start()
        refill(0, count + i)
        lbuf[i] = product(1, count + i)
        refill(1, count + i)

    pl.semaphore_wait(hops.at[1], beside)
    tell_columns(hops.at[2])

    turn = lax.rem(LANES - shift, LANES)
    keep = lane < LANES - shift

    def turned(i):
        mate_copy(pbuf, lin, psend, lrecv, i).wait_recv()
        across_copy(i).wait_recv()
        full = lbuf[i] + lin[i] + yin[i]
        return [pltpu.roll(full[:, k * LANES:(k + 1) * LANES], turn, 1) for k in range(TILES)]

    def arrive(i, first):
        rolled = turned(i)
        tiles = [jnp.where(keep, rolled[k], rolled[k + 1]) for k in range(TILES - 1)]
        at = 0
        if not first:
            tiles = [jnp.where(keep, carry[...], rolled[0])] + tiles
            at = pl.multiple_of(i * CHUNK - LANES, LANES)
        carry[...] = rolled[-1]
        z_ref[:, pl.ds(at, LANES * len(tiles))] = jnp.concatenate(tiles, axis=1)
        top = tiles[0]
        for tile in tiles[1:]:
            top = jnp.maximum(top, tile)
        if not first:
            top = jnp.maximum(top, m_ref[...])
        mass = jnp.exp(tiles[0] - top)
        for tile in tiles[1:]:
            mass = mass + jnp.exp(tile - top)
        if not first:
            mass = mass + s_ref[...] * jnp.exp(m_ref[...] - top)
        m_ref[...] = top
        s_ref[...] = mass

    arrive(0, True)
    pl.semaphore_wait(hops.at[2], beside)

    @pl.loop(1, count)
    def _(i):
        arrive(i, False)

    last = carry[...]
    z_ref[:, stride:] = last[:, :rest]
    last = jnp.where(lane < rest, last, -jnp.inf)
    top = jnp.maximum(m_ref[...], last)
    mass = s_ref[...] * jnp.exp(m_ref[...] - top) + jnp.exp(last - top)
    top = jnp.transpose(jnp.concatenate([top, top], axis=0))
    mass = jnp.transpose(jnp.concatenate([mass, mass], axis=0))
    peak = jnp.max(top, axis=0, keepdims=True)
    mass = jnp.sum(mass * jnp.exp(top - peak), axis=0, keepdims=True)
    me = col * 4 + row
    fst[me] = jnp.where(lane[:1] < rows, peak, mass)

    peers = [
        (c, lax.rem(row + dr, 4))
        for c in (3 - col, lax.rem(col + 2, 4), lax.rem(5 - col, 4), col) for dr in (2, 3, 1, 0)
    ][:-1]

    def stat_copy(k, slot):
        c, r = peers[k]
        return pltpu.make_async_remote_copy(
            src_ref=fst.at[slot], dst_ref=fst.at[slot], send_sem=fsend.at[k], recv_sem=frecv.at[slot],
            device_id={"col": c, "row": r}, device_id_type=MESH,
        )

    for k in range(15):
        stat_copy(k, me).start()
    for k in reversed(range(15)):
        c, r = peers[k]
        stat_copy(k, c * 4 + r).wait_recv()
    stats = fst[...]
    swapped = pltpu.roll(stats, LANES // 2, 2)
    peak = jnp.max(stats, axis=0)
    mass = jnp.sum(swapped * jnp.exp(stats - peak), axis=0)
    lse_ref[...] = peak + jnp.log(mass)

    for k in range(1, 4):
        norm_copy(k).wait_send()
    for src, dst, send, recv in ((qbuf, rin, qsend, rrecv), (pbuf, lin, psend, lrecv)):
        pltpu.make_async_remote_copy(
            src_ref=src, dst_ref=dst, send_sem=send, recv_sem=recv.at[0],
            device_id={"row": mate}, device_id_type=MESH,
        ).wait_send()
    pltpu.make_async_remote_copy(
        src_ref=rbuf, dst_ref=yin, send_sem=ysend, recv_sem=yrecv.at[0],
        device_id={"row": across}, device_id_type=MESH,
    ).wait_send()
    for k in range(15):
        stat_copy(k, me).wait_send()


def solution(mesh):
    def local_head(hidden, norm_gain, w_head):
        rows, feats = hidden.shape
        width = w_head.shape[1] // 4
        count = (width // LANES + 1) // TILES
        block = (count, rows, CHUNK)
        dma = pltpu.SemaphoreType.DMA

        def body(*refs):
            head_kernel(count, width, feats * 4, *refs)

        z, lse = pl.pallas_call(
            body,
            out_shape=(
                jax.ShapeDtypeStruct((rows, width), jnp.float32),
                jax.ShapeDtypeStruct((1, LANES), jnp.float32),
            ),
            in_specs=[
                pl.BlockSpec(memory_space=pltpu.HBM),
                pl.BlockSpec(memory_space=pltpu.HBM),
                pl.BlockSpec(memory_space=pltpu.HBM),
            ],
            out_specs=(pl.BlockSpec(memory_space=pltpu.VMEM), pl.BlockSpec(memory_space=pltpu.VMEM)),
            scratch_shapes=[
                pltpu.VMEM((rows, feats), hidden.dtype),
                pltpu.VMEM((feats,), jnp.float32),
                pltpu.VMEM((SLOTS, feats, CHUNK), jnp.bfloat16),
                pltpu.VMEM((SLOTS, feats, CHUNK), jnp.bfloat16),
                pltpu.VMEM((rows, feats), jnp.bfloat16),
                *[pltpu.VMEM(block, jnp.float32) for _ in range(7)],
                pltpu.VMEM((4, 1, LANES), jnp.float32),
                pltpu.VMEM((16, 1, LANES), jnp.float32),
                *[pltpu.VMEM((rows, LANES), jnp.float32) for _ in range(3)],
                dma, dma, pltpu.SemaphoreType.REGULAR((3,)),
                dma((SLOTS,)), dma((SLOTS,)), dma((4,)), dma((4,)),
                dma, dma, dma, dma((count,)), dma((count,)), dma((count,)), dma((16,)), dma((16,)),
            ],
            compiler_params=pltpu.CompilerParams(
                collective_id=0, has_side_effects=True, vmem_limit_bytes=48 * 1024 * 1024
            ),
            name="head",
        )(pltpu.with_memory_space_constraint(hidden, pltpu.HBM), pltpu.with_memory_space_constraint(norm_gain, pltpu.HBM), w_head)
        log_norm = lse[0, :rows]
        return z - log_norm[:, None], log_norm

    return jax.shard_map(
        local_head,
        mesh=mesh,
        in_specs=(P("dp", "row"), P("row"), P("row", "col")),
        out_specs=(P("dp", ("col", "row")), P("dp")),
        check_vma=False,
    )
```

```python
import jax
import jax.numpy as jnp
from jax import lax
from jax.experimental import pallas as pl
from jax.experimental.pallas import tpu as pltpu
from jax.sharding import PartitionSpec as P

EPS = 1e-5
MESH = pl.DeviceIdType.MESH
LANES = 128
TILES = 3
CHUNK = TILES * LANES
EARLY = 2
SLOTS = 4


def head_kernel(
    count, width, hidden_size,
    h_hbm, g_hbm, w_ref, z_ref, lse_ref,
    h_ref, g_ref, wa, wb, x_ref, qbuf, rbuf, pbuf, lbuf, rin, lin, yin, nst, fst, m_ref, s_ref, carry,
    h_sem, g_sem, hops, wa_sem, wb_sem, nsend, nrecv, qsend, psend, ysend, rrecv, lrecv, yrecv, fsend, frecv,
):
    rows, feats = h_ref.shape
    stride = (width // LANES) * LANES
    rest = width - stride
    col = lax.axis_index("col")
    row = lax.axis_index("row")
    core = lax.rem(row, 2)
    mate = row + 1 - 2 * core
    across = lax.rem(row + 2, 4)
    far = 3 - row
    shift = row * rest

    def fetch(stream, t):
        if stream == 0:
            first, second, buf, sem = far, mate, wa, wa_sem
        else:
            first, second, buf, sem = across, row, wb, wb_sem
        part = first + (second - first) * (t // count)
        start = pl.multiple_of(stride * part + CHUNK * lax.rem(t, count), LANES)
        slot = lax.rem(t, SLOTS)
        return pltpu.make_async_copy(w_ref.at[:, pl.ds(start, CHUNK)], buf.at[slot], sem.at[slot])

    barrier = pltpu.get_barrier_semaphore()

    def tell_columns(sem):
        for step, there in ((-1, col > 0), (1, col < 3)):
            @pl.when(there)
            def _():
                pl.semaphore_signal(sem, inc=1, device_id_type=MESH, device_id={"col": col + step})

    for k in (2, 3, 1):
        pl.semaphore_signal(barrier, inc=1, device_id_type=MESH, device_id={"row": lax.rem(row + k, 4)})
    tell_columns(barrier)
    beside = (col + 2) // 3 + (5 - col) // 3

    h_copy = pltpu.make_async_copy(h_hbm, h_ref, h_sem)
    g_copy = pltpu.make_async_copy(g_hbm, g_ref, g_sem)
    h_copy.start()
    g_copy.start()
    h_copy.wait()
    for t in range(EARLY):
        fetch(0, t).start()
        fetch(1, t).start()

    lane = lax.broadcasted_iota(jnp.int32, (rows, LANES), 1)
    sq = jnp.zeros((rows, LANES), jnp.float32)
    for j in range(feats // LANES):
        part = h_ref[:, j * LANES:(j + 1) * LANES].astype(jnp.float32)
        sq = sq + part * part
    sq = jnp.transpose(jnp.concatenate([sq, sq], axis=0))
    nst[row] = jnp.sum(sq, axis=0, keepdims=True)
    pl.semaphore_wait(barrier, 3 + beside)

    def norm_copy(k):
        return pltpu.make_async_remote_copy(
            src_ref=nst.at[row], dst_ref=nst.at[row], send_sem=nsend.at[k], recv_sem=nrecv.at[row],
            device_id={"row": lax.rem(row + k, 4)}, device_id_type=MESH,
        )

    for k in (2, 3, 1):
        norm_copy(k).start()
    for t in range(EARLY, SLOTS):
        fetch(0, t).start()
        fetch(1, t).start()
    for k in range(1, 4):
        peer = lax.rem(row + k, 4)
        pltpu.make_async_remote_copy(
            src_ref=nst.at[peer], dst_ref=nst.at[peer], send_sem=nsend.at[k], recv_sem=nrecv.at[peer],
            device_id={"row": peer}, device_id_type=MESH,
        ).wait_recv()
    tell_columns(hops.at[0])
    g_copy.wait()
    total = nst[0] + nst[1] + nst[2] + nst[3]
    scale = lax.rsqrt(total / hidden_size + EPS)
    scale = jnp.transpose(jnp.broadcast_to(scale, (LANES, LANES)))[:rows]
    for j in range(feats // LANES):
        cols = slice(j * LANES, (j + 1) * LANES)
        x_ref[:, cols] = (h_ref[:, cols].astype(jnp.float32) * scale * g_ref[cols].reshape(1, LANES)).astype(jnp.bfloat16)

    def product(stream, t):
        buf, sem = ((wa, wa_sem), (wb, wb_sem))[stream]
        fetch(stream, t).wait()
        slot = lax.rem(t, SLOTS)
        return jnp.dot(x_ref[...], buf[slot], preferred_element_type=jnp.float32)

    def refill(stream, t):
        @pl.when(t + SLOTS < 2 * count)
        def _():
            fetch(stream, t + SLOTS).start()

    def mate_copy(src, dst, send, recv, i):
        return pltpu.make_async_remote_copy(
            src_ref=src.at[i], dst_ref=dst.at[i], send_sem=send, recv_sem=recv.at[i],
            device_id={"row": mate}, device_id_type=MESH,
        )

    def across_copy(i):
        return pltpu.make_async_remote_copy(
            src_ref=rbuf.at[i], dst_ref=yin.at[i], send_sem=ysend, recv_sem=yrecv.at[i],
            device_id={"row": across}, device_id_type=MESH,
        )

    def far_step(i):
        qbuf[i] = product(0, i)
        mate_copy(qbuf, rin, qsend, rrecv, i).start()
        refill(0, i)

    def across_step(i):
        term = product(1, i)
        refill(1, i)
        mate_copy(qbuf, rin, qsend, rrecv, i).wait_recv()
        rbuf[i] = term + rin[i]
        across_copy(i).start()

    far_step(0)

    @pl.loop(0, count - 1)
    def _(i):
        far_step(i + 1)
        across_step(i)

    across_step(count - 1)
    pl.semaphore_wait(hops.at[0], beside)
    tell_columns(hops.at[1])

    @pl.loop(0, count)
    def _(i):
        pbuf[i] = product(0, count + i)
        mate_copy(pbuf, lin, psend, lrecv, i).start()
        refill(0, count + i)
        lbuf[i] = product(1, count + i)
        refill(1, count + i)

    pl.semaphore_wait(hops.at[1], beside)
    tell_columns(hops.at[2])

    turn = lax.rem(LANES - shift, LANES)
    keep = lane < LANES - shift

    def turned(i):
        mate_copy(pbuf, lin, psend, lrecv, i).wait_recv()
        across_copy(i).wait_recv()
        full = lbuf[i] + lin[i] + yin[i]
        return [pltpu.roll(full[:, k * LANES:(k + 1) * LANES], turn, 1) for k in range(TILES)]

    def arrive(i, first):
        rolled = turned(i)
        tiles = [jnp.where(keep, rolled[k], rolled[k + 1]) for k in range(TILES - 1)]
        at = 0
        if not first:
            tiles = [jnp.where(keep, carry[...], rolled[0])] + tiles
            at = pl.multiple_of(i * CHUNK - LANES, LANES)
        carry[...] = rolled[-1]
        z_ref[:, pl.ds(at, LANES * len(tiles))] = jnp.concatenate(tiles, axis=1)
        top = tiles[0]
        for tile in tiles[1:]:
            top = jnp.maximum(top, tile)
        if not first:
            top = jnp.maximum(top, m_ref[...])
        mass = jnp.exp(tiles[0] - top)
        for tile in tiles[1:]:
            mass = mass + jnp.exp(tile - top)
        if not first:
            mass = mass + s_ref[...] * jnp.exp(m_ref[...] - top)
        m_ref[...] = top
        s_ref[...] = mass

    arrive(0, True)
    pl.semaphore_wait(hops.at[2], beside)

    @pl.loop(1, count)
    def _(i):
        arrive(i, False)

    last = carry[...]
    z_ref[:, stride:] = last[:, :rest]
    last = jnp.where(lane < rest, last, -jnp.inf)
    top = jnp.maximum(m_ref[...], last)
    mass = s_ref[...] * jnp.exp(m_ref[...] - top) + jnp.exp(last - top)
    top = jnp.transpose(jnp.concatenate([top, top], axis=0))
    mass = jnp.transpose(jnp.concatenate([mass, mass], axis=0))
    peak = jnp.max(top, axis=0, keepdims=True)
    mass = jnp.sum(mass * jnp.exp(top - peak), axis=0, keepdims=True)
    me = col * 4 + row
    fst[me] = jnp.where(lane[:1] < rows, peak, mass)

    peers = [
        (c, lax.rem(row + dr, 4))
        for c in (3 - col, lax.rem(col + 2, 4), lax.rem(5 - col, 4), col) for dr in (2, 3, 1, 0)
    ][:-1]

    def stat_copy(k, slot):
        c, r = peers[k]
        return pltpu.make_async_remote_copy(
            src_ref=fst.at[slot], dst_ref=fst.at[slot], send_sem=fsend.at[k], recv_sem=frecv.at[slot],
            device_id={"col": c, "row": r}, device_id_type=MESH,
        )

    for k in range(15):
        stat_copy(k, me).start()
    for k in reversed(range(15)):
        c, r = peers[k]
        stat_copy(k, c * 4 + r).wait_recv()
    stats = fst[...]
    swapped = pltpu.roll(stats, LANES // 2, 2)
    peak = jnp.max(stats, axis=0)
    mass = jnp.sum(swapped * jnp.exp(stats - peak), axis=0)
    lse_ref[...] = peak + jnp.log(mass)

    for k in range(1, 4):
        norm_copy(k).wait_send()
    for src, dst, send, recv in ((qbuf, rin, qsend, rrecv), (pbuf, lin, psend, lrecv)):
        pltpu.make_async_remote_copy(
            src_ref=src, dst_ref=dst, send_sem=send, recv_sem=recv.at[0],
            device_id={"row": mate}, device_id_type=MESH,
        ).wait_send()
    pltpu.make_async_remote_copy(
        src_ref=rbuf, dst_ref=yin, send_sem=ysend, recv_sem=yrecv.at[0],
        device_id={"row": across}, device_id_type=MESH,
    ).wait_send()
    for k in range(15):
        stat_copy(k, me).wait_send()


def finish_kernel(z_ref, lse_ref, out_ref, buf, sems):
    rows = z_ref.shape[0]
    column = jnp.transpose(jnp.broadcast_to(lse_ref[...], (LANES, LANES)))[:rows, :1]
    copies = []
    for k in range(rows // 8):
        part = slice(k * 8, k * 8 + 8)
        buf[part] = z_ref[part] - column[part]
        copies.append(pltpu.make_async_copy(buf.at[part], out_ref.at[part], sems.at[k]))
        copies[-1].start()
    for copy in copies:
        copy.wait()


def solution(mesh):
    def local_head(hidden, norm_gain, w_head):
        rows, feats = hidden.shape
        width = w_head.shape[1] // 4
        count = (width // LANES + 1) // TILES
        block = (count, rows, CHUNK)
        dma = pltpu.SemaphoreType.DMA

        def body(*refs):
            head_kernel(count, width, feats * 4, *refs)

        z, lse = pl.pallas_call(
            body,
            out_shape=(
                jax.ShapeDtypeStruct((rows, width), jnp.float32),
                jax.ShapeDtypeStruct((1, LANES), jnp.float32),
            ),
            in_specs=[
                pl.BlockSpec(memory_space=pltpu.HBM),
                pl.BlockSpec(memory_space=pltpu.HBM),
                pl.BlockSpec(memory_space=pltpu.HBM),
            ],
            out_specs=(pl.BlockSpec(memory_space=pltpu.VMEM), pl.BlockSpec(memory_space=pltpu.VMEM)),
            scratch_shapes=[
                pltpu.VMEM((rows, feats), hidden.dtype),
                pltpu.VMEM((feats,), jnp.float32),
                pltpu.VMEM((SLOTS, feats, CHUNK), jnp.bfloat16),
                pltpu.VMEM((SLOTS, feats, CHUNK), jnp.bfloat16),
                pltpu.VMEM((rows, feats), jnp.bfloat16),
                *[pltpu.VMEM(block, jnp.float32) for _ in range(7)],
                pltpu.VMEM((4, 1, LANES), jnp.float32),
                pltpu.VMEM((16, 1, LANES), jnp.float32),
                *[pltpu.VMEM((rows, LANES), jnp.float32) for _ in range(3)],
                dma, dma, pltpu.SemaphoreType.REGULAR((3,)),
                dma((SLOTS,)), dma((SLOTS,)), dma((4,)), dma((4,)),
                dma, dma, dma, dma((count,)), dma((count,)), dma((count,)), dma((16,)), dma((16,)),
            ],
            compiler_params=pltpu.CompilerParams(
                collective_id=0, has_side_effects=True, vmem_limit_bytes=48 * 1024 * 1024
            ),
            name="head",
        )(pltpu.with_memory_space_constraint(hidden, pltpu.HBM), pltpu.with_memory_space_constraint(norm_gain, pltpu.HBM), w_head)
        log_norm = lse[0, :rows]
        log_probs = pl.pallas_call(
            finish_kernel,
            out_shape=jax.ShapeDtypeStruct((rows, width), jnp.float32),
            in_specs=[pl.BlockSpec(memory_space=pltpu.VMEM), pl.BlockSpec(memory_space=pltpu.VMEM)],
            out_specs=pl.BlockSpec(memory_space=pltpu.HBM),
            scratch_shapes=[pltpu.VMEM((rows, width), jnp.float32), dma((rows // 8,))],
            compiler_params=pltpu.CompilerParams(vmem_limit_bytes=8 * 1024 * 1024),
            name="finish",
        )(z, lse)
        return log_probs, log_norm

    return jax.shard_map(
        local_head,
        mesh=mesh,
        in_specs=(P("dp", "row"), P("row"), P("row", "col")),
        out_specs=(P("dp", ("col", "row")), P("dp")),
        check_vma=False,
    )
```

```python
import jax
import jax.numpy as jnp
from jax import lax
from jax.experimental import pallas as pl
from jax.experimental.pallas import tpu as pltpu
from jax.sharding import PartitionSpec as P

EPS = 1e-5
MESH = pl.DeviceIdType.MESH
LANES = 128
TILES = 3
CHUNK = TILES * LANES
EARLY = 2
GROUPS = (1, 1, 2, 4, 6, 6, 3, 1, 1)
SLOTS = 4


def head_kernel(
    count, width, hidden_size,
    h_hbm, g_hbm, w_ref, z_ref, lse_ref,
    h_ref, g_ref, wa, wb, x_ref, qbuf, rbuf, pbuf, lbuf, rin, lin, yin, nst, fst, m_ref, s_ref, carry, edge_out, edge_in,
    h_sem, g_sem, hops, wa_sem, wb_sem, nsend, nrecv, qsend, psend, ysend, rrecv, lrecv, yrecv, fsend, frecv, esend, erecv,
):
    rows, feats = h_ref.shape
    stride = (width // LANES) * LANES
    rest = width - stride
    col = lax.axis_index("col")
    row = lax.axis_index("row")
    core = lax.rem(row, 2)
    mate = row + 1 - 2 * core
    across = lax.rem(row + 2, 4)
    far = 3 - row
    shift = row * rest

    def fetch(stream, t):
        if stream == 0:
            first, second, buf, sem = far, mate, wa, wa_sem
        else:
            first, second, buf, sem = across, row, wb, wb_sem
        part = first + (second - first) * (t // count)
        start = pl.multiple_of(stride * part + CHUNK * lax.rem(t, count), LANES)
        slot = lax.rem(t, SLOTS)
        return pltpu.make_async_copy(w_ref.at[:, pl.ds(start, CHUNK)], buf.at[slot], sem.at[slot])

    barrier = pltpu.get_barrier_semaphore()

    def tell_columns(sem):
        for step, there in ((-1, col > 0), (1, col < 3)):
            @pl.when(there)
            def _():
                pl.semaphore_signal(sem, inc=1, device_id_type=MESH, device_id={"col": col + step})

    for k in (2, 3, 1):
        pl.semaphore_signal(barrier, inc=1, device_id_type=MESH, device_id={"row": lax.rem(row + k, 4)})
    tell_columns(barrier)
    beside = (col + 2) // 3 + (5 - col) // 3

    h_copy = pltpu.make_async_copy(h_hbm, h_ref, h_sem)
    g_copy = pltpu.make_async_copy(g_hbm, g_ref, g_sem)
    h_copy.start()
    g_copy.start()
    h_copy.wait()
    for t in range(EARLY):
        fetch(0, t).start()
        fetch(1, t).start()

    lane = lax.broadcasted_iota(jnp.int32, (rows, LANES), 1)
    sq = jnp.zeros((rows, LANES), jnp.float32)
    for j in range(feats // LANES):
        part = h_ref[:, j * LANES:(j + 1) * LANES].astype(jnp.float32)
        sq = sq + part * part
    sq = jnp.transpose(jnp.concatenate([sq, sq], axis=0))
    nst[row] = jnp.sum(sq, axis=0, keepdims=True)
    pl.semaphore_wait(barrier, 3 + beside)

    def norm_copy(k):
        return pltpu.make_async_remote_copy(
            src_ref=nst.at[row], dst_ref=nst.at[row], send_sem=nsend.at[k], recv_sem=nrecv.at[row],
            device_id={"row": lax.rem(row + k, 4)}, device_id_type=MESH,
        )

    for k in (2, 3, 1):
        norm_copy(k).start()
    for t in range(EARLY, SLOTS):
        fetch(0, t).start()
        fetch(1, t).start()
    for k in range(1, 4):
        peer = lax.rem(row + k, 4)
        pltpu.make_async_remote_copy(
            src_ref=nst.at[peer], dst_ref=nst.at[peer], send_sem=nsend.at[k], recv_sem=nrecv.at[peer],
            device_id={"row": peer}, device_id_type=MESH,
        ).wait_recv()
    tell_columns(hops.at[0])
    g_copy.wait()
    total = nst[0] + nst[1] + nst[2] + nst[3]
    scale = lax.rsqrt(total / hidden_size + EPS)
    scale = jnp.transpose(jnp.broadcast_to(scale, (LANES, LANES)))[:rows]
    for j in range(feats // LANES):
        cols = slice(j * LANES, (j + 1) * LANES)
        x_ref[:, cols] = (h_ref[:, cols].astype(jnp.float32) * scale * g_ref[cols].reshape(1, LANES)).astype(jnp.bfloat16)

    def product(stream, t):
        buf, sem = ((wa, wa_sem), (wb, wb_sem))[stream]
        fetch(stream, t).wait()
        slot = lax.rem(t, SLOTS)
        return jnp.dot(x_ref[...], buf[slot], preferred_element_type=jnp.float32)

    def refill(stream, t):
        @pl.when(t + SLOTS < 2 * count)
        def _():
            fetch(stream, t + SLOTS).start()

    def mate_copy(src, dst, send, recv, i):
        return pltpu.make_async_remote_copy(
            src_ref=src.at[i], dst_ref=dst.at[i], send_sem=send, recv_sem=recv.at[i],
            device_id={"row": mate}, device_id_type=MESH,
        )

    starts = [sum(GROUPS[:k]) for k in range(len(GROUPS))]

    def across_copy(k, tiles=TILES):
        part = (pl.ds(starts[k], GROUPS[k]), slice(None), pl.ds(0, tiles * LANES))
        return pltpu.make_async_remote_copy(
            src_ref=rbuf.at[part], dst_ref=yin.at[part], send_sem=ysend.at[k], recv_sem=yrecv.at[k],
            device_id={"row": across}, device_id_type=MESH,
        )

    def each_across(k, act):
        if k < len(GROUPS) - 1:
            act(across_copy(k))
            return

        @pl.when(core == 0)
        def _():
            act(across_copy(k, TILES - 1))

        @pl.when(core == 1)
        def _():
            act(across_copy(k))

    edge_copy = pltpu.make_async_remote_copy(
        src_ref=edge_out, dst_ref=edge_in, send_sem=esend, recv_sem=erecv,
        device_id={"row": mate}, device_id_type=MESH,
    )

    def far_step(i):
        qbuf[i] = product(0, i)
        mate_copy(qbuf, rin, qsend, rrecv, i).start()
        refill(0, i)

    def across_step(i):
        term = product(1, i)
        refill(1, i)
        mate_copy(qbuf, rin, qsend, rrecv, i).wait_recv()
        rbuf[i] = term + rin[i]

    far_step(0)

    @pl.loop(0, count - 1)
    def _(i):
        far_step(i + 1)
        across_step(i)
        for k in range(len(GROUPS) - 1):
            @pl.when(i == starts[k] + GROUPS[k] - 1)
            def _():
                each_across(k, lambda copy: copy.start())

    across_step(count - 1)
    each_across(len(GROUPS) - 1, lambda copy: copy.start())
    pl.semaphore_wait(hops.at[0], beside)
    tell_columns(hops.at[1])

    @pl.loop(0, count)
    def _(i):
        pbuf[i] = product(0, count + i)
        mate_copy(pbuf, lin, psend, lrecv, i).start()
        refill(0, count + i)
        lbuf[i] = product(1, count + i)
        refill(1, count + i)

    pl.semaphore_wait(hops.at[1], beside)
    tell_columns(hops.at[2])

    turn = lax.rem(LANES - shift, LANES)
    keep = lane < LANES - shift

    def arrive(i, first, last):
        mate_copy(pbuf, lin, psend, lrecv, i).wait_recv()
        if first or last:
            each_across(0 if first else len(GROUPS) - 1, lambda copy: copy.wait_recv())
        else:
            for k in range(1, len(GROUPS) - 1):
                @pl.when(i == starts[k])
                def _():
                    each_across(k, lambda copy: copy.wait_recv())
        full = lbuf[i] + lin[i] + yin[i]
        parts = [full[:, k * LANES:(k + 1) * LANES] for k in range(TILES)]
        if first:
            edge_out[...] = parts[0]

            @pl.when(core == 1)
            def _():
                edge_copy.start()
        if last:
            @pl.when(core == 0)
            def _():
                edge_copy.wait_recv()

            parts[-1] = jnp.where(core == 0, edge_in[...], parts[-1])
        rolled = [pltpu.roll(part, turn, 1) for part in parts]
        tiles = [jnp.where(keep, rolled[k], rolled[k + 1]) for k in range(TILES - 1)]
        at = 0
        if not first:
            tiles = [jnp.where(keep, carry[...], rolled[0])] + tiles
            at = pl.multiple_of(i * CHUNK - LANES, LANES)
        carry[...] = rolled[-1]
        z_ref[:, pl.ds(at, LANES * len(tiles))] = jnp.concatenate(tiles, axis=1)
        top = tiles[0]
        for tile in tiles[1:]:
            top = jnp.maximum(top, tile)
        if not first:
            top = jnp.maximum(top, m_ref[...])
        mass = jnp.exp(tiles[0] - top)
        for tile in tiles[1:]:
            mass = mass + jnp.exp(tile - top)
        if not first:
            mass = mass + s_ref[...] * jnp.exp(m_ref[...] - top)
        m_ref[...] = top
        s_ref[...] = mass

    arrive(0, True, False)
    pl.semaphore_wait(hops.at[2], beside)

    @pl.loop(1, count - 1)
    def _(i):
        arrive(i, False, False)

    arrive(count - 1, False, True)

    last = carry[...]
    z_ref[:, stride:] = last[:, :rest]
    last = jnp.where(lane < rest, last, -jnp.inf)
    top = jnp.maximum(m_ref[...], last)
    mass = s_ref[...] * jnp.exp(m_ref[...] - top) + jnp.exp(last - top)
    top = jnp.transpose(jnp.concatenate([top, top], axis=0))
    mass = jnp.transpose(jnp.concatenate([mass, mass], axis=0))
    peak = jnp.max(top, axis=0, keepdims=True)
    mass = jnp.sum(mass * jnp.exp(top - peak), axis=0, keepdims=True)
    me = col * 4 + row
    fst[me] = jnp.where(lane[:1] < rows, peak, mass)

    peers = [
        (c, lax.rem(row + dr, 4))
        for c in (3 - col, lax.rem(col + 2, 4), lax.rem(5 - col, 4), col) for dr in (2, 3, 1, 0)
    ][:-1]

    def stat_copy(k, slot):
        c, r = peers[k]
        return pltpu.make_async_remote_copy(
            src_ref=fst.at[slot], dst_ref=fst.at[slot], send_sem=fsend.at[k], recv_sem=frecv.at[slot],
            device_id={"col": c, "row": r}, device_id_type=MESH,
        )

    for k in range(15):
        stat_copy(k, me).start()
    for k in reversed(range(15)):
        c, r = peers[k]
        stat_copy(k, c * 4 + r).wait_recv()
    stats = fst[...]
    swapped = pltpu.roll(stats, LANES // 2, 2)
    peak = jnp.max(stats, axis=0)
    mass = jnp.sum(swapped * jnp.exp(stats - peak), axis=0)
    lse_ref[...] = peak + jnp.log(mass)

    for k in range(1, 4):
        norm_copy(k).wait_send()
    for src, dst, send, recv in ((qbuf, rin, qsend, rrecv), (pbuf, lin, psend, lrecv)):
        pltpu.make_async_remote_copy(
            src_ref=src, dst_ref=dst, send_sem=send, recv_sem=recv.at[0],
            device_id={"row": mate}, device_id_type=MESH,
        ).wait_send()
    for k in range(len(GROUPS)):
        each_across(k, lambda copy: copy.wait_send())

    @pl.when(core == 1)
    def _():
        edge_copy.wait_send()

    for k in range(15):
        stat_copy(k, me).wait_send()


def solution(mesh):
    def local_head(hidden, norm_gain, w_head):
        rows, feats = hidden.shape
        width = w_head.shape[1] // 4
        count = (width // LANES + 1) // TILES
        block = (count, rows, CHUNK)
        dma = pltpu.SemaphoreType.DMA

        def body(*refs):
            head_kernel(count, width, feats * 4, *refs)

        z, lse = pl.pallas_call(
            body,
            out_shape=(
                jax.ShapeDtypeStruct((rows, width), jnp.float32),
                jax.ShapeDtypeStruct((1, LANES), jnp.float32),
            ),
            in_specs=[
                pl.BlockSpec(memory_space=pltpu.HBM),
                pl.BlockSpec(memory_space=pltpu.HBM),
                pl.BlockSpec(memory_space=pltpu.HBM),
            ],
            out_specs=(pl.BlockSpec(memory_space=pltpu.VMEM), pl.BlockSpec(memory_space=pltpu.VMEM)),
            scratch_shapes=[
                pltpu.VMEM((rows, feats), hidden.dtype),
                pltpu.VMEM((feats,), jnp.float32),
                pltpu.VMEM((SLOTS, feats, CHUNK), jnp.bfloat16),
                pltpu.VMEM((SLOTS, feats, CHUNK), jnp.bfloat16),
                pltpu.VMEM((rows, feats), jnp.bfloat16),
                *[pltpu.VMEM(block, jnp.float32) for _ in range(7)],
                pltpu.VMEM((4, 1, LANES), jnp.float32),
                pltpu.VMEM((16, 1, LANES), jnp.float32),
                *[pltpu.VMEM((rows, LANES), jnp.float32) for _ in range(5)],
                dma, dma, pltpu.SemaphoreType.REGULAR((3,)),
                dma((SLOTS,)), dma((SLOTS,)), dma((4,)), dma((4,)),
                dma, dma, dma((len(GROUPS),)), dma((count,)), dma((count,)), dma((len(GROUPS),)), dma((16,)), dma((16,)), dma, dma,
            ],
            compiler_params=pltpu.CompilerParams(
                collective_id=0, has_side_effects=True, vmem_limit_bytes=48 * 1024 * 1024
            ),
            name="head",
        )(pltpu.with_memory_space_constraint(hidden, pltpu.HBM), pltpu.with_memory_space_constraint(norm_gain, pltpu.HBM), w_head)
        log_norm = lse[0, :rows]
        return z - log_norm[:, None], log_norm

    return jax.shard_map(
        local_head,
        mesh=mesh,
        in_specs=(P("dp", "row"), P("row"), P("row", "col")),
        out_specs=(P("dp", ("col", "row")), P("dp")),
        check_vma=False,
    )
```

```python
import jax
import jax.numpy as jnp
from jax import lax
from jax.experimental import pallas as pl
from jax.experimental.pallas import tpu as pltpu
from jax.sharding import PartitionSpec as P

EPS = 1e-5
MESH = pl.DeviceIdType.MESH
LANES = 128
TILES = 3
CHUNK = TILES * LANES
EARLY = 2
GROUPS = (1, 1, 2, 4, 6, 6, 3, 1)
RELAY_AT = 10
SLOTS = 4


def head_kernel(
    count, width, hidden_size,
    h_hbm, g_hbm, w_ref, z_ref, lse_ref,
    h_ref, g_ref, wa, wb, x_ref, qbuf, rbuf, pbuf, lbuf, rin, lin, yin, nst, fst, m_ref, s_ref, carry, edge_out, edge_in, relay_in, relay_mid,
    h_sem, g_sem, hops, wa_sem, wb_sem, nsend, nrecv, qsend, psend, ysend, rrecv, lrecv, yrecv, fsend, frecv, esend, erecv, tail_send, tail_recv, relay_send, relay_recv,
):
    rows, feats = h_ref.shape
    stride = (width // LANES) * LANES
    rest = width - stride
    col = lax.axis_index("col")
    row = lax.axis_index("row")
    core = lax.rem(row, 2)
    mate = row + 1 - 2 * core
    across = lax.rem(row + 2, 4)
    far = 3 - row
    shift = row * rest

    end = count - 1

    def chunk_at(t):
        if isinstance(t, int) and t < 2:
            return t * end
        return t - 1 - end * (t // count)

    def fetch(stream, t):
        if stream == 0:
            first, second, buf, sem = far, mate, wa, wa_sem
        else:
            first, second, buf, sem = across, row, wb, wb_sem
        part = first + (second - first) * (t // count)
        start = pl.multiple_of(stride * part + CHUNK * chunk_at(t), LANES)
        slot = lax.rem(t, SLOTS)
        return pltpu.make_async_copy(w_ref.at[:, pl.ds(start, CHUNK)], buf.at[slot], sem.at[slot])

    barrier = pltpu.get_barrier_semaphore()

    def tell_columns(sem):
        for step, there in ((-1, col > 0), (1, col < 3)):
            @pl.when(there)
            def _():
                pl.semaphore_signal(sem, inc=1, device_id_type=MESH, device_id={"col": col + step})

    for k in (2, 3, 1):
        pl.semaphore_signal(barrier, inc=1, device_id_type=MESH, device_id={"row": lax.rem(row + k, 4)})
    tell_columns(barrier)
    beside = (col + 2) // 3 + (5 - col) // 3

    h_copy = pltpu.make_async_copy(h_hbm, h_ref, h_sem)
    g_copy = pltpu.make_async_copy(g_hbm, g_ref, g_sem)
    h_copy.start()
    g_copy.start()
    h_copy.wait()
    for t in range(EARLY):
        fetch(0, t).start()
        fetch(1, t).start()

    lane = lax.broadcasted_iota(jnp.int32, (rows, LANES), 1)
    sq = jnp.zeros((rows, LANES), jnp.float32)
    for j in range(feats // LANES):
        part = h_ref[:, j * LANES:(j + 1) * LANES].astype(jnp.float32)
        sq = sq + part * part
    sq = jnp.transpose(jnp.concatenate([sq, sq], axis=0))
    nst[row] = jnp.sum(sq, axis=0, keepdims=True)
    pl.semaphore_wait(barrier, 3 + beside)
    tell_columns(hops.at[0])

    def norm_copy(k):
        return pltpu.make_async_remote_copy(
            src_ref=nst.at[row], dst_ref=nst.at[row], send_sem=nsend.at[k], recv_sem=nrecv.at[row],
            device_id={"row": lax.rem(row + k, 4)}, device_id_type=MESH,
        )

    for k in (2, 3, 1):
        norm_copy(k).start()
    for t in range(EARLY, SLOTS):
        fetch(0, t).start()
        fetch(1, t).start()
    for k in range(1, 4):
        peer = lax.rem(row + k, 4)
        pltpu.make_async_remote_copy(
            src_ref=nst.at[peer], dst_ref=nst.at[peer], send_sem=nsend.at[k], recv_sem=nrecv.at[peer],
            device_id={"row": peer}, device_id_type=MESH,
        ).wait_recv()
    g_copy.wait()
    total = nst[0] + nst[1] + nst[2] + nst[3]
    scale = lax.rsqrt(total / hidden_size + EPS)
    scale = jnp.transpose(jnp.broadcast_to(scale, (LANES, LANES)))[:rows]
    for j in range(feats // LANES):
        cols = slice(j * LANES, (j + 1) * LANES)
        x_ref[:, cols] = (h_ref[:, cols].astype(jnp.float32) * scale * g_ref[cols].reshape(1, LANES)).astype(jnp.bfloat16)

    def product(stream, t):
        buf, sem = ((wa, wa_sem), (wb, wb_sem))[stream]
        fetch(stream, t).wait()
        slot = lax.rem(t, SLOTS)
        return jnp.dot(x_ref[...], buf[slot], preferred_element_type=jnp.float32)

    def refill(stream, t):
        @pl.when(t + SLOTS < 2 * count)
        def _():
            fetch(stream, t + SLOTS).start()

    def mate_copy(src, dst, send, recv, i):
        return pltpu.make_async_remote_copy(
            src_ref=src.at[i], dst_ref=dst.at[i], send_sem=send, recv_sem=recv.at[i],
            device_id={"row": mate}, device_id_type=MESH,
        )

    starts = [sum(GROUPS[:k]) for k in range(len(GROUPS))]

    def across_copy(k):
        part = pl.ds(starts[k], GROUPS[k])
        return pltpu.make_async_remote_copy(
            src_ref=rbuf.at[part], dst_ref=yin.at[part], send_sem=ysend.at[k], recv_sem=yrecv.at[k],
            device_id={"row": across}, device_id_type=MESH,
        )

    most = pl.ds(0, (TILES - 1) * LANES)

    def tail_copy(lanes):
        return pltpu.make_async_remote_copy(
            src_ref=rbuf.at[end, :, lanes], dst_ref=yin.at[end, :, lanes], send_sem=tail_send, recv_sem=tail_recv,
            device_id={"row": across}, device_id_type=MESH,
        )

    def each_tail(act):
        @pl.when((col < 3) & (core == 0))
        def _():
            act(tail_copy(most))

        @pl.when((col < 3) & (core == 1))
        def _():
            act(tail_copy(pl.ds(0, CHUNK)))

        @pl.when((col == 3) & (core == 1))
        def _():
            act(tail_copy(pl.ds((TILES - 1) * LANES, LANES)))

    def relay_copy(k):
        src, dst, device = (
            (rbuf.at[end, :, most], relay_in, {"col": 0}),
            (relay_in, relay_mid, {"row": across}),
            (relay_mid, yin.at[end, :, most], {"col": 3}),
        )[k]
        return pltpu.make_async_remote_copy(
            src_ref=src, dst_ref=dst, send_sem=relay_send.at[k], recv_sem=relay_recv.at[k],
            device_id=device, device_id_type=MESH,
        )

    edge_copy = pltpu.make_async_remote_copy(
        src_ref=edge_out, dst_ref=edge_in, send_sem=esend, recv_sem=erecv,
        device_id={"row": mate}, device_id_type=MESH,
    )

    def far_step(t, i):
        qbuf[i] = product(0, t)
        mate_copy(qbuf, rin, qsend, rrecv, i).start()
        refill(0, t)

    def across_step(t, i):
        term = product(1, t)
        refill(1, t)
        mate_copy(qbuf, rin, qsend, rrecv, i).wait_recv()
        rbuf[i] = term + rin[i]

    pl.semaphore_wait(hops.at[0], beside)
    tell_columns(hops.at[1])
    far_step(0, 0)
    far_step(1, end)
    across_step(0, 0)
    across_copy(0).start()
    far_step(2, 1)
    across_step(1, end)
    pl.semaphore_wait(hops.at[1], beside)
    tell_columns(hops.at[2])
    each_tail(lambda copy: copy.start())

    @pl.when(col == 3)
    def _():
        relay_copy(0).start()

    @pl.loop(2, count)
    def _(t):
        @pl.when(t < end)
        def _():
            far_step(t + 1, t)

        across_step(t, t - 1)
        for k in range(1, len(GROUPS)):
            @pl.when(t == starts[k] + GROUPS[k])
            def _():
                across_copy(k).start()

        @pl.when((t == RELAY_AT) & (col == 0))
        def _():
            relay_copy(0).wait_recv()
            relay_copy(1).start()

    @pl.loop(0, count)
    def _(i):
        pbuf[i] = product(0, count + i)
        mate_copy(pbuf, lin, psend, lrecv, i).start()
        refill(0, count + i)
        lbuf[i] = product(1, count + i)
        refill(1, count + i)

    @pl.when(col == 0)
    def _():
        relay_copy(1).wait_recv()
        relay_copy(2).start()

    turn = lax.rem(LANES - shift, LANES)
    keep = lane < LANES - shift

    def arrive(i, first, last):
        mate_copy(pbuf, lin, psend, lrecv, i).wait_recv()
        if first:
            across_copy(0).wait_recv()
        elif last:
            each_tail(lambda copy: copy.wait_recv())

            @pl.when(col == 3)
            def _():
                relay_copy(2).wait_recv()
        else:
            for k in range(1, len(GROUPS)):
                @pl.when(i == starts[k])
                def _():
                    across_copy(k).wait_recv()
        full = lbuf[i] + lin[i] + yin[i]
        parts = [full[:, k * LANES:(k + 1) * LANES] for k in range(TILES)]
        if first:
            edge_out[...] = parts[0]

            @pl.when(core == 1)
            def _():
                edge_copy.start()
        if last:
            @pl.when(core == 0)
            def _():
                edge_copy.wait_recv()

            parts[-1] = jnp.where(core == 0, edge_in[...], parts[-1])
        rolled = [pltpu.roll(part, turn, 1) for part in parts]
        tiles = [jnp.where(keep, rolled[k], rolled[k + 1]) for k in range(TILES - 1)]
        at = 0
        if not first:
            tiles = [jnp.where(keep, carry[...], rolled[0])] + tiles
            at = pl.multiple_of(i * CHUNK - LANES, LANES)
        carry[...] = rolled[-1]
        z_ref[:, pl.ds(at, LANES * len(tiles))] = jnp.concatenate(tiles, axis=1)
        top = tiles[0]
        for tile in tiles[1:]:
            top = jnp.maximum(top, tile)
        if not first:
            top = jnp.maximum(top, m_ref[...])
        mass = jnp.exp(tiles[0] - top)
        for tile in tiles[1:]:
            mass = mass + jnp.exp(tile - top)
        if not first:
            mass = mass + s_ref[...] * jnp.exp(m_ref[...] - top)
        m_ref[...] = top
        s_ref[...] = mass

    arrive(0, True, False)
    pl.semaphore_wait(hops.at[2], beside)

    @pl.loop(1, count - 1)
    def _(i):
        arrive(i, False, False)

    arrive(count - 1, False, True)

    last = carry[...]
    z_ref[:, stride:] = last[:, :rest]
    last = jnp.where(lane < rest, last, -jnp.inf)
    top = jnp.maximum(m_ref[...], last)
    mass = s_ref[...] * jnp.exp(m_ref[...] - top) + jnp.exp(last - top)
    top = jnp.transpose(jnp.concatenate([top, top], axis=0))
    mass = jnp.transpose(jnp.concatenate([mass, mass], axis=0))
    peak = jnp.max(top, axis=0, keepdims=True)
    mass = jnp.sum(mass * jnp.exp(top - peak), axis=0, keepdims=True)
    me = col * 4 + row
    fst[me] = jnp.where(lane[:1] < rows, peak, mass)

    peers = [
        (c, lax.rem(row + dr, 4))
        for c in (3 - col, lax.rem(col + 2, 4), lax.rem(5 - col, 4), col) for dr in (2, 3, 1, 0)
    ][:-1]

    def stat_copy(k, slot):
        c, r = peers[k]
        return pltpu.make_async_remote_copy(
            src_ref=fst.at[slot], dst_ref=fst.at[slot], send_sem=fsend.at[k], recv_sem=frecv.at[slot],
            device_id={"col": c, "row": r}, device_id_type=MESH,
        )

    for k in range(15):
        stat_copy(k, me).start()
    for k in reversed(range(15)):
        c, r = peers[k]
        stat_copy(k, c * 4 + r).wait_recv()
    stats = fst[...]
    swapped = pltpu.roll(stats, LANES // 2, 2)
    peak = jnp.max(stats, axis=0)
    mass = jnp.sum(swapped * jnp.exp(stats - peak), axis=0)
    lse_ref[...] = peak + jnp.log(mass)

    for k in range(1, 4):
        norm_copy(k).wait_send()
    for src, dst, send, recv in ((qbuf, rin, qsend, rrecv), (pbuf, lin, psend, lrecv)):
        pltpu.make_async_remote_copy(
            src_ref=src, dst_ref=dst, send_sem=send, recv_sem=recv.at[0],
            device_id={"row": mate}, device_id_type=MESH,
        ).wait_send()
    for k in range(len(GROUPS)):
        across_copy(k).wait_send()
    each_tail(lambda copy: copy.wait_send())

    @pl.when(col == 3)
    def _():
        relay_copy(0).wait_send()

    @pl.when(col == 0)
    def _():
        relay_copy(1).wait_send()
        relay_copy(2).wait_send()

    @pl.when(core == 1)
    def _():
        edge_copy.wait_send()

    for k in range(15):
        stat_copy(k, me).wait_send()


def solution(mesh):
    def local_head(hidden, norm_gain, w_head):
        rows, feats = hidden.shape
        width = w_head.shape[1] // 4
        count = (width // LANES + 1) // TILES
        block = (count, rows, CHUNK)
        dma = pltpu.SemaphoreType.DMA

        def body(*refs):
            head_kernel(count, width, feats * 4, *refs)

        z, lse = pl.pallas_call(
            body,
            out_shape=(
                jax.ShapeDtypeStruct((rows, width), jnp.float32),
                jax.ShapeDtypeStruct((1, LANES), jnp.float32),
            ),
            in_specs=[
                pl.BlockSpec(memory_space=pltpu.HBM),
                pl.BlockSpec(memory_space=pltpu.HBM),
                pl.BlockSpec(memory_space=pltpu.HBM),
            ],
            out_specs=(pl.BlockSpec(memory_space=pltpu.VMEM), pl.BlockSpec(memory_space=pltpu.VMEM)),
            scratch_shapes=[
                pltpu.VMEM((rows, feats), hidden.dtype),
                pltpu.VMEM((feats,), jnp.float32),
                pltpu.VMEM((SLOTS, feats, CHUNK), jnp.bfloat16),
                pltpu.VMEM((SLOTS, feats, CHUNK), jnp.bfloat16),
                pltpu.VMEM((rows, feats), jnp.bfloat16),
                *[pltpu.VMEM(block, jnp.float32) for _ in range(7)],
                pltpu.VMEM((4, 1, LANES), jnp.float32),
                pltpu.VMEM((16, 1, LANES), jnp.float32),
                *[pltpu.VMEM((rows, LANES), jnp.float32) for _ in range(5)],
                *[pltpu.VMEM((rows, (TILES - 1) * LANES), jnp.float32) for _ in range(2)],
                dma, dma, pltpu.SemaphoreType.REGULAR((3,)),
                dma((SLOTS,)), dma((SLOTS,)), dma((4,)), dma((4,)),
                dma, dma, dma((len(GROUPS),)), dma((count,)), dma((count,)), dma((len(GROUPS),)), dma((16,)), dma((16,)), dma, dma, dma, dma, dma((3,)), dma((3,)),
            ],
            compiler_params=pltpu.CompilerParams(
                collective_id=0, has_side_effects=True, vmem_limit_bytes=48 * 1024 * 1024
            ),
            name="head",
        )(pltpu.with_memory_space_constraint(hidden, pltpu.HBM), pltpu.with_memory_space_constraint(norm_gain, pltpu.HBM), w_head)
        log_norm = lse[0, :rows]
        return z - log_norm[:, None], log_norm

    return jax.shard_map(
        local_head,
        mesh=mesh,
        in_specs=(P("dp", "row"), P("row"), P("row", "col")),
        out_specs=(P("dp", ("col", "row")), P("dp")),
        check_vma=False,
    )
```

```python
import jax
import jax.numpy as jnp
from jax import lax
from jax.experimental import pallas as pl
from jax.experimental.pallas import tpu as pltpu
from jax.sharding import PartitionSpec as P

EPS = 1e-5
MESH = pl.DeviceIdType.MESH
LANES = 128
TILES = 3
CHUNK = TILES * LANES
EARLY = 2
GROUPS = (1, 1, 1, 1, 2, 3, 4, 5, 4, 1, 1)
RELAY_AT = (16, 18)
SLOTS = 6


def head_kernel(
    count, width, hidden_size,
    h_hbm, g_hbm, w_ref, z_ref, lse_ref,
    h_ref, g_ref, wa, wb, x_ref, qbuf, rbuf, pbuf, lbuf, rin, lin, yin, nst, fst, m_ref, s_ref, carry, edge_out, edge_in, relay_in, relay_mid,
    h_sem, g_sem, hops, wa_sem, wb_sem, nsend, nrecv, qsend, psend, ysend, rrecv, lrecv, yrecv, fsend, frecv, esend, erecv, tail_send, tail_recv, relay_send, relay_recv,
):
    rows, feats = h_ref.shape
    stride = (width // LANES) * LANES
    rest = width - stride
    col = lax.axis_index("col")
    row = lax.axis_index("row")
    core = lax.rem(row, 2)
    mate = row + 1 - 2 * core
    across = lax.rem(row + 2, 4)
    far = 3 - row
    shift = row * rest

    end = count - 1

    def chunk_at(t):
        if isinstance(t, int) and t < 2:
            return t * end
        return t - 1 - end * (t // count)

    def fetch(stream, t):
        if stream == 0:
            first, second, buf, sem = far, mate, wa, wa_sem
        else:
            first, second, buf, sem = across, row, wb, wb_sem
        part = first + (second - first) * (t // count)
        start = pl.multiple_of(stride * part + CHUNK * chunk_at(t), LANES)
        slot = lax.rem(t, SLOTS)
        return pltpu.make_async_copy(w_ref.at[:, pl.ds(start, CHUNK)], buf.at[slot], sem.at[slot])

    barrier = pltpu.get_barrier_semaphore()

    def tell_columns(sem):
        for step, there in ((-1, col > 0), (1, col < 3)):
            @pl.when(there)
            def _():
                pl.semaphore_signal(sem, inc=1, device_id_type=MESH, device_id={"col": col + step})

    for k in (2, 3, 1):
        pl.semaphore_signal(barrier, inc=1, device_id_type=MESH, device_id={"row": lax.rem(row + k, 4)})
    tell_columns(barrier)
    beside = (col + 2) // 3 + (5 - col) // 3

    h_copy = pltpu.make_async_copy(h_hbm, h_ref, h_sem)
    g_copy = pltpu.make_async_copy(g_hbm, g_ref, g_sem)
    h_copy.start()
    g_copy.start()
    h_copy.wait()
    for t in range(EARLY):
        fetch(0, t).start()
        fetch(1, t).start()

    lane = lax.broadcasted_iota(jnp.int32, (rows, LANES), 1)
    sq = jnp.zeros((rows, LANES), jnp.float32)
    for j in range(feats // LANES):
        part = h_ref[:, j * LANES:(j + 1) * LANES].astype(jnp.float32)
        sq = sq + part * part
    sq = jnp.transpose(jnp.concatenate([sq, sq], axis=0))
    nst[row] = jnp.sum(sq, axis=0, keepdims=True)
    pl.semaphore_wait(barrier, 3 + beside)
    tell_columns(hops.at[0])

    def norm_copy(k):
        return pltpu.make_async_remote_copy(
            src_ref=nst.at[row], dst_ref=nst.at[row], send_sem=nsend.at[k], recv_sem=nrecv.at[row],
            device_id={"row": lax.rem(row + k, 4)}, device_id_type=MESH,
        )

    for k in (2, 3, 1):
        norm_copy(k).start()
    for t in range(EARLY, SLOTS):
        fetch(0, t).start()
        fetch(1, t).start()
    for k in range(1, 4):
        peer = lax.rem(row + k, 4)
        pltpu.make_async_remote_copy(
            src_ref=nst.at[peer], dst_ref=nst.at[peer], send_sem=nsend.at[k], recv_sem=nrecv.at[peer],
            device_id={"row": peer}, device_id_type=MESH,
        ).wait_recv()
    g_copy.wait()
    total = nst[0] + nst[1] + nst[2] + nst[3]
    scale = lax.rsqrt(total / hidden_size + EPS)
    scale = jnp.transpose(jnp.broadcast_to(scale, (LANES, LANES)))[:rows]
    for j in range(feats // LANES):
        cols = slice(j * LANES, (j + 1) * LANES)
        x_ref[:, cols] = (h_ref[:, cols].astype(jnp.float32) * scale * g_ref[cols].reshape(1, LANES)).astype(jnp.bfloat16)

    def product(stream, t):
        buf, sem = ((wa, wa_sem), (wb, wb_sem))[stream]
        fetch(stream, t).wait()
        slot = lax.rem(t, SLOTS)
        return jnp.dot(x_ref[...], buf[slot], preferred_element_type=jnp.float32)

    def refill(stream, t):
        @pl.when(t + SLOTS < 2 * count)
        def _():
            fetch(stream, t + SLOTS).start()

    def mate_copy(src, dst, send, recv, i):
        return pltpu.make_async_remote_copy(
            src_ref=src.at[i], dst_ref=dst.at[i], send_sem=send, recv_sem=recv.at[i],
            device_id={"row": mate}, device_id_type=MESH,
        )

    starts = [sum(GROUPS[:k]) for k in range(len(GROUPS))]

    def across_copy(k):
        part = pl.ds(starts[k], GROUPS[k])
        return pltpu.make_async_remote_copy(
            src_ref=rbuf.at[part], dst_ref=yin.at[part], send_sem=ysend.at[k], recv_sem=yrecv.at[k],
            device_id={"row": across}, device_id_type=MESH,
        )

    most = pl.ds(0, (TILES - 1) * LANES)

    def tail_copy(lanes):
        return pltpu.make_async_remote_copy(
            src_ref=rbuf.at[end, :, lanes], dst_ref=yin.at[end, :, lanes], send_sem=tail_send, recv_sem=tail_recv,
            device_id={"row": across}, device_id_type=MESH,
        )

    def each_tail(act):
        @pl.when((col < 3) & (core == 0))
        def _():
            act(tail_copy(most))

        @pl.when((col < 3) & (core == 1))
        def _():
            act(tail_copy(pl.ds(0, CHUNK)))

        @pl.when((col == 3) & (core == 1))
        def _():
            act(tail_copy(pl.ds((TILES - 1) * LANES, LANES)))

    def relay_copy(k):
        src, dst, device = (
            (rbuf.at[end, :, most], relay_in, {"col": 0}),
            (relay_in, relay_mid, {"row": across}),
            (relay_mid, yin.at[end, :, most], {"col": 3}),
        )[k]
        return pltpu.make_async_remote_copy(
            src_ref=src, dst_ref=dst, send_sem=relay_send.at[k], recv_sem=relay_recv.at[k],
            device_id=device, device_id_type=MESH,
        )

    edge_copy = pltpu.make_async_remote_copy(
        src_ref=edge_out, dst_ref=edge_in, send_sem=esend, recv_sem=erecv,
        device_id={"row": mate}, device_id_type=MESH,
    )

    def far_step(t, i):
        qbuf[i] = product(0, t)
        mate_copy(qbuf, rin, qsend, rrecv, i).start()
        refill(0, t)

    def across_step(t, i):
        term = product(1, t)
        refill(1, t)
        mate_copy(qbuf, rin, qsend, rrecv, i).wait_recv()
        rbuf[i] = term + rin[i]

    pl.semaphore_wait(hops.at[0], beside)
    tell_columns(hops.at[1])
    far_step(0, 0)
    far_step(1, end)
    across_step(0, 0)
    across_copy(0).start()
    far_step(2, 1)
    far_step(3, 2)
    across_step(1, end)
    pl.semaphore_wait(hops.at[1], beside)
    tell_columns(hops.at[2])
    each_tail(lambda copy: copy.start())

    @pl.when(col == 3)
    def _():
        relay_copy(0).start()

    @pl.loop(2, count)
    def _(t):
        @pl.when(t < end - 1)
        def _():
            far_step(t + 2, t + 1)

        across_step(t, t - 1)
        for k in range(1, len(GROUPS)):
            @pl.when(t == starts[k] + GROUPS[k])
            def _():
                across_copy(k).start()

        @pl.when((t == RELAY_AT[0]) & (col == 0))
        def _():
            relay_copy(0).wait_recv()
            relay_copy(1).start()

    @pl.loop(0, count)
    def _(i):
        pbuf[i] = product(0, count + i)
        mate_copy(pbuf, lin, psend, lrecv, i).start()
        refill(0, count + i)
        lbuf[i] = product(1, count + i)
        refill(1, count + i)

    turn = lax.rem(LANES - shift, LANES)
    keep = lane < LANES - shift

    def arrive(i, first, last):
        mate_copy(pbuf, lin, psend, lrecv, i).wait_recv()
        if first:
            across_copy(0).wait_recv()
        elif last:
            each_tail(lambda copy: copy.wait_recv())

            @pl.when(col == 3)
            def _():
                relay_copy(2).wait_recv()
        else:
            for k in range(1, len(GROUPS)):
                @pl.when(i == starts[k])
                def _():
                    across_copy(k).wait_recv()
        full = lbuf[i] + lin[i] + yin[i]
        parts = [full[:, k * LANES:(k + 1) * LANES] for k in range(TILES)]
        if first:
            edge_out[...] = parts[0]

            @pl.when(core == 1)
            def _():
                edge_copy.start()
        if last:
            @pl.when(core == 0)
            def _():
                edge_copy.wait_recv()

            parts[-1] = jnp.where(core == 0, edge_in[...], parts[-1])
        rolled = [pltpu.roll(part, turn, 1) for part in parts]
        tiles = [jnp.where(keep, rolled[k], rolled[k + 1]) for k in range(TILES - 1)]
        at = 0
        if not first:
            tiles = [jnp.where(keep, carry[...], rolled[0])] + tiles
            at = pl.multiple_of(i * CHUNK - LANES, LANES)
        carry[...] = rolled[-1]
        z_ref[:, pl.ds(at, LANES * len(tiles))] = jnp.concatenate(tiles, axis=1)
        top = tiles[0]
        for tile in tiles[1:]:
            top = jnp.maximum(top, tile)
        if not first:
            top = jnp.maximum(top, m_ref[...])
        mass = jnp.exp(tiles[0] - top)
        for tile in tiles[1:]:
            mass = mass + jnp.exp(tile - top)
        if not first:
            mass = mass + s_ref[...] * jnp.exp(m_ref[...] - top)
        m_ref[...] = top
        s_ref[...] = mass

    arrive(0, True, False)
    pl.semaphore_wait(hops.at[2], beside)

    @pl.loop(1, count - 1)
    def _(i):
        arrive(i, False, False)

        @pl.when((i == RELAY_AT[1]) & (col == 0))
        def _():
            relay_copy(1).wait_recv()
            relay_copy(2).start()

    arrive(count - 1, False, True)

    last = carry[...]
    z_ref[:, stride:] = last[:, :rest]
    last = jnp.where(lane < rest, last, -jnp.inf)
    top = jnp.maximum(m_ref[...], last)
    mass = s_ref[...] * jnp.exp(m_ref[...] - top) + jnp.exp(last - top)
    top = jnp.transpose(jnp.concatenate([top, top], axis=0))
    mass = jnp.transpose(jnp.concatenate([mass, mass], axis=0))
    peak = jnp.max(top, axis=0, keepdims=True)
    mass = jnp.sum(mass * jnp.exp(top - peak), axis=0, keepdims=True)
    me = col * 4 + row
    fst[me] = jnp.where(lane[:1] < rows, peak, mass)

    peers = [
        (c, lax.rem(row + dr, 4))
        for c in (3 - col, lax.rem(col + 2, 4), lax.rem(5 - col, 4), col) for dr in (2, 3, 1, 0)
    ][:-1]

    def stat_copy(k, slot):
        c, r = peers[k]
        return pltpu.make_async_remote_copy(
            src_ref=fst.at[slot], dst_ref=fst.at[slot], send_sem=fsend.at[k], recv_sem=frecv.at[slot],
            device_id={"col": c, "row": r}, device_id_type=MESH,
        )

    for k in range(15):
        stat_copy(k, me).start()
    for k in reversed(range(15)):
        c, r = peers[k]
        stat_copy(k, c * 4 + r).wait_recv()
    stats = fst[...]
    swapped = pltpu.roll(stats, LANES // 2, 2)
    peak = jnp.max(stats, axis=0)
    mass = jnp.sum(swapped * jnp.exp(stats - peak), axis=0)
    lse_ref[...] = peak + jnp.log(mass)

    for k in range(1, 4):
        norm_copy(k).wait_send()
    for src, dst, send, recv in ((qbuf, rin, qsend, rrecv), (pbuf, lin, psend, lrecv)):
        pltpu.make_async_remote_copy(
            src_ref=src, dst_ref=dst, send_sem=send, recv_sem=recv.at[0],
            device_id={"row": mate}, device_id_type=MESH,
        ).wait_send()
    for k in range(len(GROUPS)):
        across_copy(k).wait_send()
    each_tail(lambda copy: copy.wait_send())

    @pl.when(col == 3)
    def _():
        relay_copy(0).wait_send()

    @pl.when(col == 0)
    def _():
        relay_copy(1).wait_send()
        relay_copy(2).wait_send()

    @pl.when(core == 1)
    def _():
        edge_copy.wait_send()

    for k in range(15):
        stat_copy(k, me).wait_send()


def solution(mesh):
    def local_head(hidden, norm_gain, w_head):
        rows, feats = hidden.shape
        width = w_head.shape[1] // 4
        count = (width // LANES + 1) // TILES
        block = (count, rows, CHUNK)
        dma = pltpu.SemaphoreType.DMA

        def body(*refs):
            head_kernel(count, width, feats * 4, *refs)

        z, lse = pl.pallas_call(
            body,
            out_shape=(
                jax.ShapeDtypeStruct((rows, width), jnp.float32),
                jax.ShapeDtypeStruct((1, LANES), jnp.float32),
            ),
            in_specs=[
                pl.BlockSpec(memory_space=pltpu.HBM),
                pl.BlockSpec(memory_space=pltpu.HBM),
                pl.BlockSpec(memory_space=pltpu.HBM),
            ],
            out_specs=(pl.BlockSpec(memory_space=pltpu.VMEM), pl.BlockSpec(memory_space=pltpu.VMEM)),
            scratch_shapes=[
                pltpu.VMEM((rows, feats), hidden.dtype),
                pltpu.VMEM((feats,), jnp.float32),
                pltpu.VMEM((SLOTS, feats, CHUNK), jnp.bfloat16),
                pltpu.VMEM((SLOTS, feats, CHUNK), jnp.bfloat16),
                pltpu.VMEM((rows, feats), jnp.bfloat16),
                *[pltpu.VMEM(block, jnp.float32) for _ in range(7)],
                pltpu.VMEM((4, 1, LANES), jnp.float32),
                pltpu.VMEM((16, 1, LANES), jnp.float32),
                *[pltpu.VMEM((rows, LANES), jnp.float32) for _ in range(5)],
                *[pltpu.VMEM((rows, (TILES - 1) * LANES), jnp.float32) for _ in range(2)],
                dma, dma, pltpu.SemaphoreType.REGULAR((3,)),
                dma((SLOTS,)), dma((SLOTS,)), dma((4,)), dma((4,)),
                dma, dma, dma((len(GROUPS),)), dma((count,)), dma((count,)), dma((len(GROUPS),)), dma((16,)), dma((16,)), dma, dma, dma, dma, dma((3,)), dma((3,)),
            ],
            compiler_params=pltpu.CompilerParams(
                collective_id=0, has_side_effects=True, vmem_limit_bytes=48 * 1024 * 1024
            ),
            name="head",
        )(pltpu.with_memory_space_constraint(hidden, pltpu.HBM), pltpu.with_memory_space_constraint(norm_gain, pltpu.HBM), w_head)
        log_norm = lse[0, :rows]
        return z - log_norm[:, None], log_norm

    return jax.shard_map(
        local_head,
        mesh=mesh,
        in_specs=(P("dp", "row"), P("row"), P("row", "col")),
        out_specs=(P("dp", ("col", "row")), P("dp")),
        check_vma=False,
    )
```

```python
import jax
import jax.numpy as jnp
from jax import lax
from jax.experimental import pallas as pl
from jax.experimental.pallas import tpu as pltpu
from jax.sharding import PartitionSpec as P

EPS = 1e-5
MESH = pl.DeviceIdType.MESH
LANES = 128
TILES = 3
CHUNK = TILES * LANES
SLOTS = 3
RELAY_AT = (4, 10)


def head_kernel(
    count, width, hidden_size,
    h_hbm, g_hbm, w_ref, z_ref, lse_ref,
    h_ref, g_ref, wq, wr, wp, wl, x_ref, qbuf, rbuf, pbuf, lbuf, rin, lin, yin, nst, fst, m_ref, s_ref, carry, edge_out, edge_in, relay_in, relay_mid,
    h_sem, g_sem, hops, wq_sem, wr_sem, wp_sem, wl_sem, nsend, nrecv, qsend, psend, ysend, rrecv, lrecv, yrecv, fsend, frecv, esend, erecv, tail_send, tail_recv, relay_send, relay_recv,
):
    rows, feats = h_ref.shape
    stride = (width // LANES) * LANES
    rest = width - stride
    col = lax.axis_index("col")
    row = lax.axis_index("row")
    core = lax.rem(row, 2)
    mate = row + 1 - 2 * core
    across = lax.rem(row + 2, 4)
    far = 3 - row
    shift = row * rest

    end = count - 1

    streams = {
        "far": (far, wq, wq_sem), "across": (across, wr, wr_sem), "mate": (mate, wp, wp_sem), "own": (row, wl, wl_sem)
    }

    def fetch(name, t):
        part, buf, sem = streams[name]
        chunk = t
        if name in ("far", "across"):
            chunk = (0, end)[t] if isinstance(t, int) and t < 2 else t - 1
        start = pl.multiple_of(stride * part + CHUNK * chunk, LANES)
        slot = lax.rem(t, SLOTS)
        return pltpu.make_async_copy(w_ref.at[:, pl.ds(start, CHUNK)], buf.at[slot], sem.at[slot])

    barrier = pltpu.get_barrier_semaphore()

    def tell_columns(sem):
        for step, there in ((-1, col > 0), (1, col < 3)):
            @pl.when(there)
            def _():
                pl.semaphore_signal(sem, inc=1, device_id_type=MESH, device_id={"col": col + step})

    for k in (2, 3, 1):
        pl.semaphore_signal(barrier, inc=1, device_id_type=MESH, device_id={"row": lax.rem(row + k, 4)})
    tell_columns(barrier)
    beside = (col + 2) // 3 + (5 - col) // 3

    h_copy = pltpu.make_async_copy(h_hbm, h_ref, h_sem)
    g_copy = pltpu.make_async_copy(g_hbm, g_ref, g_sem)
    h_copy.start()
    g_copy.start()
    h_copy.wait()
    for name, t in (("far", 0), ("far", 1), ("across", 0)):
        fetch(name, t).start()

    lane = lax.broadcasted_iota(jnp.int32, (rows, LANES), 1)
    sq = jnp.zeros((rows, LANES), jnp.float32)
    for j in range(feats // LANES):
        part = h_ref[:, j * LANES:(j + 1) * LANES].astype(jnp.float32)
        sq = sq + part * part
    sq = jnp.transpose(jnp.concatenate([sq, sq], axis=0))
    nst[row] = jnp.sum(sq, axis=0, keepdims=True)
    pl.semaphore_wait(barrier, 3 + beside)
    tell_columns(hops.at[0])

    def norm_copy(k):
        return pltpu.make_async_remote_copy(
            src_ref=nst.at[row], dst_ref=nst.at[row], send_sem=nsend.at[k], recv_sem=nrecv.at[row],
            device_id={"row": lax.rem(row + k, 4)}, device_id_type=MESH,
        )

    for k in (2, 3, 1):
        norm_copy(k).start()
    for name, t in (("far", 2), ("across", 1), ("across", 2), *[(n, t) for t in range(SLOTS) for n in ("mate", "own")]):
        fetch(name, t).start()
    for k in range(1, 4):
        peer = lax.rem(row + k, 4)
        pltpu.make_async_remote_copy(
            src_ref=nst.at[peer], dst_ref=nst.at[peer], send_sem=nsend.at[k], recv_sem=nrecv.at[peer],
            device_id={"row": peer}, device_id_type=MESH,
        ).wait_recv()
    g_copy.wait()
    total = nst[0] + nst[1] + nst[2] + nst[3]
    scale = lax.rsqrt(total / hidden_size + EPS)
    scale = jnp.transpose(jnp.broadcast_to(scale, (LANES, LANES)))[:rows]
    for j in range(feats // LANES):
        cols = slice(j * LANES, (j + 1) * LANES)
        x_ref[:, cols] = (h_ref[:, cols].astype(jnp.float32) * scale * g_ref[cols].reshape(1, LANES)).astype(jnp.bfloat16)

    def product(name, t):
        fetch(name, t).wait()
        return jnp.dot(x_ref[...], streams[name][1][lax.rem(t, SLOTS)], preferred_element_type=jnp.float32)

    def refill(name, t):
        @pl.when(t + SLOTS < count)
        def _():
            fetch(name, t + SLOTS).start()

    def mate_copy(src, dst, send, recv, i):
        return pltpu.make_async_remote_copy(
            src_ref=src.at[i], dst_ref=dst.at[i], send_sem=send, recv_sem=recv.at[i],
            device_id={"row": mate}, device_id_type=MESH,
        )

    def across_copy(i):
        return pltpu.make_async_remote_copy(
            src_ref=rbuf.at[i], dst_ref=yin.at[i], send_sem=ysend.at[i], recv_sem=yrecv.at[i],
            device_id={"row": across}, device_id_type=MESH,
        )

    most = pl.ds(0, (TILES - 1) * LANES)

    def tail_copy(lanes):
        return pltpu.make_async_remote_copy(
            src_ref=rbuf.at[end, :, lanes], dst_ref=yin.at[end, :, lanes], send_sem=tail_send, recv_sem=tail_recv,
            device_id={"row": across}, device_id_type=MESH,
        )

    def each_tail(act):
        @pl.when((col < 3) & (core == 0))
        def _():
            act(tail_copy(most))

        @pl.when((col < 3) & (core == 1))
        def _():
            act(tail_copy(pl.ds(0, CHUNK)))

        @pl.when((col == 3) & (core == 1))
        def _():
            act(tail_copy(pl.ds((TILES - 1) * LANES, LANES)))

    def relay_copy(k):
        src, dst, device = (
            (rbuf.at[end, :, most], relay_in, {"col": 0}),
            (relay_in, relay_mid, {"row": across}),
            (relay_mid, yin.at[end, :, most], {"col": 3}),
        )[k]
        return pltpu.make_async_remote_copy(
            src_ref=src, dst_ref=dst, send_sem=relay_send.at[k], recv_sem=relay_recv.at[k],
            device_id=device, device_id_type=MESH,
        )

    edge_copy = pltpu.make_async_remote_copy(
        src_ref=edge_out, dst_ref=edge_in, send_sem=esend, recv_sem=erecv,
        device_id={"row": mate}, device_id_type=MESH,
    )

    def far_step(t, i):
        qbuf[i] = product("far", t)
        mate_copy(qbuf, rin, qsend, rrecv, i).start()
        refill("far", t)

    def across_step(t, i):
        term = product("across", t)
        refill("across", t)
        mate_copy(qbuf, rin, qsend, rrecv, i).wait_recv()
        rbuf[i] = term + rin[i]

    def mate_step(i):
        pbuf[i] = product("mate", i)
        mate_copy(pbuf, lin, psend, lrecv, i).start()
        refill("mate", i)

    def own_step(i):
        lbuf[i] = product("own", i)
        refill("own", i)

    turn = lax.rem(LANES - shift, LANES)
    keep = lane < LANES - shift

    def arrive(i, first, last):
        mate_copy(pbuf, lin, psend, lrecv, i).wait_recv()
        if last:
            each_tail(lambda copy: copy.wait_recv())

            @pl.when(col == 3)
            def _():
                relay_copy(2).wait_recv()
        else:
            across_copy(i).wait_recv()
        full = lbuf[i] + lin[i] + yin[i]
        parts = [full[:, k * LANES:(k + 1) * LANES] for k in range(TILES)]
        if first:
            edge_out[...] = parts[0]

            @pl.when(core == 1)
            def _():
                edge_copy.start()
        if last:
            @pl.when(core == 0)
            def _():
                edge_copy.wait_recv()

            parts[-1] = jnp.where(core == 0, edge_in[...], parts[-1])
        rolled = [pltpu.roll(part, turn, 1) for part in parts]
        tiles = [jnp.where(keep, rolled[k], rolled[k + 1]) for k in range(TILES - 1)]
        at = 0
        if not first:
            tiles = [jnp.where(keep, carry[...], rolled[0])] + tiles
            at = pl.multiple_of(i * CHUNK - LANES, LANES)
        carry[...] = rolled[-1]
        z_ref[:, pl.ds(at, LANES * len(tiles))] = jnp.concatenate(tiles, axis=1)
        top = tiles[0]
        for tile in tiles[1:]:
            top = jnp.maximum(top, tile)
        if not first:
            top = jnp.maximum(top, m_ref[...])
        mass = jnp.exp(tiles[0] - top)
        for tile in tiles[1:]:
            mass = mass + jnp.exp(tile - top)
        if not first:
            mass = mass + s_ref[...] * jnp.exp(m_ref[...] - top)
        m_ref[...] = top
        s_ref[...] = mass

    pl.semaphore_wait(hops.at[0], beside)
    tell_columns(hops.at[1])
    far_step(0, 0)
    far_step(1, end)
    across_step(0, 0)
    across_copy(0).start()
    far_step(2, 1)
    far_step(3, 2)
    across_step(1, end)
    pl.semaphore_wait(hops.at[1], beside)
    tell_columns(hops.at[2])
    each_tail(lambda copy: copy.start())

    @pl.when(col == 3)
    def _():
        relay_copy(0).start()

    across_step(2, 1)
    across_copy(1).start()
    mate_step(0)
    mate_step(1)
    own_step(0)
    arrive(0, True, False)

    @pl.loop(1, end)
    def _(i):
        @pl.when(i < end - 2)
        def _():
            far_step(i + 3, i + 2)

        @pl.when(i < end - 1)
        def _():
            across_step(i + 2, i + 1)
            across_copy(i + 1).start()

        mate_step(i + 1)
        own_step(i)
        arrive(i, False, False)

        @pl.when((i == RELAY_AT[0]) & (col == 0))
        def _():
            relay_copy(0).wait_recv()
            relay_copy(1).start()

        @pl.when((i == RELAY_AT[1]) & (col == 0))
        def _():
            relay_copy(1).wait_recv()
            relay_copy(2).start()

    pl.semaphore_wait(hops.at[2], beside)
    own_step(end)
    arrive(end, False, True)

    last = carry[...]
    z_ref[:, stride:] = last[:, :rest]
    last = jnp.where(lane < rest, last, -jnp.inf)
    top = jnp.maximum(m_ref[...], last)
    mass = s_ref[...] * jnp.exp(m_ref[...] - top) + jnp.exp(last - top)
    top = jnp.transpose(jnp.concatenate([top, top], axis=0))
    mass = jnp.transpose(jnp.concatenate([mass, mass], axis=0))
    peak = jnp.max(top, axis=0, keepdims=True)
    mass = jnp.sum(mass * jnp.exp(top - peak), axis=0, keepdims=True)
    me = col * 4 + row
    fst[me] = jnp.where(lane[:1] < rows, peak, mass)

    peers = [
        (c, lax.rem(row + dr, 4))
        for c in (3 - col, lax.rem(col + 2, 4), lax.rem(5 - col, 4), col) for dr in (2, 3, 1, 0)
    ][:-1]

    def stat_copy(k, slot):
        c, r = peers[k]
        return pltpu.make_async_remote_copy(
            src_ref=fst.at[slot], dst_ref=fst.at[slot], send_sem=fsend.at[k], recv_sem=frecv.at[slot],
            device_id={"col": c, "row": r}, device_id_type=MESH,
        )

    for k in range(15):
        stat_copy(k, me).start()
    for k in reversed(range(15)):
        c, r = peers[k]
        stat_copy(k, c * 4 + r).wait_recv()
    stats = fst[...]
    swapped = pltpu.roll(stats, LANES // 2, 2)
    peak = jnp.max(stats, axis=0)
    mass = jnp.sum(swapped * jnp.exp(stats - peak), axis=0)
    lse_ref[...] = peak + jnp.log(mass)

    for k in range(1, 4):
        norm_copy(k).wait_send()
    for src, dst, send, recv in ((qbuf, rin, qsend, rrecv), (pbuf, lin, psend, lrecv)):
        pltpu.make_async_remote_copy(
            src_ref=src, dst_ref=dst, send_sem=send, recv_sem=recv.at[0],
            device_id={"row": mate}, device_id_type=MESH,
        ).wait_send()
    @pl.loop(0, end)
    def _(i):
        across_copy(i).wait_send()

    each_tail(lambda copy: copy.wait_send())

    @pl.when(col == 3)
    def _():
        relay_copy(0).wait_send()

    @pl.when(col == 0)
    def _():
        relay_copy(1).wait_send()
        relay_copy(2).wait_send()

    @pl.when(core == 1)
    def _():
        edge_copy.wait_send()

    for k in range(15):
        stat_copy(k, me).wait_send()


def solution(mesh):
    def local_head(hidden, norm_gain, w_head):
        rows, feats = hidden.shape
        width = w_head.shape[1] // 4
        count = (width // LANES + 1) // TILES
        block = (count, rows, CHUNK)
        dma = pltpu.SemaphoreType.DMA

        def body(*refs):
            head_kernel(count, width, feats * 4, *refs)

        z, lse = pl.pallas_call(
            body,
            out_shape=(
                jax.ShapeDtypeStruct((rows, width), jnp.float32),
                jax.ShapeDtypeStruct((1, LANES), jnp.float32),
            ),
            in_specs=[
                pl.BlockSpec(memory_space=pltpu.HBM),
                pl.BlockSpec(memory_space=pltpu.HBM),
                pl.BlockSpec(memory_space=pltpu.HBM),
            ],
            out_specs=(pl.BlockSpec(memory_space=pltpu.VMEM), pl.BlockSpec(memory_space=pltpu.VMEM)),
            scratch_shapes=[
                pltpu.VMEM((rows, feats), hidden.dtype),
                pltpu.VMEM((feats,), jnp.float32),
                *[pltpu.VMEM((SLOTS, feats, CHUNK), jnp.bfloat16) for _ in range(4)],
                pltpu.VMEM((rows, feats), jnp.bfloat16),
                *[pltpu.VMEM(block, jnp.float32) for _ in range(7)],
                pltpu.VMEM((4, 1, LANES), jnp.float32),
                pltpu.VMEM((16, 1, LANES), jnp.float32),
                *[pltpu.VMEM((rows, LANES), jnp.float32) for _ in range(5)],
                *[pltpu.VMEM((rows, (TILES - 1) * LANES), jnp.float32) for _ in range(2)],
                dma, dma, pltpu.SemaphoreType.REGULAR((3,)),
                *[dma((SLOTS,)) for _ in range(4)], dma((4,)), dma((4,)),
                dma, dma, dma((count,)), dma((count,)), dma((count,)), dma((count,)), dma((16,)), dma((16,)), dma, dma, dma, dma, dma((3,)), dma((3,)),
            ],
            compiler_params=pltpu.CompilerParams(
                collective_id=0, has_side_effects=True, vmem_limit_bytes=48 * 1024 * 1024
            ),
            name="head",
        )(pltpu.with_memory_space_constraint(hidden, pltpu.HBM), pltpu.with_memory_space_constraint(norm_gain, pltpu.HBM), w_head)
        log_norm = lse[0, :rows]
        return z - log_norm[:, None], log_norm

    return jax.shard_map(
        local_head,
        mesh=mesh,
        in_specs=(P("dp", "row"), P("row"), P("row", "col")),
        out_specs=(P("dp", ("col", "row")), P("dp")),
        check_vma=False,
    )
```

```python
import jax
import jax.numpy as jnp
from jax import lax
from jax.experimental import pallas as pl
from jax.experimental.pallas import tpu as pltpu
from jax.sharding import PartitionSpec as P

EPS = 1e-5
MESH = pl.DeviceIdType.MESH
LANES = 128
TILES = 3
CHUNK = TILES * LANES
AHEAD = 3
SLOTS = 3
RELAY_AT = (4, 10)


def head_kernel(
    count, width, hidden_size,
    h_hbm, g_hbm, w_ref, z_ref, lse_ref,
    h_ref, g_ref, wq, wr, wp, wl, x_ref, qbuf, rbuf, pbuf, lbuf, rin, lin, yin, nst, fst, m_ref, s_ref, carry, edge_out, edge_in, relay_in, relay_mid,
    h_sem, g_sem, hops, wq_sem, wr_sem, wp_sem, wl_sem, nsend, nrecv, qsend, psend, ysend, rrecv, lrecv, yrecv, fsend, frecv, esend, erecv, tail_send, tail_recv, relay_send, relay_recv,
):
    rows, feats = h_ref.shape
    stride = (width // LANES) * LANES
    rest = width - stride
    col = lax.axis_index("col")
    row = lax.axis_index("row")
    core = lax.rem(row, 2)
    mate = row + 1 - 2 * core
    across = lax.rem(row + 2, 4)
    far = 3 - row
    shift = row * rest

    end = count - 1

    streams = {
        "far": (far, wq, wq_sem), "across": (across, wr, wr_sem), "mate": (mate, wp, wp_sem), "own": (row, wl, wl_sem)
    }

    def fetch(name, t):
        part, buf, sem = streams[name]
        chunk = t
        if name in ("far", "across"):
            chunk = (0, end)[t] if isinstance(t, int) and t < 2 else t - 1
        start = pl.multiple_of(stride * part + CHUNK * chunk, LANES)
        slot = lax.rem(t, SLOTS)
        return pltpu.make_async_copy(w_ref.at[:, pl.ds(start, CHUNK)], buf.at[slot], sem.at[slot])

    barrier = pltpu.get_barrier_semaphore()

    def tell_columns(sem):
        for step, there in ((-1, col > 0), (1, col < 3)):
            @pl.when(there)
            def _():
                pl.semaphore_signal(sem, inc=1, device_id_type=MESH, device_id={"col": col + step})

    for k in (2, 3, 1):
        pl.semaphore_signal(barrier, inc=1, device_id_type=MESH, device_id={"row": lax.rem(row + k, 4)})
    tell_columns(barrier)
    beside = (col + 2) // 3 + (5 - col) // 3

    h_copy = pltpu.make_async_copy(h_hbm, h_ref, h_sem)
    g_copy = pltpu.make_async_copy(g_hbm, g_ref, g_sem)
    h_copy.start()
    g_copy.start()
    h_copy.wait()
    for name, t in (("far", 0), ("far", 1), ("across", 0)):
        fetch(name, t).start()

    lane = lax.broadcasted_iota(jnp.int32, (rows, LANES), 1)
    sq = jnp.zeros((rows, LANES), jnp.float32)
    for j in range(feats // LANES):
        part = h_ref[:, j * LANES:(j + 1) * LANES].astype(jnp.float32)
        sq = sq + part * part
    sq = jnp.transpose(jnp.concatenate([sq, sq], axis=0))
    nst[row] = jnp.sum(sq, axis=0, keepdims=True)
    pl.semaphore_wait(barrier, 3 + beside)
    tell_columns(hops.at[0])

    def norm_copy(k):
        return pltpu.make_async_remote_copy(
            src_ref=nst.at[row], dst_ref=nst.at[row], send_sem=nsend.at[k], recv_sem=nrecv.at[row],
            device_id={"row": lax.rem(row + k, 4)}, device_id_type=MESH,
        )

    for k in (2, 3, 1):
        norm_copy(k).start()
    for name, t in (("far", 2), ("across", 1), ("across", 2), *[(n, t) for t in range(SLOTS) for n in ("mate", "own")]):
        fetch(name, t).start()
    for k in range(1, 4):
        peer = lax.rem(row + k, 4)
        pltpu.make_async_remote_copy(
            src_ref=nst.at[peer], dst_ref=nst.at[peer], send_sem=nsend.at[k], recv_sem=nrecv.at[peer],
            device_id={"row": peer}, device_id_type=MESH,
        ).wait_recv()
    g_copy.wait()
    total = nst[0] + nst[1] + nst[2] + nst[3]
    scale = lax.rsqrt(total / hidden_size + EPS)
    scale = jnp.transpose(jnp.broadcast_to(scale, (LANES, LANES)))[:rows]
    for j in range(feats // LANES):
        cols = slice(j * LANES, (j + 1) * LANES)
        x_ref[:, cols] = (h_ref[:, cols].astype(jnp.float32) * scale * g_ref[cols].reshape(1, LANES)).astype(jnp.bfloat16)

    def product(name, t):
        fetch(name, t).wait()
        return jnp.dot(x_ref[...], streams[name][1][lax.rem(t, SLOTS)], preferred_element_type=jnp.float32)

    def refill(name, t):
        @pl.when(t + SLOTS < count)
        def _():
            fetch(name, t + SLOTS).start()

    def mate_copy(src, dst, send, recv, i):
        return pltpu.make_async_remote_copy(
            src_ref=src.at[i], dst_ref=dst.at[i], send_sem=send, recv_sem=recv.at[i],
            device_id={"row": mate}, device_id_type=MESH,
        )

    def across_copy(i):
        return pltpu.make_async_remote_copy(
            src_ref=rbuf.at[i], dst_ref=yin.at[i], send_sem=ysend.at[i], recv_sem=yrecv.at[i],
            device_id={"row": across}, device_id_type=MESH,
        )

    most = pl.ds(0, (TILES - 1) * LANES)

    def tail_copy(lanes):
        return pltpu.make_async_remote_copy(
            src_ref=rbuf.at[end, :, lanes], dst_ref=yin.at[end, :, lanes], send_sem=tail_send, recv_sem=tail_recv,
            device_id={"row": across}, device_id_type=MESH,
        )

    def each_tail(act):
        @pl.when((col < 3) & (core == 0))
        def _():
            act(tail_copy(most))

        @pl.when((col < 3) & (core == 1))
        def _():
            act(tail_copy(pl.ds(0, CHUNK)))

        @pl.when((col == 3) & (core == 1))
        def _():
            act(tail_copy(pl.ds((TILES - 1) * LANES, LANES)))

    def relay_copy(k):
        src, dst, device = (
            (rbuf.at[end, :, most], relay_in, {"col": 0}),
            (relay_in, relay_mid, {"row": across}),
            (relay_mid, yin.at[end, :, most], {"col": 3}),
        )[k]
        return pltpu.make_async_remote_copy(
            src_ref=src, dst_ref=dst, send_sem=relay_send.at[k], recv_sem=relay_recv.at[k],
            device_id=device, device_id_type=MESH,
        )

    edge_copy = pltpu.make_async_remote_copy(
        src_ref=edge_out, dst_ref=edge_in, send_sem=esend, recv_sem=erecv,
        device_id={"row": mate}, device_id_type=MESH,
    )

    def far_step(t, i):
        qbuf[i] = product("far", t)
        mate_copy(qbuf, rin, qsend, rrecv, i).start()
        refill("far", t)

    def across_step(t, i):
        term = product("across", t)
        refill("across", t)
        mate_copy(qbuf, rin, qsend, rrecv, i).wait_recv()
        rbuf[i] = term + rin[i]

    def mate_step(i):
        pbuf[i] = product("mate", i)
        mate_copy(pbuf, lin, psend, lrecv, i).start()
        refill("mate", i)

    def own_step(i):
        lbuf[i] = product("own", i)
        refill("own", i)

    turn = lax.rem(LANES - shift, LANES)
    keep = lane < LANES - shift

    def arrive(i, first, last):
        mate_copy(pbuf, lin, psend, lrecv, i).wait_recv()
        if last:
            each_tail(lambda copy: copy.wait_recv())

            @pl.when(col == 3)
            def _():
                relay_copy(2).wait_recv()
        else:
            across_copy(i).wait_recv()
        full = lbuf[i] + lin[i] + yin[i]
        parts = [full[:, k * LANES:(k + 1) * LANES] for k in range(TILES)]
        if first:
            edge_out[...] = parts[0]

            @pl.when(core == 1)
            def _():
                edge_copy.start()
        if last:
            @pl.when(core == 0)
            def _():
                edge_copy.wait_recv()

            parts[-1] = jnp.where(core == 0, edge_in[...], parts[-1])
        rolled = [pltpu.roll(part, turn, 1) for part in parts]
        tiles = [jnp.where(keep, rolled[k], rolled[k + 1]) for k in range(TILES - 1)]
        at = 0
        if not first:
            tiles = [jnp.where(keep, carry[...], rolled[0])] + tiles
            at = pl.multiple_of(i * CHUNK - LANES, LANES)
        carry[...] = rolled[-1]
        z_ref[:, pl.ds(at, LANES * len(tiles))] = jnp.concatenate(tiles, axis=1)
        top = tiles[0]
        for tile in tiles[1:]:
            top = jnp.maximum(top, tile)
        if not first:
            top = jnp.maximum(top, m_ref[...])
        mass = jnp.exp(tiles[0] - top)
        for tile in tiles[1:]:
            mass = mass + jnp.exp(tile - top)
        if not first:
            mass = mass + s_ref[...] * jnp.exp(m_ref[...] - top)
        m_ref[...] = top
        s_ref[...] = mass

    pl.semaphore_wait(hops.at[0], beside)
    tell_columns(hops.at[1])
    far_step(0, 0)
    far_step(1, end)
    across_step(0, 0)
    across_copy(0).start()
    far_step(2, 1)
    far_step(3, 2)
    across_step(1, end)
    pl.semaphore_wait(hops.at[1], beside)
    tell_columns(hops.at[2])
    each_tail(lambda copy: copy.start())

    @pl.when(col == 3)
    def _():
        relay_copy(0).start()

    @pl.loop(2, AHEAD + 2)
    def _(t):
        far_step(t + 2, t + 1)
        across_step(t, t - 1)
        across_copy(t - 1).start()

    mate_step(0)
    mate_step(1)
    own_step(0)
    arrive(0, True, False)

    @pl.loop(1, end)
    def _(i):
        t = i + AHEAD + 1

        @pl.when(t + 2 <= end)
        def _():
            far_step(t + 2, t + 1)

        @pl.when(t <= end)
        def _():
            across_step(t, t - 1)
            across_copy(t - 1).start()

        mate_step(i + 1)
        own_step(i)
        arrive(i, False, False)

        @pl.when((i == RELAY_AT[0]) & (col == 0))
        def _():
            relay_copy(0).wait_recv()
            relay_copy(1).start()

        @pl.when((i == RELAY_AT[1]) & (col == 0))
        def _():
            relay_copy(1).wait_recv()
            relay_copy(2).start()

    pl.semaphore_wait(hops.at[2], beside)
    own_step(end)
    arrive(end, False, True)

    last = carry[...]
    z_ref[:, stride:] = last[:, :rest]
    last = jnp.where(lane < rest, last, -jnp.inf)
    top = jnp.maximum(m_ref[...], last)
    mass = s_ref[...] * jnp.exp(m_ref[...] - top) + jnp.exp(last - top)
    top = jnp.transpose(jnp.concatenate([top, top], axis=0))
    mass = jnp.transpose(jnp.concatenate([mass, mass], axis=0))
    peak = jnp.max(top, axis=0, keepdims=True)
    mass = jnp.sum(mass * jnp.exp(top - peak), axis=0, keepdims=True)
    me = col * 4 + row
    fst[me] = jnp.where(lane[:1] < rows, peak, mass)

    peers = [
        (c, lax.rem(row + dr, 4))
        for c in (3 - col, lax.rem(col + 2, 4), lax.rem(5 - col, 4), col) for dr in (2, 3, 1, 0)
    ][:-1]

    def stat_copy(k, slot):
        c, r = peers[k]
        return pltpu.make_async_remote_copy(
            src_ref=fst.at[slot], dst_ref=fst.at[slot], send_sem=fsend.at[k], recv_sem=frecv.at[slot],
            device_id={"col": c, "row": r}, device_id_type=MESH,
        )

    for k in range(15):
        stat_copy(k, me).start()
    for k in reversed(range(15)):
        c, r = peers[k]
        stat_copy(k, c * 4 + r).wait_recv()
    stats = fst[...]
    swapped = pltpu.roll(stats, LANES // 2, 2)
    peak = jnp.max(stats, axis=0)
    mass = jnp.sum(swapped * jnp.exp(stats - peak), axis=0)
    lse_ref[...] = peak + jnp.log(mass)

    for k in range(1, 4):
        norm_copy(k).wait_send()
    for src, dst, send, recv in ((qbuf, rin, qsend, rrecv), (pbuf, lin, psend, lrecv)):
        pltpu.make_async_remote_copy(
            src_ref=src, dst_ref=dst, send_sem=send, recv_sem=recv.at[0],
            device_id={"row": mate}, device_id_type=MESH,
        ).wait_send()
    @pl.loop(0, end)
    def _(i):
        across_copy(i).wait_send()

    each_tail(lambda copy: copy.wait_send())

    @pl.when(col == 3)
    def _():
        relay_copy(0).wait_send()

    @pl.when(col == 0)
    def _():
        relay_copy(1).wait_send()
        relay_copy(2).wait_send()

    @pl.when(core == 1)
    def _():
        edge_copy.wait_send()

    for k in range(15):
        stat_copy(k, me).wait_send()


def solution(mesh):
    def local_head(hidden, norm_gain, w_head):
        rows, feats = hidden.shape
        width = w_head.shape[1] // 4
        count = (width // LANES + 1) // TILES
        block = (count, rows, CHUNK)
        dma = pltpu.SemaphoreType.DMA

        def body(*refs):
            head_kernel(count, width, feats * 4, *refs)

        z, lse = pl.pallas_call(
            body,
            out_shape=(
                jax.ShapeDtypeStruct((rows, width), jnp.float32),
                jax.ShapeDtypeStruct((1, LANES), jnp.float32),
            ),
            in_specs=[
                pl.BlockSpec(memory_space=pltpu.HBM),
                pl.BlockSpec(memory_space=pltpu.HBM),
                pl.BlockSpec(memory_space=pltpu.HBM),
            ],
            out_specs=(pl.BlockSpec(memory_space=pltpu.VMEM), pl.BlockSpec(memory_space=pltpu.VMEM)),
            scratch_shapes=[
                pltpu.VMEM((rows, feats), hidden.dtype),
                pltpu.VMEM((feats,), jnp.float32),
                *[pltpu.VMEM((SLOTS, feats, CHUNK), jnp.bfloat16) for _ in range(4)],
                pltpu.VMEM((rows, feats), jnp.bfloat16),
                *[pltpu.VMEM(block, jnp.float32) for _ in range(7)],
                pltpu.VMEM((4, 1, LANES), jnp.float32),
                pltpu.VMEM((16, 1, LANES), jnp.float32),
                *[pltpu.VMEM((rows, LANES), jnp.float32) for _ in range(5)],
                *[pltpu.VMEM((rows, (TILES - 1) * LANES), jnp.float32) for _ in range(2)],
                dma, dma, pltpu.SemaphoreType.REGULAR((3,)),
                *[dma((SLOTS,)) for _ in range(4)], dma((4,)), dma((4,)),
                dma, dma, dma((count,)), dma((count,)), dma((count,)), dma((count,)), dma((16,)), dma((16,)), dma, dma, dma, dma, dma((3,)), dma((3,)),
            ],
            compiler_params=pltpu.CompilerParams(
                collective_id=0, has_side_effects=True, vmem_limit_bytes=48 * 1024 * 1024
            ),
            name="head",
        )(pltpu.with_memory_space_constraint(hidden, pltpu.HBM), pltpu.with_memory_space_constraint(norm_gain, pltpu.HBM), w_head)
        log_norm = lse[0, :rows]
        return z - log_norm[:, None], log_norm

    return jax.shard_map(
        local_head,
        mesh=mesh,
        in_specs=(P("dp", "row"), P("row"), P("row", "col")),
        out_specs=(P("dp", ("col", "row")), P("dp")),
        check_vma=False,
    )
```

```python
import jax
import jax.numpy as jnp
from jax import lax
from jax.experimental import pallas as pl
from jax.experimental.pallas import tpu as pltpu
from jax.sharding import PartitionSpec as P

EPS = 1e-5
MESH = pl.DeviceIdType.MESH
LANES = 128
TILES = 3
CHUNK = TILES * LANES
AHEAD = 3
LOCAL = 5
SLOTS = 3
RELAY_AT = (4, 10)


def head_kernel(
    count, width, hidden_size,
    h_hbm, g_hbm, w_ref, z_ref, lse_ref,
    h_ref, g_ref, wq, wr, wp, wl, x_ref, qbuf, rbuf, pbuf, lbuf, rin, lin, yin, nst, fst, m_ref, s_ref, carry, edge_out, edge_in, relay_in, relay_mid,
    h_sem, g_sem, hops, wq_sem, wr_sem, wp_sem, wl_sem, nsend, nrecv, qsend, psend, ysend, rrecv, lrecv, yrecv, fsend, frecv, esend, erecv, tail_send, tail_recv, relay_send, relay_recv,
):
    rows, feats = h_ref.shape
    stride = (width // LANES) * LANES
    rest = width - stride
    col = lax.axis_index("col")
    row = lax.axis_index("row")
    core = lax.rem(row, 2)
    mate = row + 1 - 2 * core
    across = lax.rem(row + 2, 4)
    far = 3 - row
    shift = row * rest

    end = count - 1

    streams = {
        "far": (far, wq, wq_sem), "across": (across, wr, wr_sem), "mate": (mate, wp, wp_sem), "own": (row, wl, wl_sem)
    }

    def fetch(name, t):
        part, buf, sem = streams[name]
        chunk = t
        if name in ("far", "across"):
            chunk = (0, end)[t] if isinstance(t, int) and t < 2 else t - 1
        start = pl.multiple_of(stride * part + CHUNK * chunk, LANES)
        slot = lax.rem(t, SLOTS)
        return pltpu.make_async_copy(w_ref.at[:, pl.ds(start, CHUNK)], buf.at[slot], sem.at[slot])

    barrier = pltpu.get_barrier_semaphore()

    def tell_columns(sem):
        for step, there in ((-1, col > 0), (1, col < 3)):
            @pl.when(there)
            def _():
                pl.semaphore_signal(sem, inc=1, device_id_type=MESH, device_id={"col": col + step})

    for k in (2, 3, 1):
        pl.semaphore_signal(barrier, inc=1, device_id_type=MESH, device_id={"row": lax.rem(row + k, 4)})
    tell_columns(barrier)
    beside = (col + 2) // 3 + (5 - col) // 3

    h_copy = pltpu.make_async_copy(h_hbm, h_ref, h_sem)
    g_copy = pltpu.make_async_copy(g_hbm, g_ref, g_sem)
    h_copy.start()
    g_copy.start()
    h_copy.wait()
    for name, t in (("far", 0), ("far", 1), ("across", 0)):
        fetch(name, t).start()

    lane = lax.broadcasted_iota(jnp.int32, (rows, LANES), 1)
    sq = jnp.zeros((rows, LANES), jnp.float32)
    for j in range(feats // LANES):
        part = h_ref[:, j * LANES:(j + 1) * LANES].astype(jnp.float32)
        sq = sq + part * part
    sq = jnp.transpose(jnp.concatenate([sq, sq], axis=0))
    nst[row] = jnp.sum(sq, axis=0, keepdims=True)
    pl.semaphore_wait(barrier, 3 + beside)
    tell_columns(hops.at[0])

    def norm_copy(k):
        return pltpu.make_async_remote_copy(
            src_ref=nst.at[row], dst_ref=nst.at[row], send_sem=nsend.at[k], recv_sem=nrecv.at[row],
            device_id={"row": lax.rem(row + k, 4)}, device_id_type=MESH,
        )

    for k in (2, 3, 1):
        norm_copy(k).start()
    for name, t in (("far", 2), ("across", 1), ("across", 2), *[(n, t) for t in range(SLOTS) for n in ("mate", "own")]):
        fetch(name, t).start()
    for k in range(1, 4):
        peer = lax.rem(row + k, 4)
        pltpu.make_async_remote_copy(
            src_ref=nst.at[peer], dst_ref=nst.at[peer], send_sem=nsend.at[k], recv_sem=nrecv.at[peer],
            device_id={"row": peer}, device_id_type=MESH,
        ).wait_recv()
    g_copy.wait()
    total = nst[0] + nst[1] + nst[2] + nst[3]
    scale = lax.rsqrt(total / hidden_size + EPS)
    scale = jnp.transpose(jnp.broadcast_to(scale, (LANES, LANES)))[:rows]
    for j in range(feats // LANES):
        cols = slice(j * LANES, (j + 1) * LANES)
        x_ref[:, cols] = (h_ref[:, cols].astype(jnp.float32) * scale * g_ref[cols].reshape(1, LANES)).astype(jnp.bfloat16)

    def product(name, t):
        fetch(name, t).wait()
        return jnp.dot(x_ref[...], streams[name][1][lax.rem(t, SLOTS)], preferred_element_type=jnp.float32)

    def refill(name, t):
        @pl.when(t + SLOTS < count)
        def _():
            fetch(name, t + SLOTS).start()

    def mate_copy(src, dst, send, recv, i):
        return pltpu.make_async_remote_copy(
            src_ref=src.at[i], dst_ref=dst.at[i], send_sem=send, recv_sem=recv.at[i],
            device_id={"row": mate}, device_id_type=MESH,
        )

    def across_copy(i):
        return pltpu.make_async_remote_copy(
            src_ref=rbuf.at[i], dst_ref=yin.at[i], send_sem=ysend.at[i], recv_sem=yrecv.at[i],
            device_id={"row": across}, device_id_type=MESH,
        )

    most = pl.ds(0, (TILES - 1) * LANES)

    def tail_copy(lanes):
        return pltpu.make_async_remote_copy(
            src_ref=rbuf.at[end, :, lanes], dst_ref=yin.at[end, :, lanes], send_sem=tail_send, recv_sem=tail_recv,
            device_id={"row": across}, device_id_type=MESH,
        )

    def each_tail(act):
        @pl.when((col < 3) & (core == 0))
        def _():
            act(tail_copy(most))

        @pl.when((col < 3) & (core == 1))
        def _():
            act(tail_copy(pl.ds(0, CHUNK)))

        @pl.when((col == 3) & (core == 1))
        def _():
            act(tail_copy(pl.ds((TILES - 1) * LANES, LANES)))

    def relay_copy(k):
        src, dst, device = (
            (rbuf.at[end, :, most], relay_in, {"col": 0}),
            (relay_in, relay_mid, {"row": across}),
            (relay_mid, yin.at[end, :, most], {"col": 3}),
        )[k]
        return pltpu.make_async_remote_copy(
            src_ref=src, dst_ref=dst, send_sem=relay_send.at[k], recv_sem=relay_recv.at[k],
            device_id=device, device_id_type=MESH,
        )

    edge_copy = pltpu.make_async_remote_copy(
        src_ref=edge_out, dst_ref=edge_in, send_sem=esend, recv_sem=erecv,
        device_id={"row": mate}, device_id_type=MESH,
    )

    def far_step(t, i):
        qbuf[i] = product("far", t)
        mate_copy(qbuf, rin, qsend, rrecv, i).start()
        refill("far", t)

    def across_step(t, i):
        term = product("across", t)
        refill("across", t)
        mate_copy(qbuf, rin, qsend, rrecv, i).wait_recv()
        rbuf[i] = term + rin[i]

    def mate_step(i):
        pbuf[i] = product("mate", i)
        mate_copy(pbuf, lin, psend, lrecv, i).start()
        refill("mate", i)

    def own_step(i):
        lbuf[i] = product("own", i)
        refill("own", i)

    turn = lax.rem(LANES - shift, LANES)
    keep = lane < LANES - shift

    def arrive(i, first, last):
        mate_copy(pbuf, lin, psend, lrecv, i).wait_recv()
        if last:
            each_tail(lambda copy: copy.wait_recv())

            @pl.when(col == 3)
            def _():
                relay_copy(2).wait_recv()
        else:
            across_copy(i).wait_recv()
        full = lbuf[i] + lin[i] + yin[i]
        parts = [full[:, k * LANES:(k + 1) * LANES] for k in range(TILES)]
        if first:
            edge_out[...] = parts[0]

            @pl.when(core == 1)
            def _():
                edge_copy.start()
        if last:
            @pl.when(core == 0)
            def _():
                edge_copy.wait_recv()

            parts[-1] = jnp.where(core == 0, edge_in[...], parts[-1])
        rolled = [pltpu.roll(part, turn, 1) for part in parts]
        tiles = [jnp.where(keep, rolled[k], rolled[k + 1]) for k in range(TILES - 1)]
        at = 0
        if not first:
            tiles = [jnp.where(keep, carry[...], rolled[0])] + tiles
            at = pl.multiple_of(i * CHUNK - LANES, LANES)
        carry[...] = rolled[-1]
        z_ref[:, pl.ds(at, LANES * len(tiles))] = jnp.concatenate(tiles, axis=1)
        top = tiles[0]
        for tile in tiles[1:]:
            top = jnp.maximum(top, tile)
        if not first:
            top = jnp.maximum(top, m_ref[...])
        mass = jnp.exp(tiles[0] - top)
        for tile in tiles[1:]:
            mass = mass + jnp.exp(tile - top)
        if not first:
            mass = mass + s_ref[...] * jnp.exp(m_ref[...] - top)
        m_ref[...] = top
        s_ref[...] = mass

    pl.semaphore_wait(hops.at[0], beside)
    tell_columns(hops.at[1])
    far_step(0, 0)
    far_step(1, end)
    across_step(0, 0)
    across_copy(0).start()
    far_step(2, 1)
    far_step(3, 2)
    across_step(1, end)
    pl.semaphore_wait(hops.at[1], beside)
    tell_columns(hops.at[2])
    each_tail(lambda copy: copy.start())

    @pl.when(col == 3)
    def _():
        relay_copy(0).start()

    @pl.loop(2, AHEAD + 2)
    def _(t):
        far_step(t + 2, t + 1)
        across_step(t, t - 1)
        across_copy(t - 1).start()

    @pl.loop(0, LOCAL)
    def _(i):
        mate_step(i)
        own_step(i)

    arrive(0, True, False)

    @pl.loop(1, end)
    def _(i):
        t = i + AHEAD + 1

        @pl.when(t + 2 <= end)
        def _():
            far_step(t + 2, t + 1)

        @pl.when(t <= end)
        def _():
            across_step(t, t - 1)
            across_copy(t - 1).start()

        @pl.when(i + LOCAL <= end + 1)
        def _():
            mate_step(i + LOCAL - 1)
            own_step(i + LOCAL - 1)

        arrive(i, False, False)

        @pl.when((i == RELAY_AT[0]) & (col == 0))
        def _():
            relay_copy(0).wait_recv()
            relay_copy(1).start()

        @pl.when((i == RELAY_AT[1]) & (col == 0))
        def _():
            relay_copy(1).wait_recv()
            relay_copy(2).start()

    pl.semaphore_wait(hops.at[2], beside)
    arrive(end, False, True)

    last = carry[...]
    z_ref[:, stride:] = last[:, :rest]
    last = jnp.where(lane < rest, last, -jnp.inf)
    top = jnp.maximum(m_ref[...], last)
    mass = s_ref[...] * jnp.exp(m_ref[...] - top) + jnp.exp(last - top)
    top = jnp.transpose(jnp.concatenate([top, top], axis=0))
    mass = jnp.transpose(jnp.concatenate([mass, mass], axis=0))
    peak = jnp.max(top, axis=0, keepdims=True)
    mass = jnp.sum(mass * jnp.exp(top - peak), axis=0, keepdims=True)
    me = col * 4 + row
    fst[me] = jnp.where(lane[:1] < rows, peak, mass)

    peers = [
        (c, lax.rem(row + dr, 4))
        for c in (3 - col, lax.rem(col + 2, 4), lax.rem(5 - col, 4), col) for dr in (2, 3, 1, 0)
    ][:-1]

    def stat_copy(k, slot):
        c, r = peers[k]
        return pltpu.make_async_remote_copy(
            src_ref=fst.at[slot], dst_ref=fst.at[slot], send_sem=fsend.at[k], recv_sem=frecv.at[slot],
            device_id={"col": c, "row": r}, device_id_type=MESH,
        )

    for k in range(15):
        stat_copy(k, me).start()
    for k in reversed(range(15)):
        c, r = peers[k]
        stat_copy(k, c * 4 + r).wait_recv()
    stats = fst[...]
    swapped = pltpu.roll(stats, LANES // 2, 2)
    peak = jnp.max(stats, axis=0)
    mass = jnp.sum(swapped * jnp.exp(stats - peak), axis=0)
    lse_ref[...] = peak + jnp.log(mass)

    for k in range(1, 4):
        norm_copy(k).wait_send()
    for src, dst, send, recv in ((qbuf, rin, qsend, rrecv), (pbuf, lin, psend, lrecv)):
        pltpu.make_async_remote_copy(
            src_ref=src, dst_ref=dst, send_sem=send, recv_sem=recv.at[0],
            device_id={"row": mate}, device_id_type=MESH,
        ).wait_send()
    @pl.loop(0, end)
    def _(i):
        across_copy(i).wait_send()

    each_tail(lambda copy: copy.wait_send())

    @pl.when(col == 3)
    def _():
        relay_copy(0).wait_send()

    @pl.when(col == 0)
    def _():
        relay_copy(1).wait_send()
        relay_copy(2).wait_send()

    @pl.when(core == 1)
    def _():
        edge_copy.wait_send()

    for k in range(15):
        stat_copy(k, me).wait_send()


def solution(mesh):
    def local_head(hidden, norm_gain, w_head):
        rows, feats = hidden.shape
        width = w_head.shape[1] // 4
        count = (width // LANES + 1) // TILES
        block = (count, rows, CHUNK)
        dma = pltpu.SemaphoreType.DMA

        def body(*refs):
            head_kernel(count, width, feats * 4, *refs)

        z, lse = pl.pallas_call(
            body,
            out_shape=(
                jax.ShapeDtypeStruct((rows, width), jnp.float32),
                jax.ShapeDtypeStruct((1, LANES), jnp.float32),
            ),
            in_specs=[
                pl.BlockSpec(memory_space=pltpu.HBM),
                pl.BlockSpec(memory_space=pltpu.HBM),
                pl.BlockSpec(memory_space=pltpu.HBM),
            ],
            out_specs=(pl.BlockSpec(memory_space=pltpu.VMEM), pl.BlockSpec(memory_space=pltpu.VMEM)),
            scratch_shapes=[
                pltpu.VMEM((rows, feats), hidden.dtype),
                pltpu.VMEM((feats,), jnp.float32),
                *[pltpu.VMEM((SLOTS, feats, CHUNK), jnp.bfloat16) for _ in range(4)],
                pltpu.VMEM((rows, feats), jnp.bfloat16),
                *[pltpu.VMEM(block, jnp.float32) for _ in range(7)],
                pltpu.VMEM((4, 1, LANES), jnp.float32),
                pltpu.VMEM((16, 1, LANES), jnp.float32),
                *[pltpu.VMEM((rows, LANES), jnp.float32) for _ in range(5)],
                *[pltpu.VMEM((rows, (TILES - 1) * LANES), jnp.float32) for _ in range(2)],
                dma, dma, pltpu.SemaphoreType.REGULAR((3,)),
                *[dma((SLOTS,)) for _ in range(4)], dma((4,)), dma((4,)),
                dma, dma, dma((count,)), dma((count,)), dma((count,)), dma((count,)), dma((16,)), dma((16,)), dma, dma, dma, dma, dma((3,)), dma((3,)),
            ],
            compiler_params=pltpu.CompilerParams(
                collective_id=0, has_side_effects=True, vmem_limit_bytes=48 * 1024 * 1024
            ),
            name="head",
        )(pltpu.with_memory_space_constraint(hidden, pltpu.HBM), pltpu.with_memory_space_constraint(norm_gain, pltpu.HBM), w_head)
        log_norm = lse[0, :rows]
        return z - log_norm[:, None], log_norm

    return jax.shard_map(
        local_head,
        mesh=mesh,
        in_specs=(P("dp", "row"), P("row"), P("row", "col")),
        out_specs=(P("dp", ("col", "row")), P("dp")),
        check_vma=False,
    )
```

```python
import jax
import jax.numpy as jnp
from jax import lax
from jax.experimental import pallas as pl
from jax.experimental.pallas import tpu as pltpu
from jax.sharding import PartitionSpec as P

EPS = 1e-5
MESH = pl.DeviceIdType.MESH
LANES = 128
TILES = 3
CHUNK = TILES * LANES
SLOTS = 4
GROUPS = ((0,), (1, 2), (3, 7), (8, 17), (18, 23), (24,))
RELAY = 12
RELAY_AT = 14


def head_kernel(
    count, width, hidden_size,
    h_hbm, g_hbm, w_ref, z_ref, lse_ref,
    h_ref, g_ref, wq, wr, wp, wl, x_ref, qbuf, rbuf, pbuf, lbuf, rin, lin, yin, nst, fst, m_ref, s_ref, carry, edge_out, edge_in, relay_in, relay_mid,
    h_sem, g_sem, hops, wq_sem, wr_sem, wp_sem, wl_sem, nsend, nrecv, qsend, psend, ysend, rrecv, lrecv, yrecv, fsend, frecv, esend, erecv, relay_send, relay_recv,
):
    rows, feats = h_ref.shape
    stride = (width // LANES) * LANES
    rest = width - stride
    col = lax.axis_index("col")
    row = lax.axis_index("row")
    core = lax.rem(row, 2)
    mate = row + 1 - 2 * core
    across = lax.rem(row + 2, 4)
    far = 3 - row
    shift = row * rest

    end = count - 1

    streams = {
        "far": (far, wq, wq_sem), "across": (across, wr, wr_sem), "mate": (mate, wp, wp_sem), "own": (row, wl, wl_sem)
    }

    def chunk_at(t):
        if isinstance(t, int) and t < 2:
            return t * RELAY
        return t - 1 + t // (RELAY + 1)

    def fetch(name, t):
        part, buf, sem = streams[name]
        chunk = t
        if name in ("far", "across"):
            chunk = chunk_at(t)
        start = pl.multiple_of(stride * part + CHUNK * chunk, LANES)
        slot = lax.rem(t, SLOTS)
        return pltpu.make_async_copy(w_ref.at[:, pl.ds(start, CHUNK)], buf.at[slot], sem.at[slot])

    barrier = pltpu.get_barrier_semaphore()

    def tell_columns(sem):
        for step, there in ((-1, col > 0), (1, col < 3)):
            @pl.when(there)
            def _():
                pl.semaphore_signal(sem, inc=1, device_id_type=MESH, device_id={"col": col + step})

    for k in (2, 3, 1):
        pl.semaphore_signal(barrier, inc=1, device_id_type=MESH, device_id={"row": lax.rem(row + k, 4)})
    tell_columns(barrier)
    beside = (col + 2) // 3 + (5 - col) // 3

    h_copy = pltpu.make_async_copy(h_hbm, h_ref, h_sem)
    g_copy = pltpu.make_async_copy(g_hbm, g_ref, g_sem)
    h_copy.start()
    g_copy.start()
    h_copy.wait()
    for name, t in (("far", 0), ("far", 1), ("across", 0)):
        fetch(name, t).start()

    lane = lax.broadcasted_iota(jnp.int32, (rows, LANES), 1)
    sq = jnp.zeros((rows, LANES), jnp.float32)
    for j in range(feats // LANES):
        part = h_ref[:, j * LANES:(j + 1) * LANES].astype(jnp.float32)
        sq = sq + part * part
    sq = jnp.transpose(jnp.concatenate([sq, sq], axis=0))
    nst[row] = jnp.sum(sq, axis=0, keepdims=True)
    pl.semaphore_wait(barrier, 3 + beside)
    tell_columns(hops.at[0])

    def norm_copy(k):
        return pltpu.make_async_remote_copy(
            src_ref=nst.at[row], dst_ref=nst.at[row], send_sem=nsend.at[k], recv_sem=nrecv.at[row],
            device_id={"row": lax.rem(row + k, 4)}, device_id_type=MESH,
        )

    for k in (2, 3, 1):
        norm_copy(k).start()
    for name, t in (
        *[(n, t) for t in range(1, SLOTS) for n in ("far", "across") if n == "across" or t > 1], *[(n, t) for t in range(SLOTS) for n in ("mate", "own")]
    ):
        fetch(name, t).start()
    for k in range(1, 4):
        peer = lax.rem(row + k, 4)
        pltpu.make_async_remote_copy(
            src_ref=nst.at[peer], dst_ref=nst.at[peer], send_sem=nsend.at[k], recv_sem=nrecv.at[peer],
            device_id={"row": peer}, device_id_type=MESH,
        ).wait_recv()
    g_copy.wait()
    total = nst[0] + nst[1] + nst[2] + nst[3]
    scale = lax.rsqrt(total / hidden_size + EPS)
    scale = jnp.transpose(jnp.broadcast_to(scale, (LANES, LANES)))[:rows]
    for j in range(feats // LANES):
        cols = slice(j * LANES, (j + 1) * LANES)
        x_ref[:, cols] = (h_ref[:, cols].astype(jnp.float32) * scale * g_ref[cols].reshape(1, LANES)).astype(jnp.bfloat16)

    def product(name, t):
        fetch(name, t).wait()
        return jnp.dot(x_ref[...], streams[name][1][lax.rem(t, SLOTS)], preferred_element_type=jnp.float32)

    def refill(name, t):
        @pl.when(t + SLOTS < count)
        def _():
            fetch(name, t + SLOTS).start()

    def mate_copy(src, dst, send, recv, i):
        return pltpu.make_async_remote_copy(
            src_ref=src.at[i], dst_ref=dst.at[i], send_sem=send, recv_sem=recv.at[i],
            device_id={"row": mate}, device_id_type=MESH,
        )

    most = pl.ds(0, (TILES - 1) * LANES)
    final = len(GROUPS) - 1

    def across_copy(k, where):
        return pltpu.make_async_remote_copy(
            src_ref=rbuf.at[where], dst_ref=yin.at[where], send_sem=ysend.at[k], recv_sem=yrecv.at[k],
            device_id={"row": across}, device_id_type=MESH,
        )

    def pieces(k):
        lo, hi = GROUPS[k][0], GROUPS[k][-1]
        if lo <= RELAY <= hi:
            return [(k, pl.ds(lo, RELAY - lo)), (len(GROUPS), pl.ds(RELAY + 1, hi - RELAY))]
        return [(k, pl.ds(lo, hi - lo + 1))]

    def each_group(k, act):
        if k < final:
            for sem, where in pieces(k):
                act(across_copy(sem, where))
            return

        @pl.when(core == 0)
        def _():
            act(across_copy(k, (end, slice(None), most)))

        @pl.when(core == 1)
        def _():
            act(across_copy(k, end))

    def each_single(act):
        @pl.when(col < 3)
        def _():
            act(across_copy(len(GROUPS) + 1, RELAY))

        @pl.when(col == 3)
        def _():
            act(across_copy(len(GROUPS) + 1, (RELAY, slice(None), pl.ds((TILES - 1) * LANES, LANES))))

    def relay_copy(k):
        src, dst, device = (
            (rbuf.at[RELAY, :, most], relay_in, {"col": 0}),
            (relay_in, relay_mid, {"row": across}),
            (relay_mid, yin.at[RELAY, :, most], {"col": 3}),
        )[k]
        return pltpu.make_async_remote_copy(
            src_ref=src, dst_ref=dst, send_sem=relay_send.at[k], recv_sem=relay_recv.at[k],
            device_id=device, device_id_type=MESH,
        )

    edge_copy = pltpu.make_async_remote_copy(
        src_ref=edge_out, dst_ref=edge_in, send_sem=esend, recv_sem=erecv,
        device_id={"row": mate}, device_id_type=MESH,
    )

    def far_step(t, i):
        qbuf[i] = product("far", t)
        mate_copy(qbuf, rin, qsend, rrecv, i).start()
        refill("far", t)

    def across_step(t, i):
        term = product("across", t)
        refill("across", t)
        mate_copy(qbuf, rin, qsend, rrecv, i).wait_recv()
        rbuf[i] = term + rin[i]

    def mate_step(i):
        pbuf[i] = product("mate", i)
        mate_copy(pbuf, lin, psend, lrecv, i).start()
        refill("mate", i)

    def own_step(i):
        lbuf[i] = product("own", i)
        refill("own", i)

    turn = lax.rem(LANES - shift, LANES)
    keep = lane < LANES - shift

    def arrive(i, first, last):
        mate_copy(pbuf, lin, psend, lrecv, i).wait_recv()
        if first or last:
            each_group(0 if first else final, lambda copy: copy.wait_recv())
        else:
            for k in range(1, final):
                for sem, where in pieces(k):
                    @pl.when(i == where.start)
                    def _():
                        across_copy(sem, where).wait_recv()

            @pl.when(i == RELAY)
            def _():
                each_single(lambda copy: copy.wait_recv())

                @pl.when(col == 3)
                def _():
                    relay_copy(2).wait_recv()
        full = lbuf[i] + lin[i] + yin[i]
        parts = [full[:, k * LANES:(k + 1) * LANES] for k in range(TILES)]
        if first:
            edge_out[...] = parts[0]

            @pl.when(core == 1)
            def _():
                edge_copy.start()
        if last:
            @pl.when(core == 0)
            def _():
                edge_copy.wait_recv()

            parts[-1] = jnp.where(core == 0, edge_in[...], parts[-1])
        rolled = [pltpu.roll(part, turn, 1) for part in parts]
        tiles = [jnp.where(keep, rolled[k], rolled[k + 1]) for k in range(TILES - 1)]
        at = 0
        if not first:
            tiles = [jnp.where(keep, carry[...], rolled[0])] + tiles
            at = pl.multiple_of(i * CHUNK - LANES, LANES)
        carry[...] = rolled[-1]
        z_ref[:, pl.ds(at, LANES * len(tiles))] = jnp.concatenate(tiles, axis=1)
        top = tiles[0]
        for tile in tiles[1:]:
            top = jnp.maximum(top, tile)
        if not first:
            top = jnp.maximum(top, m_ref[...])
        mass = jnp.exp(tiles[0] - top)
        for tile in tiles[1:]:
            mass = mass + jnp.exp(tile - top)
        if not first:
            mass = mass + s_ref[...] * jnp.exp(m_ref[...] - top)
        m_ref[...] = top
        s_ref[...] = mass

    far_step(0, 0)
    pl.semaphore_wait(hops.at[0], beside)
    tell_columns(hops.at[1])
    far_step(1, RELAY)
    across_step(0, 0)
    each_group(0, lambda copy: copy.start())
    far_step(2, 1)
    far_step(3, 2)
    across_step(1, RELAY)
    pl.semaphore_wait(hops.at[1], beside)
    tell_columns(hops.at[2])
    each_single(lambda copy: copy.start())

    @pl.when(col == 3)
    def _():
        relay_copy(0).start()

    @pl.loop(2, count)
    def _(t):
        @pl.when(t < end - 1)
        def _():
            far_step(t + 2, chunk_at(t + 2))

        i = chunk_at(t)
        across_step(t, i)
        for k in range(1, final):
            for sem, where in pieces(k):
                @pl.when(i == where.start + where.size - 1)
                def _():
                    across_copy(sem, where).start()

        @pl.when((t == RELAY_AT) & (col == 0))
        def _():
            relay_copy(0).wait_recv()
            relay_copy(1).start()

    each_group(final, lambda copy: copy.start())

    @pl.loop(0, count)
    def _(i):
        mate_step(i)
        own_step(i)

    @pl.when(col == 0)
    def _():
        relay_copy(1).wait_recv()
        relay_copy(2).start()

    pl.semaphore_wait(hops.at[2], beside)
    arrive(0, True, False)

    @pl.loop(1, end)
    def _(i):
        arrive(i, False, False)

    arrive(end, False, True)

    last = carry[...]
    z_ref[:, stride:] = last[:, :rest]
    last = jnp.where(lane < rest, last, -jnp.inf)
    top = jnp.maximum(m_ref[...], last)
    mass = s_ref[...] * jnp.exp(m_ref[...] - top) + jnp.exp(last - top)
    top = jnp.transpose(jnp.concatenate([top, top], axis=0))
    mass = jnp.transpose(jnp.concatenate([mass, mass], axis=0))
    peak = jnp.max(top, axis=0, keepdims=True)
    mass = jnp.sum(mass * jnp.exp(top - peak), axis=0, keepdims=True)
    me = col * 4 + row
    fst[me] = jnp.where(lane[:1] < rows, peak, mass)

    peers = [
        (c, lax.rem(row + dr, 4))
        for c in (3 - col, lax.rem(col + 2, 4), lax.rem(5 - col, 4), col) for dr in (2, 3, 1, 0)
    ][:-1]

    def stat_copy(k, slot):
        c, r = peers[k]
        return pltpu.make_async_remote_copy(
            src_ref=fst.at[slot], dst_ref=fst.at[slot], send_sem=fsend.at[k], recv_sem=frecv.at[slot],
            device_id={"col": c, "row": r}, device_id_type=MESH,
        )

    for k in range(15):
        stat_copy(k, me).start()
    for k in reversed(range(15)):
        c, r = peers[k]
        stat_copy(k, c * 4 + r).wait_recv()
    stats = fst[...]
    swapped = pltpu.roll(stats, LANES // 2, 2)
    peak = jnp.max(stats, axis=0)
    mass = jnp.sum(swapped * jnp.exp(stats - peak), axis=0)
    lse_ref[...] = peak + jnp.log(mass)

    for k in range(1, 4):
        norm_copy(k).wait_send()
    for src, dst, send, recv in ((qbuf, rin, qsend, rrecv), (pbuf, lin, psend, lrecv)):
        pltpu.make_async_remote_copy(
            src_ref=src, dst_ref=dst, send_sem=send, recv_sem=recv.at[0],
            device_id={"row": mate}, device_id_type=MESH,
        ).wait_send()
    for k in range(len(GROUPS)):
        each_group(k, lambda copy: copy.wait_send())
    each_single(lambda copy: copy.wait_send())

    @pl.when(col == 3)
    def _():
        relay_copy(0).wait_send()

    @pl.when(col == 0)
    def _():
        relay_copy(1).wait_send()
        relay_copy(2).wait_send()

    @pl.when(core == 1)
    def _():
        edge_copy.wait_send()

    for k in range(15):
        stat_copy(k, me).wait_send()


def solution(mesh):
    def local_head(hidden, norm_gain, w_head):
        rows, feats = hidden.shape
        width = w_head.shape[1] // 4
        count = (width // LANES + 1) // TILES
        block = (count, rows, CHUNK)
        dma = pltpu.SemaphoreType.DMA

        def body(*refs):
            head_kernel(count, width, feats * 4, *refs)

        z, lse = pl.pallas_call(
            body,
            out_shape=(
                jax.ShapeDtypeStruct((rows, width), jnp.float32),
                jax.ShapeDtypeStruct((1, LANES), jnp.float32),
            ),
            in_specs=[
                pl.BlockSpec(memory_space=pltpu.HBM),
                pl.BlockSpec(memory_space=pltpu.HBM),
                pl.BlockSpec(memory_space=pltpu.HBM),
            ],
            out_specs=(pl.BlockSpec(memory_space=pltpu.VMEM), pl.BlockSpec(memory_space=pltpu.VMEM)),
            scratch_shapes=[
                pltpu.VMEM((rows, feats), hidden.dtype),
                pltpu.VMEM((feats,), jnp.float32),
                *[pltpu.VMEM((SLOTS, feats, CHUNK), jnp.bfloat16) for _ in range(4)],
                pltpu.VMEM((rows, feats), jnp.bfloat16),
                *[pltpu.VMEM(block, jnp.float32) for _ in range(7)],
                pltpu.VMEM((4, 1, LANES), jnp.float32),
                pltpu.VMEM((16, 1, LANES), jnp.float32),
                *[pltpu.VMEM((rows, LANES), jnp.float32) for _ in range(5)],
                *[pltpu.VMEM((rows, (TILES - 1) * LANES), jnp.float32) for _ in range(2)],
                dma, dma, pltpu.SemaphoreType.REGULAR((3,)),
                *[dma((SLOTS,)) for _ in range(4)], dma((4,)), dma((4,)),
                dma, dma, dma((len(GROUPS) + 2,)), dma((count,)), dma((count,)), dma((len(GROUPS) + 2,)), dma((16,)), dma((16,)), dma, dma, dma((3,)), dma((3,)),
            ],
            compiler_params=pltpu.CompilerParams(
                collective_id=0, has_side_effects=True, vmem_limit_bytes=48 * 1024 * 1024
            ),
            name="head",
        )(pltpu.with_memory_space_constraint(hidden, pltpu.HBM), pltpu.with_memory_space_constraint(norm_gain, pltpu.HBM), w_head)
        log_norm = lse[0, :rows]
        return z - log_norm[:, None], log_norm

    return jax.shard_map(
        local_head,
        mesh=mesh,
        in_specs=(P("dp", "row"), P("row"), P("row", "col")),
        out_specs=(P("dp", ("col", "row")), P("dp")),
        check_vma=False,
    )
```

```python
import jax
import jax.numpy as jnp
from jax import lax
from jax.experimental import pallas as pl
from jax.experimental.pallas import tpu as pltpu
from jax.sharding import PartitionSpec as P

EPS = 1e-5
MESH = pl.DeviceIdType.MESH
LANES = 128
TILES = 3
CHUNK = TILES * LANES
SLOTS = 4
GROUPS = ((0,), (1, 2), (3, 7), (8, 17), (18, 23), (24,))
RELAY = 12
RELAY_AT = 14


def head_kernel(
    count, width, hidden_size,
    h_hbm, g_hbm, w_ref, z_ref, lse_ref,
    h_ref, g_ref, wq, wr, wp, wl, x_ref, qbuf, rbuf, pbuf, lbuf, rin, lin, yin, nst, fst, m_ref, s_ref, carry, edge_out, edge_in, relay_in, relay_mid,
    h_sem, g_sem, hops, wq_sem, wr_sem, wp_sem, wl_sem, nsend, nrecv, qsend, psend, ysend, rrecv, lrecv, yrecv, fsend, frecv, esend, erecv, relay_send, relay_recv,
):
    rows, feats = h_ref.shape
    stride = (width // LANES) * LANES
    rest = width - stride
    col = lax.axis_index("col")
    row = lax.axis_index("row")
    core = lax.rem(row, 2)
    mate = row + 1 - 2 * core
    across = lax.rem(row + 2, 4)
    far = 3 - row
    shift = row * rest

    end = count - 1

    streams = {
        "far": (far, wq, wq_sem), "across": (across, wr, wr_sem), "mate": (mate, wp, wp_sem), "own": (row, wl, wl_sem)
    }

    def chunk_at(t):
        if isinstance(t, int) and t < 2:
            return t * RELAY
        return t - 1 + t // (RELAY + 1)

    def fetch(name, t):
        part, buf, sem = streams[name]
        chunk = t
        if name in ("far", "across"):
            chunk = chunk_at(t)
        start = pl.multiple_of(stride * part + CHUNK * chunk, LANES)
        slot = lax.rem(t, SLOTS)
        return pltpu.make_async_copy(w_ref.at[:, pl.ds(start, CHUNK)], buf.at[slot], sem.at[slot])

    barrier = pltpu.get_barrier_semaphore()

    def tell_column(sem, step):
        @pl.when((col + step >= 0) & (col + step < 4))
        def _():
            pl.semaphore_signal(sem, inc=1, device_id_type=MESH, device_id={"col": col + step})

    def tell_columns(sem):
        tell_column(sem, -1)
        tell_column(sem, 1)

    for k in (2, 3, 1):
        pl.semaphore_signal(barrier, inc=1, device_id_type=MESH, device_id={"row": lax.rem(row + k, 4)})
    tell_column(barrier, 1)
    below = (col + 2) // 3
    above = (5 - col) // 3
    beside = below + above

    h_copy = pltpu.make_async_copy(h_hbm, h_ref, h_sem)
    g_copy = pltpu.make_async_copy(g_hbm, g_ref, g_sem)
    h_copy.start()
    g_copy.start()
    h_copy.wait()
    for name, t in (("far", 0), ("far", 1), ("across", 0)):
        fetch(name, t).start()

    lane = lax.broadcasted_iota(jnp.int32, (rows, LANES), 1)
    sq = jnp.zeros((rows, LANES), jnp.float32)
    for j in range(feats // LANES):
        part = h_ref[:, j * LANES:(j + 1) * LANES].astype(jnp.float32)
        sq = sq + part * part
    sq = jnp.transpose(jnp.concatenate([sq, sq], axis=0))
    nst[row] = jnp.sum(sq, axis=0, keepdims=True)
    pl.semaphore_wait(barrier, 3 + below)
    tell_column(hops.at[0], -1)

    def norm_copy(k):
        return pltpu.make_async_remote_copy(
            src_ref=nst.at[row], dst_ref=nst.at[row], send_sem=nsend.at[k], recv_sem=nrecv.at[row],
            device_id={"row": lax.rem(row + k, 4)}, device_id_type=MESH,
        )

    for k in (2, 3, 1):
        norm_copy(k).start()
    for name, t in (
        *[(n, t) for t in range(1, SLOTS) for n in ("far", "across") if n == "across" or t > 1], *[(n, t) for t in range(SLOTS) for n in ("mate", "own")]
    ):
        fetch(name, t).start()
    for k in range(1, 4):
        peer = lax.rem(row + k, 4)
        pltpu.make_async_remote_copy(
            src_ref=nst.at[peer], dst_ref=nst.at[peer], send_sem=nsend.at[k], recv_sem=nrecv.at[peer],
            device_id={"row": peer}, device_id_type=MESH,
        ).wait_recv()
    g_copy.wait()
    total = nst[0] + nst[1] + nst[2] + nst[3]
    scale = lax.rsqrt(total / hidden_size + EPS)
    scale = jnp.transpose(jnp.broadcast_to(scale, (LANES, LANES)))[:rows]
    for j in range(feats // LANES):
        cols = slice(j * LANES, (j + 1) * LANES)
        x_ref[:, cols] = (h_ref[:, cols].astype(jnp.float32) * scale * g_ref[cols].reshape(1, LANES)).astype(jnp.bfloat16)

    def product(name, t):
        fetch(name, t).wait()
        return jnp.dot(x_ref[...], streams[name][1][lax.rem(t, SLOTS)], preferred_element_type=jnp.float32)

    def refill(name, t):
        @pl.when(t + SLOTS < count)
        def _():
            fetch(name, t + SLOTS).start()

    def mate_copy(src, dst, send, recv, i):
        return pltpu.make_async_remote_copy(
            src_ref=src.at[i], dst_ref=dst.at[i], send_sem=send, recv_sem=recv.at[i],
            device_id={"row": mate}, device_id_type=MESH,
        )

    most = pl.ds(0, (TILES - 1) * LANES)
    final = len(GROUPS) - 1

    def across_copy(k, where):
        return pltpu.make_async_remote_copy(
            src_ref=rbuf.at[where], dst_ref=yin.at[where], send_sem=ysend.at[k], recv_sem=yrecv.at[k],
            device_id={"row": across}, device_id_type=MESH,
        )

    def pieces(k):
        lo, hi = GROUPS[k][0], GROUPS[k][-1]
        if lo <= RELAY <= hi:
            return [(k, pl.ds(lo, RELAY - lo)), (len(GROUPS), pl.ds(RELAY + 1, hi - RELAY))]
        return [(k, pl.ds(lo, hi - lo + 1))]

    def each_group(k, act):
        if k < final:
            for sem, where in pieces(k):
                act(across_copy(sem, where))
            return

        @pl.when(core == 0)
        def _():
            act(across_copy(k, (end, slice(None), most)))

        @pl.when(core == 1)
        def _():
            act(across_copy(k, end))

    def each_single(act):
        @pl.when(col < 3)
        def _():
            act(across_copy(len(GROUPS) + 1, RELAY))

        @pl.when(col == 3)
        def _():
            act(across_copy(len(GROUPS) + 1, (RELAY, slice(None), pl.ds((TILES - 1) * LANES, LANES))))

    def relay_copy(k):
        src, dst, device = (
            (rbuf.at[RELAY, :, most], relay_in, {"col": 0}),
            (relay_in, relay_mid, {"row": across}),
            (relay_mid, yin.at[RELAY, :, most], {"col": 3}),
        )[k]
        return pltpu.make_async_remote_copy(
            src_ref=src, dst_ref=dst, send_sem=relay_send.at[k], recv_sem=relay_recv.at[k],
            device_id=device, device_id_type=MESH,
        )

    edge_copy = pltpu.make_async_remote_copy(
        src_ref=edge_out, dst_ref=edge_in, send_sem=esend, recv_sem=erecv,
        device_id={"row": mate}, device_id_type=MESH,
    )

    def far_step(t, i):
        qbuf[i] = product("far", t)
        mate_copy(qbuf, rin, qsend, rrecv, i).start()
        refill("far", t)

    def across_step(t, i):
        term = product("across", t)
        refill("across", t)
        mate_copy(qbuf, rin, qsend, rrecv, i).wait_recv()
        rbuf[i] = term + rin[i]

    def mate_step(i):
        pbuf[i] = product("mate", i)
        mate_copy(pbuf, lin, psend, lrecv, i).start()
        refill("mate", i)

    def own_step(i):
        lbuf[i] = product("own", i)
        refill("own", i)

    turn = lax.rem(LANES - shift, LANES)
    keep = lane < LANES - shift

    def arrive(i, first, last):
        mate_copy(pbuf, lin, psend, lrecv, i).wait_recv()
        if first or last:
            each_group(0 if first else final, lambda copy: copy.wait_recv())
        else:
            for k in range(1, final):
                for sem, where in pieces(k):
                    @pl.when(i == where.start)
                    def _():
                        across_copy(sem, where).wait_recv()

            @pl.when(i == RELAY)
            def _():
                each_single(lambda copy: copy.wait_recv())

                @pl.when(col == 3)
                def _():
                    relay_copy(2).wait_recv()
        full = lbuf[i] + lin[i] + yin[i]
        parts = [full[:, k * LANES:(k + 1) * LANES] for k in range(TILES)]
        if first:
            edge_out[...] = parts[0]

            @pl.when(core == 1)
            def _():
                edge_copy.start()
        if last:
            @pl.when(core == 0)
            def _():
                edge_copy.wait_recv()

            parts[-1] = jnp.where(core == 0, edge_in[...], parts[-1])
        rolled = [pltpu.roll(part, turn, 1) for part in parts]
        tiles = [jnp.where(keep, rolled[k], rolled[k + 1]) for k in range(TILES - 1)]
        at = 0
        if not first:
            tiles = [jnp.where(keep, carry[...], rolled[0])] + tiles
            at = pl.multiple_of(i * CHUNK - LANES, LANES)
        carry[...] = rolled[-1]
        z_ref[:, pl.ds(at, LANES * len(tiles))] = jnp.concatenate(tiles, axis=1)
        top = tiles[0]
        for tile in tiles[1:]:
            top = jnp.maximum(top, tile)
        if not first:
            top = jnp.maximum(top, m_ref[...])
        mass = jnp.exp(tiles[0] - top)
        for tile in tiles[1:]:
            mass = mass + jnp.exp(tile - top)
        if not first:
            mass = mass + s_ref[...] * jnp.exp(m_ref[...] - top)
        m_ref[...] = top
        s_ref[...] = mass

    far_step(0, 0)

    @pl.when(col < 3)
    def _():
        pl.semaphore_wait(hops.at[0], 1)

    tell_columns(hops.at[1])
    far_step(1, RELAY)
    across_step(0, 0)
    each_group(0, lambda copy: copy.start())
    far_step(2, 1)
    pl.semaphore_wait(hops.at[1], beside)
    tell_columns(hops.at[2])
    far_step(3, 2)
    across_step(1, RELAY)
    pl.semaphore_wait(hops.at[2], beside)
    tell_columns(hops.at[3])
    each_single(lambda copy: copy.start())

    @pl.when(col == 3)
    def _():
        relay_copy(0).start()

    @pl.loop(2, count)
    def _(t):
        @pl.when(t < end - 1)
        def _():
            far_step(t + 2, chunk_at(t + 2))

        i = chunk_at(t)
        across_step(t, i)
        for k in range(1, final):
            for sem, where in pieces(k):
                @pl.when(i == where.start + where.size - 1)
                def _():
                    across_copy(sem, where).start()

        @pl.when((t == RELAY_AT) & (col == 0))
        def _():
            relay_copy(0).wait_recv()
            relay_copy(1).start()

    each_group(final, lambda copy: copy.start())

    @pl.loop(0, count)
    def _(i):
        mate_step(i)
        own_step(i)

    @pl.when(col == 0)
    def _():
        relay_copy(1).wait_recv()
        relay_copy(2).start()

    pl.semaphore_wait(hops.at[3], beside)
    arrive(0, True, False)

    @pl.loop(1, end)
    def _(i):
        arrive(i, False, False)

    arrive(end, False, True)

    last = carry[...]
    z_ref[:, stride:] = last[:, :rest]
    last = jnp.where(lane < rest, last, -jnp.inf)
    top = jnp.maximum(m_ref[...], last)
    mass = s_ref[...] * jnp.exp(m_ref[...] - top) + jnp.exp(last - top)
    top = jnp.transpose(jnp.concatenate([top, top], axis=0))
    mass = jnp.transpose(jnp.concatenate([mass, mass], axis=0))
    peak = jnp.max(top, axis=0, keepdims=True)
    mass = jnp.sum(mass * jnp.exp(top - peak), axis=0, keepdims=True)
    me = col * 4 + row
    fst[me] = jnp.where(lane[:1] < rows, peak, mass)

    peers = [
        (c, lax.rem(row + dr, 4))
        for c in (3 - col, lax.rem(col + 2, 4), lax.rem(5 - col, 4), col) for dr in (2, 3, 1, 0)
    ][:-1]

    def stat_copy(k, slot):
        c, r = peers[k]
        return pltpu.make_async_remote_copy(
            src_ref=fst.at[slot], dst_ref=fst.at[slot], send_sem=fsend.at[k], recv_sem=frecv.at[slot],
            device_id={"col": c, "row": r}, device_id_type=MESH,
        )

    for k in range(15):
        stat_copy(k, me).start()
    for k in reversed(range(15)):
        c, r = peers[k]
        stat_copy(k, c * 4 + r).wait_recv()
    stats = fst[...]
    swapped = pltpu.roll(stats, LANES // 2, 2)
    peak = jnp.max(stats, axis=0)
    mass = jnp.sum(swapped * jnp.exp(stats - peak), axis=0)
    lse_ref[...] = peak + jnp.log(mass)

    for k in range(1, 4):
        norm_copy(k).wait_send()
    for src, dst, send, recv in ((qbuf, rin, qsend, rrecv), (pbuf, lin, psend, lrecv)):
        pltpu.make_async_remote_copy(
            src_ref=src, dst_ref=dst, send_sem=send, recv_sem=recv.at[0],
            device_id={"row": mate}, device_id_type=MESH,
        ).wait_send()
    for k in range(len(GROUPS)):
        each_group(k, lambda copy: copy.wait_send())
    each_single(lambda copy: copy.wait_send())

    @pl.when(col == 3)
    def _():
        relay_copy(0).wait_send()

    @pl.when(col == 0)
    def _():
        relay_copy(1).wait_send()
        relay_copy(2).wait_send()

    @pl.when(core == 1)
    def _():
        edge_copy.wait_send()

    for k in range(15):
        stat_copy(k, me).wait_send()


def solution(mesh):
    def local_head(hidden, norm_gain, w_head):
        rows, feats = hidden.shape
        width = w_head.shape[1] // 4
        count = (width // LANES + 1) // TILES
        block = (count, rows, CHUNK)
        dma = pltpu.SemaphoreType.DMA

        def body(*refs):
            head_kernel(count, width, feats * 4, *refs)

        z, lse = pl.pallas_call(
            body,
            out_shape=(
                jax.ShapeDtypeStruct((rows, width), jnp.float32),
                jax.ShapeDtypeStruct((1, LANES), jnp.float32),
            ),
            in_specs=[
                pl.BlockSpec(memory_space=pltpu.HBM),
                pl.BlockSpec(memory_space=pltpu.HBM),
                pl.BlockSpec(memory_space=pltpu.HBM),
            ],
            out_specs=(pl.BlockSpec(memory_space=pltpu.VMEM), pl.BlockSpec(memory_space=pltpu.VMEM)),
            scratch_shapes=[
                pltpu.VMEM((rows, feats), hidden.dtype),
                pltpu.VMEM((feats,), jnp.float32),
                *[pltpu.VMEM((SLOTS, feats, CHUNK), jnp.bfloat16) for _ in range(4)],
                pltpu.VMEM((rows, feats), jnp.bfloat16),
                *[pltpu.VMEM(block, jnp.float32) for _ in range(7)],
                pltpu.VMEM((4, 1, LANES), jnp.float32),
                pltpu.VMEM((16, 1, LANES), jnp.float32),
                *[pltpu.VMEM((rows, LANES), jnp.float32) for _ in range(5)],
                *[pltpu.VMEM((rows, (TILES - 1) * LANES), jnp.float32) for _ in range(2)],
                dma, dma, pltpu.SemaphoreType.REGULAR((4,)),
                *[dma((SLOTS,)) for _ in range(4)], dma((4,)), dma((4,)),
                dma, dma, dma((len(GROUPS) + 2,)), dma((count,)), dma((count,)), dma((len(GROUPS) + 2,)), dma((16,)), dma((16,)), dma, dma, dma((3,)), dma((3,)),
            ],
            compiler_params=pltpu.CompilerParams(
                collective_id=0, has_side_effects=True, vmem_limit_bytes=48 * 1024 * 1024
            ),
            name="head",
        )(pltpu.with_memory_space_constraint(hidden, pltpu.HBM), pltpu.with_memory_space_constraint(norm_gain, pltpu.HBM), w_head)
        log_norm = lse[0, :rows]
        return z - log_norm[:, None], log_norm

    return jax.shard_map(
        local_head,
        mesh=mesh,
        in_specs=(P("dp", "row"), P("row"), P("row", "col")),
        out_specs=(P("dp", ("col", "row")), P("dp")),
        check_vma=False,
    )
```

```python
import jax
import jax.numpy as jnp
from jax import lax
from jax.experimental import pallas as pl
from jax.experimental.pallas import tpu as pltpu
from jax.sharding import PartitionSpec as P

EPS = 1e-5
MESH = pl.DeviceIdType.MESH
LANES = 128
TILES = 3
CHUNK = TILES * LANES
SLOTS = 4
GROUPS = ((0,), (1, 2), (3, 7), (8, 17), (18, 23), (24,))
RELAY = 12
RELAY_AT = 14


def head_kernel(
    count, width, hidden_size,
    h_hbm, g_hbm, w_ref, z_ref, lse_ref,
    h_ref, g_ref, wq, wr, wp, wl, x_ref, qbuf, rbuf, pbuf, lbuf, rin, lin, yin, nst, fst, m_ref, s_ref, carry, edge_out, edge_in, relay_in, relay_mid, rx, qx,
    h_sem, g_sem, hops, wq_sem, wr_sem, wp_sem, wl_sem, nsend, nrecv, qsend, psend, ysend, rrecv, lrecv, yrecv, fsend, frecv, esend, erecv, relay_send, relay_recv, rx_send, rx_recv, qx_send,
):
    rows, feats = h_ref.shape
    stride = (width // LANES) * LANES
    rest = width - stride
    col = lax.axis_index("col")
    row = lax.axis_index("row")
    core = lax.rem(row, 2)
    mate = row + 1 - 2 * core
    across = lax.rem(row + 2, 4)
    far = 3 - row
    shift = row * rest

    end = count - 1

    streams = {
        "far": (far, wq, wq_sem), "across": (across, wr, wr_sem), "mate": (mate, wp, wp_sem), "own": (row, wl, wl_sem)
    }

    def chunk_at(t):
        if isinstance(t, int) and t < 2:
            return t * RELAY
        return t - 1 + t // (RELAY + 1)

    def fetch(name, t):
        part, buf, sem = streams[name]
        chunk = t
        if name in ("far", "across"):
            chunk = chunk_at(t)
        start = pl.multiple_of(stride * part + CHUNK * chunk, LANES)
        slot = lax.rem(t, SLOTS)
        return pltpu.make_async_copy(w_ref.at[:, pl.ds(start, CHUNK)], buf.at[slot], sem.at[slot])

    barrier = pltpu.get_barrier_semaphore()

    def tell_column(sem, step):
        @pl.when((col + step >= 0) & (col + step < 4))
        def _():
            pl.semaphore_signal(sem, inc=1, device_id_type=MESH, device_id={"col": col + step})

    def tell_columns(sem):
        tell_column(sem, -1)
        tell_column(sem, 1)

    for k in (2, 3, 1):
        pl.semaphore_signal(barrier, inc=1, device_id_type=MESH, device_id={"row": lax.rem(row + k, 4)})
    tell_column(barrier, 1)
    below = (col + 2) // 3
    above = (5 - col) // 3
    beside = below + above

    h_copy = pltpu.make_async_copy(h_hbm, h_ref, h_sem)
    g_copy = pltpu.make_async_copy(g_hbm, g_ref, g_sem)
    h_copy.start()
    g_copy.start()
    h_copy.wait()
    for name, t in (("far", 0), ("far", 1), ("across", 0)):
        fetch(name, t).start()

    lane = lax.broadcasted_iota(jnp.int32, (rows, LANES), 1)
    sq = jnp.zeros((rows, LANES), jnp.float32)
    for j in range(feats // LANES):
        part = h_ref[:, j * LANES:(j + 1) * LANES].astype(jnp.float32)
        sq = sq + part * part
    sq = jnp.transpose(jnp.concatenate([sq, sq], axis=0))
    nst[row] = jnp.sum(sq, axis=0, keepdims=True)
    pl.semaphore_wait(barrier, 3 + below)
    tell_column(hops.at[0], -1)

    def norm_copy(k):
        return pltpu.make_async_remote_copy(
            src_ref=nst.at[row], dst_ref=nst.at[row], send_sem=nsend.at[k], recv_sem=nrecv.at[row],
            device_id={"row": lax.rem(row + k, 4)}, device_id_type=MESH,
        )

    for k in (2, 3, 1):
        norm_copy(k).start()
    for name, t in (
        *[(n, t) for t in range(1, SLOTS) for n in ("far", "across") if n == "across" or t > 1], *[(n, t) for t in range(SLOTS) for n in ("mate", "own")]
    ):
        fetch(name, t).start()
    for k in range(1, 4):
        peer = lax.rem(row + k, 4)
        pltpu.make_async_remote_copy(
            src_ref=nst.at[peer], dst_ref=nst.at[peer], send_sem=nsend.at[k], recv_sem=nrecv.at[peer],
            device_id={"row": peer}, device_id_type=MESH,
        ).wait_recv()
    g_copy.wait()
    total = nst[0] + nst[1] + nst[2] + nst[3]
    scale = lax.rsqrt(total / hidden_size + EPS)
    scale = jnp.transpose(jnp.broadcast_to(scale, (LANES, LANES)))[:rows]
    for j in range(feats // LANES):
        cols = slice(j * LANES, (j + 1) * LANES)
        x_ref[:, cols] = (h_ref[:, cols].astype(jnp.float32) * scale * g_ref[cols].reshape(1, LANES)).astype(jnp.bfloat16)

    def product(name, t):
        fetch(name, t).wait()
        return jnp.dot(x_ref[...], streams[name][1][lax.rem(t, SLOTS)], preferred_element_type=jnp.float32)

    def refill(name, t):
        @pl.when(t + SLOTS < count)
        def _():
            fetch(name, t + SLOTS).start()

    def mate_copy(src, dst, send, recv, i):
        return pltpu.make_async_remote_copy(
            src_ref=src.at[i], dst_ref=dst.at[i], send_sem=send, recv_sem=recv.at[i],
            device_id={"row": mate}, device_id_type=MESH,
        )

    most = pl.ds(0, (TILES - 1) * LANES)
    final = len(GROUPS) - 1

    def across_copy(k, where):
        return pltpu.make_async_remote_copy(
            src_ref=rbuf.at[where], dst_ref=yin.at[where], send_sem=ysend.at[k], recv_sem=yrecv.at[k],
            device_id={"row": across}, device_id_type=MESH,
        )

    def pieces(k):
        lo, hi = GROUPS[k][0], GROUPS[k][-1]
        if lo <= RELAY <= hi:
            return [(k, pl.ds(lo, RELAY - lo)), (len(GROUPS), pl.ds(RELAY + 1, hi - RELAY))]
        return [(k, pl.ds(lo, hi - lo + 1))]

    rx_copy = pltpu.make_async_remote_copy(
        src_ref=rbuf.at[end, :, most], dst_ref=rx, send_sem=rx_send, recv_sem=rx_recv,
        device_id={"row": mate}, device_id_type=MESH,
    )
    qx_copy = pltpu.make_async_remote_copy(
        src_ref=qx, dst_ref=yin.at[end, :, most], send_sem=qx_send, recv_sem=yrecv.at[final],
        device_id={"row": far}, device_id_type=MESH,
    )

    def last_step():
        rbuf[end] = product("across", end)

        @pl.when(core == 0)
        def _():
            rx_copy.start()

        mate_copy(qbuf, rin, qsend, rrecv, end).wait_recv()

        @pl.when(core == 1)
        def _():
            rx_copy.wait_recv()
            qx[...] = qbuf[end, :, most] + rx[...]
            qx_copy.start()
            rbuf[end] = rbuf[end] + rin[end]
            across_copy(final, end).start()

    def each_group(k, act):
        for sem, where in pieces(k):
            act(across_copy(sem, where))

    def each_single(act):
        @pl.when(col < 3)
        def _():
            act(across_copy(len(GROUPS) + 1, RELAY))

        @pl.when(col == 3)
        def _():
            act(across_copy(len(GROUPS) + 1, (RELAY, slice(None), pl.ds((TILES - 1) * LANES, LANES))))

    def relay_copy(k):
        src, dst, device = (
            (rbuf.at[RELAY, :, most], relay_in, {"col": 0}),
            (relay_in, relay_mid, {"row": across}),
            (relay_mid, yin.at[RELAY, :, most], {"col": 3}),
        )[k]
        return pltpu.make_async_remote_copy(
            src_ref=src, dst_ref=dst, send_sem=relay_send.at[k], recv_sem=relay_recv.at[k],
            device_id=device, device_id_type=MESH,
        )

    edge_copy = pltpu.make_async_remote_copy(
        src_ref=edge_out, dst_ref=edge_in, send_sem=esend, recv_sem=erecv,
        device_id={"row": mate}, device_id_type=MESH,
    )

    def far_step(t, i):
        qbuf[i] = product("far", t)
        mate_copy(qbuf, rin, qsend, rrecv, i).start()
        refill("far", t)

    def across_step(t, i):
        term = product("across", t)
        refill("across", t)
        mate_copy(qbuf, rin, qsend, rrecv, i).wait_recv()
        rbuf[i] = term + rin[i]

    def mate_step(i):
        pbuf[i] = product("mate", i)
        mate_copy(pbuf, lin, psend, lrecv, i).start()
        refill("mate", i)

    def own_step(i):
        lbuf[i] = product("own", i)
        refill("own", i)

    turn = lax.rem(LANES - shift, LANES)
    keep = lane < LANES - shift

    def arrive(i, first, last):
        mate_copy(pbuf, lin, psend, lrecv, i).wait_recv()
        if first:
            each_group(0, lambda copy: copy.wait_recv())
        elif last:
            @pl.when(core == 0)
            def _():
                qx_copy.wait_recv()

            @pl.when(core == 1)
            def _():
                across_copy(final, end).wait_recv()
        else:
            for k in range(1, final):
                for sem, where in pieces(k):
                    @pl.when(i == where.start)
                    def _():
                        across_copy(sem, where).wait_recv()

            @pl.when(i == RELAY)
            def _():
                each_single(lambda copy: copy.wait_recv())

                @pl.when(col == 3)
                def _():
                    relay_copy(2).wait_recv()
        full = lbuf[i] + lin[i] + yin[i]
        parts = [full[:, k * LANES:(k + 1) * LANES] for k in range(TILES)]
        if first:
            edge_out[...] = parts[0]

            @pl.when(core == 1)
            def _():
                edge_copy.start()
        if last:
            @pl.when(core == 0)
            def _():
                edge_copy.wait_recv()

            parts[-1] = jnp.where(core == 0, edge_in[...], parts[-1])
        rolled = [pltpu.roll(part, turn, 1) for part in parts]
        tiles = [jnp.where(keep, rolled[k], rolled[k + 1]) for k in range(TILES - 1)]
        at = 0
        if not first:
            tiles = [jnp.where(keep, carry[...], rolled[0])] + tiles
            at = pl.multiple_of(i * CHUNK - LANES, LANES)
        carry[...] = rolled[-1]
        z_ref[:, pl.ds(at, LANES * len(tiles))] = jnp.concatenate(tiles, axis=1)
        top = tiles[0]
        for tile in tiles[1:]:
            top = jnp.maximum(top, tile)
        if not first:
            top = jnp.maximum(top, m_ref[...])
        mass = jnp.exp(tiles[0] - top)
        for tile in tiles[1:]:
            mass = mass + jnp.exp(tile - top)
        if not first:
            mass = mass + s_ref[...] * jnp.exp(m_ref[...] - top)
        m_ref[...] = top
        s_ref[...] = mass

    far_step(0, 0)

    @pl.when(col < 3)
    def _():
        pl.semaphore_wait(hops.at[0], 1)

    tell_columns(hops.at[1])
    far_step(1, RELAY)
    across_step(0, 0)
    each_group(0, lambda copy: copy.start())
    far_step(2, 1)
    pl.semaphore_wait(hops.at[1], beside)
    tell_columns(hops.at[2])
    far_step(3, 2)
    across_step(1, RELAY)
    pl.semaphore_wait(hops.at[2], beside)
    tell_columns(hops.at[3])
    each_single(lambda copy: copy.start())

    @pl.when(col == 3)
    def _():
        relay_copy(0).start()

    @pl.loop(2, end)
    def _(t):
        @pl.when(t < end - 1)
        def _():
            far_step(t + 2, chunk_at(t + 2))

        i = chunk_at(t)
        across_step(t, i)
        for k in range(1, final):
            for sem, where in pieces(k):
                @pl.when(i == where.start + where.size - 1)
                def _():
                    across_copy(sem, where).start()

        @pl.when((t == RELAY_AT) & (col == 0))
        def _():
            relay_copy(0).wait_recv()
            relay_copy(1).start()

    last_step()

    @pl.loop(0, count)
    def _(i):
        mate_step(i)
        own_step(i)

    @pl.when(col == 0)
    def _():
        relay_copy(1).wait_recv()
        relay_copy(2).start()

    pl.semaphore_wait(hops.at[3], beside)
    arrive(0, True, False)

    @pl.loop(1, end)
    def _(i):
        arrive(i, False, False)

    arrive(end, False, True)

    last = carry[...]
    z_ref[:, stride:] = last[:, :rest]
    last = jnp.where(lane < rest, last, -jnp.inf)
    top = jnp.maximum(m_ref[...], last)
    mass = s_ref[...] * jnp.exp(m_ref[...] - top) + jnp.exp(last - top)
    top = jnp.transpose(jnp.concatenate([top, top], axis=0))
    mass = jnp.transpose(jnp.concatenate([mass, mass], axis=0))
    peak = jnp.max(top, axis=0, keepdims=True)
    mass = jnp.sum(mass * jnp.exp(top - peak), axis=0, keepdims=True)
    me = col * 4 + row
    fst[me] = jnp.where(lane[:1] < rows, peak, mass)

    def stat_copy(c, dr, slot):
        return pltpu.make_async_remote_copy(
            src_ref=fst.at[slot], dst_ref=fst.at[slot], send_sem=fsend.at[c * 4 + dr], recv_sem=frecv.at[slot],
            device_id={"col": c, "row": lax.rem(row + dr, 4)}, device_id_type=MESH,
        )

    def each_peer(act):
        for c in range(4):
            for dr in (2, 3, 1):
                act(c, dr)

            @pl.when(col != c)
            def _():
                act(c, 0)

    each_peer(lambda c, dr: stat_copy(c, dr, me).start())
    each_peer(lambda c, dr: stat_copy(c, dr, c * 4 + lax.rem(row + dr, 4)).wait_recv())
    stats = fst[...]
    swapped = pltpu.roll(stats, LANES // 2, 2)
    peak = jnp.max(stats, axis=0)
    mass = jnp.sum(swapped * jnp.exp(stats - peak), axis=0)
    lse_ref[...] = peak + jnp.log(mass)

    for k in range(1, 4):
        norm_copy(k).wait_send()
    for src, dst, send, recv in ((qbuf, rin, qsend, rrecv), (pbuf, lin, psend, lrecv)):
        pltpu.make_async_remote_copy(
            src_ref=src, dst_ref=dst, send_sem=send, recv_sem=recv.at[0],
            device_id={"row": mate}, device_id_type=MESH,
        ).wait_send()
    for k in range(final):
        each_group(k, lambda copy: copy.wait_send())
    each_single(lambda copy: copy.wait_send())

    @pl.when(core == 0)
    def _():
        rx_copy.wait_send()

    @pl.when(core == 1)
    def _():
        qx_copy.wait_send()
        across_copy(final, end).wait_send()

    @pl.when(col == 3)
    def _():
        relay_copy(0).wait_send()

    @pl.when(col == 0)
    def _():
        relay_copy(1).wait_send()
        relay_copy(2).wait_send()

    @pl.when(core == 1)
    def _():
        edge_copy.wait_send()

    each_peer(lambda c, dr: stat_copy(c, dr, me).wait_send())


def solution(mesh):
    def local_head(hidden, norm_gain, w_head):
        rows, feats = hidden.shape
        width = w_head.shape[1] // 4
        count = (width // LANES + 1) // TILES
        block = (count, rows, CHUNK)
        dma = pltpu.SemaphoreType.DMA

        def body(*refs):
            head_kernel(count, width, feats * 4, *refs)

        z, lse = pl.pallas_call(
            body,
            out_shape=(
                jax.ShapeDtypeStruct((rows, width), jnp.float32),
                jax.ShapeDtypeStruct((1, LANES), jnp.float32),
            ),
            in_specs=[
                pl.BlockSpec(memory_space=pltpu.HBM),
                pl.BlockSpec(memory_space=pltpu.HBM),
                pl.BlockSpec(memory_space=pltpu.HBM),
            ],
            out_specs=(pl.BlockSpec(memory_space=pltpu.VMEM), pl.BlockSpec(memory_space=pltpu.VMEM)),
            scratch_shapes=[
                pltpu.VMEM((rows, feats), hidden.dtype),
                pltpu.VMEM((feats,), jnp.float32),
                *[pltpu.VMEM((SLOTS, feats, CHUNK), jnp.bfloat16) for _ in range(4)],
                pltpu.VMEM((rows, feats), jnp.bfloat16),
                *[pltpu.VMEM(block, jnp.float32) for _ in range(7)],
                pltpu.VMEM((4, 1, LANES), jnp.float32),
                pltpu.VMEM((16, 1, LANES), jnp.float32),
                *[pltpu.VMEM((rows, LANES), jnp.float32) for _ in range(5)],
                *[pltpu.VMEM((rows, (TILES - 1) * LANES), jnp.float32) for _ in range(4)],
                dma, dma, pltpu.SemaphoreType.REGULAR((4,)),
                *[dma((SLOTS,)) for _ in range(4)], dma((4,)), dma((4,)),
                dma, dma, dma((len(GROUPS) + 2,)), dma((count,)), dma((count,)), dma((len(GROUPS) + 2,)), dma((16,)), dma((16,)), dma, dma, dma((3,)), dma((3,)), dma, dma, dma,
            ],
            compiler_params=pltpu.CompilerParams(
                collective_id=0, has_side_effects=True, vmem_limit_bytes=48 * 1024 * 1024
            ),
            name="head",
        )(pltpu.with_memory_space_constraint(hidden, pltpu.HBM), pltpu.with_memory_space_constraint(norm_gain, pltpu.HBM), w_head)
        log_norm = lse[0, :rows]
        return z - log_norm[:, None], log_norm

    return jax.shard_map(
        local_head,
        mesh=mesh,
        in_specs=(P("dp", "row"), P("row"), P("row", "col")),
        out_specs=(P("dp", ("col", "row")), P("dp")),
        check_vma=False,
    )
```

```python
import jax
import jax.numpy as jnp
from jax import lax
from jax.experimental import pallas as pl
from jax.experimental.pallas import tpu as pltpu
from jax.sharding import PartitionSpec as P

EPS = 1e-5
MESH = pl.DeviceIdType.MESH
LANES = 128
TILES = 3
CHUNK = TILES * LANES
SLOTS = 4
GROUPS = ((0,), (1, 4), (5, 18), (19, 23), (24,))
RELAY = 12
RELAY_AT = 14


def head_kernel(
    count, width, hidden_size,
    h_hbm, g_hbm, w_ref, z_ref, lse_ref,
    h_ref, g_ref, wq, wr, wp, wl, x_ref, qbuf, rbuf, pbuf, lbuf, rin, lin, yin, nst, fst, m_ref, s_ref, carry, edge_out, edge_in, relay_in, relay_mid, rx, qx, first_in,
    h_sem, g_sem, hops, wq_sem, wr_sem, wp_sem, wl_sem, nsend, nrecv, qsend, psend, ysend, rrecv, lrecv, yrecv, fsend, frecv, esend, erecv, relay_send, relay_recv, rx_send, rx_recv, qx_send, first_send, first_recv,
):
    rows, feats = h_ref.shape
    stride = (width // LANES) * LANES
    rest = width - stride
    col = lax.axis_index("col")
    row = lax.axis_index("row")
    core = lax.rem(row, 2)
    mate = row + 1 - 2 * core
    across = lax.rem(row + 2, 4)
    far = 3 - row
    shift = row * rest

    end = count - 1

    streams = {
        "far": (far, wq, wq_sem), "across": (across, wr, wr_sem), "mate": (mate, wp, wp_sem), "own": (row, wl, wl_sem)
    }

    def chunk_at(t):
        if isinstance(t, int) and t < 2:
            return t * RELAY
        return t - 1 + t // (RELAY + 1)

    def fetch(name, t):
        part, buf, sem = streams[name]
        chunk = t
        if name in ("far", "across"):
            chunk = chunk_at(t)
        start = pl.multiple_of(stride * part + CHUNK * chunk, LANES)
        slot = lax.rem(t, SLOTS)
        return pltpu.make_async_copy(w_ref.at[:, pl.ds(start, CHUNK)], buf.at[slot], sem.at[slot])

    barrier = pltpu.get_barrier_semaphore()

    def tell_column(sem, step):
        @pl.when((col + step >= 0) & (col + step < 4))
        def _():
            pl.semaphore_signal(sem, inc=1, device_id_type=MESH, device_id={"col": col + step})

    def tell_columns(sem):
        tell_column(sem, -1)
        tell_column(sem, 1)

    for k in (2, 3, 1):
        pl.semaphore_signal(barrier, inc=1, device_id_type=MESH, device_id={"row": lax.rem(row + k, 4)})
    tell_column(barrier, 1)
    below = (col + 2) // 3
    above = (5 - col) // 3
    beside = below + above

    h_copy = pltpu.make_async_copy(h_hbm, h_ref, h_sem)
    g_copy = pltpu.make_async_copy(g_hbm, g_ref, g_sem)
    h_copy.start()
    g_copy.start()
    h_copy.wait()
    for name, t in (("far", 0), ("far", 1), ("across", 0)):
        fetch(name, t).start()

    lane = lax.broadcasted_iota(jnp.int32, (rows, LANES), 1)
    sq = jnp.zeros((rows, LANES), jnp.float32)
    for j in range(feats // LANES):
        part = h_ref[:, j * LANES:(j + 1) * LANES].astype(jnp.float32)
        sq = sq + part * part
    sq = jnp.transpose(jnp.concatenate([sq, sq], axis=0))
    nst[row] = jnp.sum(sq, axis=0, keepdims=True)
    pl.semaphore_wait(barrier, 3 + below)
    tell_column(hops.at[0], -1)

    def norm_copy(k):
        return pltpu.make_async_remote_copy(
            src_ref=nst.at[row], dst_ref=nst.at[row], send_sem=nsend.at[k], recv_sem=nrecv.at[row],
            device_id={"row": lax.rem(row + k, 4)}, device_id_type=MESH,
        )

    for k in (2, 3, 1):
        norm_copy(k).start()
    for name, t in (
        *[(n, t) for t in range(1, SLOTS) for n in ("far", "across") if n == "across" or t > 1], *[(n, t) for t in range(SLOTS) for n in ("mate", "own")]
    ):
        fetch(name, t).start()
    for k in range(1, 4):
        peer = lax.rem(row + k, 4)
        pltpu.make_async_remote_copy(
            src_ref=nst.at[peer], dst_ref=nst.at[peer], send_sem=nsend.at[k], recv_sem=nrecv.at[peer],
            device_id={"row": peer}, device_id_type=MESH,
        ).wait_recv()
    g_copy.wait()
    total = nst[0] + nst[1] + nst[2] + nst[3]
    scale = lax.rsqrt(total / hidden_size + EPS)
    scale = jnp.transpose(jnp.broadcast_to(scale, (LANES, LANES)))[:rows]
    for j in range(feats // LANES):
        cols = slice(j * LANES, (j + 1) * LANES)
        x_ref[:, cols] = (h_ref[:, cols].astype(jnp.float32) * scale * g_ref[cols].reshape(1, LANES)).astype(jnp.bfloat16)

    def product(name, t):
        fetch(name, t).wait()
        return jnp.dot(x_ref[...], streams[name][1][lax.rem(t, SLOTS)], preferred_element_type=jnp.float32)

    def refill(name, t):
        @pl.when(t + SLOTS < count)
        def _():
            fetch(name, t + SLOTS).start()

    def mate_copy(src, dst, send, recv, i):
        return pltpu.make_async_remote_copy(
            src_ref=src.at[i], dst_ref=dst.at[i], send_sem=send, recv_sem=recv.at[i],
            device_id={"row": mate}, device_id_type=MESH,
        )

    most = pl.ds(0, (TILES - 1) * LANES)
    final = len(GROUPS) - 1

    def across_copy(k, where):
        return pltpu.make_async_remote_copy(
            src_ref=rbuf.at[where], dst_ref=yin.at[where], send_sem=ysend.at[k], recv_sem=yrecv.at[k],
            device_id={"row": across}, device_id_type=MESH,
        )

    def pieces(k):
        lo, hi = GROUPS[k][0], GROUPS[k][-1]
        if lo <= RELAY <= hi:
            return [(k, pl.ds(lo, RELAY - lo)), (len(GROUPS), pl.ds(RELAY + 1, hi - RELAY))]
        return [(k, pl.ds(lo, hi - lo + 1))]

    rx_copy = pltpu.make_async_remote_copy(
        src_ref=rbuf.at[end, :, most], dst_ref=rx, send_sem=rx_send, recv_sem=rx_recv,
        device_id={"row": mate}, device_id_type=MESH,
    )
    qx_copy = pltpu.make_async_remote_copy(
        src_ref=qx, dst_ref=yin.at[end, :, most], send_sem=qx_send, recv_sem=yrecv.at[final],
        device_id={"row": far}, device_id_type=MESH,
    )

    lead = pl.ds(0, LANES)
    rest_of = pl.ds(LANES, (TILES - 1) * LANES)

    def first_copy(k):
        src, dst, device = (
            (qbuf.at[0, :, lead], first_in, far),
            (rbuf.at[0, :, lead], yin.at[0, :, lead], across),
            (rbuf.at[0, :, rest_of], yin.at[0, :, rest_of], across),
        )[k]
        return pltpu.make_async_remote_copy(
            src_ref=src, dst_ref=dst, send_sem=first_send.at[k], recv_sem=first_recv.at[k],
            device_id={"row": device}, device_id_type=MESH,
        )

    def last_step():
        rbuf[end] = product("across", end)

        @pl.when(core == 0)
        def _():
            rx_copy.start()

        mate_copy(qbuf, rin, qsend, rrecv, end).wait_recv()

        @pl.when(core == 1)
        def _():
            rx_copy.wait_recv()
            qx[...] = qbuf[end, :, most] + rx[...]
            qx_copy.start()
            rbuf[end] = rbuf[end] + rin[end]
            across_copy(final, end).start()

    def each_group(k, act):
        for sem, where in pieces(k):
            act(across_copy(sem, where))

    def each_single(act):
        @pl.when(col < 3)
        def _():
            act(across_copy(len(GROUPS) + 1, RELAY))

        @pl.when(col == 3)
        def _():
            act(across_copy(len(GROUPS) + 1, (RELAY, slice(None), pl.ds((TILES - 1) * LANES, LANES))))

    def relay_copy(k):
        src, dst, device = (
            (rbuf.at[RELAY, :, most], relay_in, {"col": 0}),
            (relay_in, relay_mid, {"row": across}),
            (relay_mid, yin.at[RELAY, :, most], {"col": 3}),
        )[k]
        return pltpu.make_async_remote_copy(
            src_ref=src, dst_ref=dst, send_sem=relay_send.at[k], recv_sem=relay_recv.at[k],
            device_id=device, device_id_type=MESH,
        )

    edge_copy = pltpu.make_async_remote_copy(
        src_ref=edge_out, dst_ref=edge_in, send_sem=esend, recv_sem=erecv,
        device_id={"row": mate}, device_id_type=MESH,
    )

    def far_step(t, i):
        qbuf[i] = product("far", t)
        mate_copy(qbuf, rin, qsend, rrecv, i).start()
        refill("far", t)

    def across_step(t, i):
        term = product("across", t)
        refill("across", t)
        mate_copy(qbuf, rin, qsend, rrecv, i).wait_recv()
        rbuf[i] = term + rin[i]

    def mate_step(i):
        pbuf[i] = product("mate", i)
        mate_copy(pbuf, lin, psend, lrecv, i).start()
        refill("mate", i)

    def own_step(i):
        lbuf[i] = product("own", i)
        refill("own", i)

    turn = lax.rem(LANES - shift, LANES)
    keep = lane < LANES - shift

    def arrive(i, first, last):
        mate_copy(pbuf, lin, psend, lrecv, i).wait_recv()
        if first:
            for k in range(3):
                first_copy(k).wait_recv()
        elif last:
            @pl.when(core == 0)
            def _():
                qx_copy.wait_recv()

            @pl.when(core == 1)
            def _():
                across_copy(final, end).wait_recv()
        else:
            for k in range(1, final):
                for sem, where in pieces(k):
                    @pl.when(i == where.start)
                    def _():
                        across_copy(sem, where).wait_recv()

            @pl.when(i == RELAY)
            def _():
                each_single(lambda copy: copy.wait_recv())

                @pl.when(col == 3)
                def _():
                    relay_copy(2).wait_recv()
        full = lbuf[i] + lin[i] + yin[i]
        parts = [full[:, k * LANES:(k + 1) * LANES] for k in range(TILES)]
        if first:
            parts[0] = parts[0] + first_in[...]
            edge_out[...] = parts[0]

            @pl.when(core == 1)
            def _():
                edge_copy.start()
        if last:
            @pl.when(core == 0)
            def _():
                edge_copy.wait_recv()

            parts[-1] = jnp.where(core == 0, edge_in[...], parts[-1])
        rolled = [pltpu.roll(part, turn, 1) for part in parts]
        tiles = [jnp.where(keep, rolled[k], rolled[k + 1]) for k in range(TILES - 1)]
        at = 0
        if not first:
            tiles = [jnp.where(keep, carry[...], rolled[0])] + tiles
            at = pl.multiple_of(i * CHUNK - LANES, LANES)
        carry[...] = rolled[-1]
        z_ref[:, pl.ds(at, LANES * len(tiles))] = jnp.concatenate(tiles, axis=1)
        top = tiles[0]
        for tile in tiles[1:]:
            top = jnp.maximum(top, tile)
        if not first:
            top = jnp.maximum(top, m_ref[...])
        mass = jnp.exp(tiles[0] - top)
        for tile in tiles[1:]:
            mass = mass + jnp.exp(tile - top)
        if not first:
            mass = mass + s_ref[...] * jnp.exp(m_ref[...] - top)
        m_ref[...] = top
        s_ref[...] = mass

    far_step(0, 0)
    first_copy(0).start()
    rbuf[0] = product("across", 0)
    first_copy(1).start()
    refill("across", 0)

    @pl.when(col < 3)
    def _():
        pl.semaphore_wait(hops.at[0], 1)

    tell_columns(hops.at[1])
    far_step(1, RELAY)
    mate_copy(qbuf, rin, qsend, rrecv, 0).wait_recv()
    rbuf[0, :, LANES:] = rbuf[0, :, LANES:] + rin[0, :, LANES:]
    first_copy(2).start()
    far_step(2, 1)
    pl.semaphore_wait(hops.at[1], beside)
    tell_columns(hops.at[2])
    far_step(3, 2)
    across_step(1, RELAY)
    pl.semaphore_wait(hops.at[2], beside)
    tell_columns(hops.at[3])
    each_single(lambda copy: copy.start())

    @pl.when(col == 3)
    def _():
        relay_copy(0).start()

    @pl.loop(2, end)
    def _(t):
        @pl.when(t < end - 1)
        def _():
            far_step(t + 2, chunk_at(t + 2))

        i = chunk_at(t)
        across_step(t, i)
        for k in range(1, final):
            for sem, where in pieces(k):
                @pl.when(i == where.start + where.size - 1)
                def _():
                    across_copy(sem, where).start()

        @pl.when((t == RELAY_AT) & (col == 0))
        def _():
            relay_copy(0).wait_recv()
            relay_copy(1).start()

    last_step()

    @pl.loop(0, count)
    def _(i):
        mate_step(i)
        own_step(i)

    @pl.when(col == 0)
    def _():
        relay_copy(1).wait_recv()
        relay_copy(2).start()

    pl.semaphore_wait(hops.at[3], beside)
    arrive(0, True, False)

    @pl.loop(1, end)
    def _(i):
        arrive(i, False, False)

    arrive(end, False, True)

    last = carry[...]
    z_ref[:, stride:] = last[:, :rest]
    last = jnp.where(lane < rest, last, -jnp.inf)
    top = jnp.maximum(m_ref[...], last)
    mass = s_ref[...] * jnp.exp(m_ref[...] - top) + jnp.exp(last - top)
    top = jnp.transpose(jnp.concatenate([top, top], axis=0))
    mass = jnp.transpose(jnp.concatenate([mass, mass], axis=0))
    peak = jnp.max(top, axis=0, keepdims=True)
    mass = jnp.sum(mass * jnp.exp(top - peak), axis=0, keepdims=True)
    me = col * 4 + row
    fst[me] = jnp.where(lane[:1] < rows, peak, mass)

    def stat_copy(c, dr, slot):
        return pltpu.make_async_remote_copy(
            src_ref=fst.at[slot], dst_ref=fst.at[slot], send_sem=fsend.at[c * 4 + dr], recv_sem=frecv.at[slot],
            device_id={"col": c, "row": lax.rem(row + dr, 4)}, device_id_type=MESH,
        )

    def each_peer(act):
        for c in range(4):
            for dr in (2, 3, 1):
                act(c, dr)

            @pl.when(col != c)
            def _():
                act(c, 0)

    each_peer(lambda c, dr: stat_copy(c, dr, me).start())
    each_peer(lambda c, dr: stat_copy(c, dr, c * 4 + lax.rem(row + dr, 4)).wait_recv())
    stats = fst[...]
    swapped = pltpu.roll(stats, LANES // 2, 2)
    peak = jnp.max(stats, axis=0)
    mass = jnp.sum(swapped * jnp.exp(stats - peak), axis=0)
    lse_ref[...] = peak + jnp.log(mass)

    for k in range(1, 4):
        norm_copy(k).wait_send()
    for src, dst, send, recv in ((qbuf, rin, qsend, rrecv), (pbuf, lin, psend, lrecv)):
        pltpu.make_async_remote_copy(
            src_ref=src, dst_ref=dst, send_sem=send, recv_sem=recv.at[0],
            device_id={"row": mate}, device_id_type=MESH,
        ).wait_send()
    for k in range(3):
        first_copy(k).wait_send()
    for k in range(1, final):
        each_group(k, lambda copy: copy.wait_send())
    each_single(lambda copy: copy.wait_send())

    @pl.when(core == 0)
    def _():
        rx_copy.wait_send()

    @pl.when(core == 1)
    def _():
        qx_copy.wait_send()
        across_copy(final, end).wait_send()

    @pl.when(col == 3)
    def _():
        relay_copy(0).wait_send()

    @pl.when(col == 0)
    def _():
        relay_copy(1).wait_send()
        relay_copy(2).wait_send()

    @pl.when(core == 1)
    def _():
        edge_copy.wait_send()

    each_peer(lambda c, dr: stat_copy(c, dr, me).wait_send())


def solution(mesh):
    def local_head(hidden, norm_gain, w_head):
        rows, feats = hidden.shape
        width = w_head.shape[1] // 4
        count = (width // LANES + 1) // TILES
        block = (count, rows, CHUNK)
        dma = pltpu.SemaphoreType.DMA

        def body(*refs):
            head_kernel(count, width, feats * 4, *refs)

        z, lse = pl.pallas_call(
            body,
            out_shape=(
                jax.ShapeDtypeStruct((rows, width), jnp.float32),
                jax.ShapeDtypeStruct((1, LANES), jnp.float32),
            ),
            in_specs=[
                pl.BlockSpec(memory_space=pltpu.HBM),
                pl.BlockSpec(memory_space=pltpu.HBM),
                pl.BlockSpec(memory_space=pltpu.HBM),
            ],
            out_specs=(pl.BlockSpec(memory_space=pltpu.VMEM), pl.BlockSpec(memory_space=pltpu.VMEM)),
            scratch_shapes=[
                pltpu.VMEM((rows, feats), hidden.dtype),
                pltpu.VMEM((feats,), jnp.float32),
                *[pltpu.VMEM((SLOTS, feats, CHUNK), jnp.bfloat16) for _ in range(4)],
                pltpu.VMEM((rows, feats), jnp.bfloat16),
                *[pltpu.VMEM(block, jnp.float32) for _ in range(7)],
                pltpu.VMEM((4, 1, LANES), jnp.float32),
                pltpu.VMEM((16, 1, LANES), jnp.float32),
                *[pltpu.VMEM((rows, LANES), jnp.float32) for _ in range(5)],
                *[pltpu.VMEM((rows, (TILES - 1) * LANES), jnp.float32) for _ in range(4)],
                pltpu.VMEM((rows, LANES), jnp.float32),
                dma, dma, pltpu.SemaphoreType.REGULAR((4,)),
                *[dma((SLOTS,)) for _ in range(4)], dma((4,)), dma((4,)),
                dma, dma, dma((len(GROUPS) + 2,)), dma((count,)), dma((count,)), dma((len(GROUPS) + 2,)), dma((16,)), dma((16,)), dma, dma, dma((3,)), dma((3,)), dma, dma, dma,
                dma((3,)), dma((3,)),
            ],
            compiler_params=pltpu.CompilerParams(
                collective_id=0, has_side_effects=True, vmem_limit_bytes=48 * 1024 * 1024
            ),
            name="head",
        )(pltpu.with_memory_space_constraint(hidden, pltpu.HBM), pltpu.with_memory_space_constraint(norm_gain, pltpu.HBM), w_head)
        log_norm = lse[0, :rows]
        return z - log_norm[:, None], log_norm

    return jax.shard_map(
        local_head,
        mesh=mesh,
        in_specs=(P("dp", "row"), P("row"), P("row", "col")),
        out_specs=(P("dp", ("col", "row")), P("dp")),
        check_vma=False,
    )
```

```python
import jax
import jax.numpy as jnp
from jax import lax
from jax.experimental import pallas as pl
from jax.experimental.pallas import tpu as pltpu
from jax.sharding import PartitionSpec as P

EPS = 1e-5
MESH = pl.DeviceIdType.MESH
LANES = 128
TILES = 3
CHUNK = TILES * LANES
SLOTS = 4
GROUPS = ((0,), (1, 2), (3, 7), (8, 17), (18, 23), (24,))
RELAY = 12
RELAY_AT = 14


def head_kernel(
    count, width, hidden_size,
    h_hbm, g_hbm, w_ref, z_ref, lse_ref,
    h_ref, g_ref, wq, wr, wp, wl, x_ref, qbuf, rbuf, pbuf, lbuf, rin, lin, yin, nst, fst, m_ref, s_ref, carry, edge_out, edge_in, relay_in, relay_mid, rx, qx, first_in,
    h_sem, g_sem, hops, wq_sem, wr_sem, wp_sem, wl_sem, nsend, nrecv, qsend, psend, ysend, rrecv, lrecv, yrecv, fsend, frecv, esend, erecv, relay_send, relay_recv, rx_send, rx_recv, qx_send, first_send, first_recv,
):
    rows, feats = h_ref.shape
    stride = (width // LANES) * LANES
    rest = width - stride
    col = lax.axis_index("col")
    row = lax.axis_index("row")
    core = lax.rem(row, 2)
    mate = row + 1 - 2 * core
    across = lax.rem(row + 2, 4)
    far = 3 - row
    shift = row * rest

    end = count - 1

    streams = {
        "far": (far, wq, wq_sem), "across": (across, wr, wr_sem), "mate": (mate, wp, wp_sem), "own": (row, wl, wl_sem)
    }

    def chunk_at(t):
        if isinstance(t, int) and t < 2:
            return t * RELAY
        return t - 1 + t // (RELAY + 1)

    def fetch(name, t):
        part, buf, sem = streams[name]
        chunk = t
        if name in ("far", "across"):
            chunk = chunk_at(t)
        start = pl.multiple_of(stride * part + CHUNK * chunk, LANES)
        slot = lax.rem(t, SLOTS)
        return pltpu.make_async_copy(w_ref.at[:, pl.ds(start, CHUNK)], buf.at[slot], sem.at[slot])

    barrier = pltpu.get_barrier_semaphore()

    def tell_column(sem, step):
        @pl.when((col + step >= 0) & (col + step < 4))
        def _():
            pl.semaphore_signal(sem, inc=1, device_id_type=MESH, device_id={"col": col + step})

    def tell_columns(sem):
        tell_column(sem, -1)
        tell_column(sem, 1)

    for k in (2, 3, 1):
        pl.semaphore_signal(barrier, inc=1, device_id_type=MESH, device_id={"row": lax.rem(row + k, 4)})
    tell_column(barrier, 1)
    below = (col + 2) // 3
    above = (5 - col) // 3
    beside = below + above

    h_copy = pltpu.make_async_copy(h_hbm, h_ref, h_sem)
    g_copy = pltpu.make_async_copy(g_hbm, g_ref, g_sem)
    h_copy.start()
    g_copy.start()
    h_copy.wait()
    for name, t in (("far", 0), ("far", 1), ("across", 0)):
        fetch(name, t).start()

    lane = lax.broadcasted_iota(jnp.int32, (rows, LANES), 1)
    sq = jnp.zeros((rows, LANES), jnp.float32)
    for j in range(feats // LANES):
        part = h_ref[:, j * LANES:(j + 1) * LANES].astype(jnp.float32)
        sq = sq + part * part
    sq = jnp.transpose(jnp.concatenate([sq, sq], axis=0))
    nst[row] = jnp.sum(sq, axis=0, keepdims=True)
    pl.semaphore_wait(barrier, 3 + below)
    tell_column(hops.at[0], -1)

    def norm_copy(k):
        return pltpu.make_async_remote_copy(
            src_ref=nst.at[row], dst_ref=nst.at[row], send_sem=nsend.at[k], recv_sem=nrecv.at[row],
            device_id={"row": lax.rem(row + k, 4)}, device_id_type=MESH,
        )

    for k in (2, 3, 1):
        norm_copy(k).start()
    for name, t in (
        *[(n, t) for t in range(1, SLOTS) for n in ("far", "across") if n == "across" or t > 1], *[(n, t) for t in range(SLOTS) for n in ("mate", "own")]
    ):
        fetch(name, t).start()
    for k in range(1, 4):
        peer = lax.rem(row + k, 4)
        pltpu.make_async_remote_copy(
            src_ref=nst.at[peer], dst_ref=nst.at[peer], send_sem=nsend.at[k], recv_sem=nrecv.at[peer],
            device_id={"row": peer}, device_id_type=MESH,
        ).wait_recv()
    g_copy.wait()
    total = nst[0] + nst[1] + nst[2] + nst[3]
    scale = lax.rsqrt(total / hidden_size + EPS)
    scale = jnp.transpose(jnp.broadcast_to(scale, (LANES, LANES)))[:rows]
    for j in range(feats // LANES):
        cols = slice(j * LANES, (j + 1) * LANES)
        x_ref[:, cols] = (h_ref[:, cols].astype(jnp.float32) * scale * g_ref[cols].reshape(1, LANES)).astype(jnp.bfloat16)

    def product(name, t):
        fetch(name, t).wait()
        return jnp.dot(x_ref[...], streams[name][1][lax.rem(t, SLOTS)], preferred_element_type=jnp.float32)

    def refill(name, t):
        @pl.when(t + SLOTS < count)
        def _():
            fetch(name, t + SLOTS).start()

    def mate_copy(src, dst, send, recv, i):
        return pltpu.make_async_remote_copy(
            src_ref=src.at[i], dst_ref=dst.at[i], send_sem=send, recv_sem=recv.at[i],
            device_id={"row": mate}, device_id_type=MESH,
        )

    most = pl.ds(0, (TILES - 1) * LANES)
    final = len(GROUPS) - 1

    def across_copy(k, where):
        return pltpu.make_async_remote_copy(
            src_ref=rbuf.at[where], dst_ref=yin.at[where], send_sem=ysend.at[k], recv_sem=yrecv.at[k],
            device_id={"row": across}, device_id_type=MESH,
        )

    def pieces(k):
        lo, hi = GROUPS[k][0], GROUPS[k][-1]
        if lo <= RELAY <= hi:
            return [(k, pl.ds(lo, RELAY - lo)), (len(GROUPS), pl.ds(RELAY + 1, hi - RELAY))]
        return [(k, pl.ds(lo, hi - lo + 1))]

    rx_copy = pltpu.make_async_remote_copy(
        src_ref=rbuf.at[end, :, most], dst_ref=rx, send_sem=rx_send, recv_sem=rx_recv,
        device_id={"row": mate}, device_id_type=MESH,
    )
    qx_copy = pltpu.make_async_remote_copy(
        src_ref=qx, dst_ref=yin.at[end, :, most], send_sem=qx_send, recv_sem=yrecv.at[final],
        device_id={"row": far}, device_id_type=MESH,
    )

    lead = pl.ds(0, LANES)
    rest_of = pl.ds(LANES, (TILES - 1) * LANES)

    def first_copy(k):
        src, dst, device = (
            (qbuf.at[0, :, lead], first_in, far),
            (rbuf.at[0, :, lead], yin.at[0, :, lead], across),
            (rbuf.at[0, :, rest_of], yin.at[0, :, rest_of], across),
        )[k]
        return pltpu.make_async_remote_copy(
            src_ref=src, dst_ref=dst, send_sem=first_send.at[k], recv_sem=first_recv.at[k],
            device_id={"row": device}, device_id_type=MESH,
        )

    def last_step():
        rbuf[end] = product("across", end)

        @pl.when(core == 0)
        def _():
            rx_copy.start()

        mate_copy(qbuf, rin, qsend, rrecv, end).wait_recv()

        @pl.when(core == 1)
        def _():
            rx_copy.wait_recv()
            qx[...] = qbuf[end, :, most] + rx[...]
            qx_copy.start()
            rbuf[end] = rbuf[end] + rin[end]
            across_copy(final, end).start()

    def each_group(k, act):
        for sem, where in pieces(k):
            act(across_copy(sem, where))

    def each_single(act):
        @pl.when(col < 3)
        def _():
            act(across_copy(len(GROUPS) + 1, RELAY))

        @pl.when(col == 3)
        def _():
            act(across_copy(len(GROUPS) + 1, (RELAY, slice(None), pl.ds((TILES - 1) * LANES, LANES))))

    def relay_copy(k):
        src, dst, device = (
            (rbuf.at[RELAY, :, most], relay_in, {"col": 0}),
            (relay_in, relay_mid, {"row": across}),
            (relay_mid, yin.at[RELAY, :, most], {"col": 3}),
        )[k]
        return pltpu.make_async_remote_copy(
            src_ref=src, dst_ref=dst, send_sem=relay_send.at[k], recv_sem=relay_recv.at[k],
            device_id=device, device_id_type=MESH,
        )

    edge_copy = pltpu.make_async_remote_copy(
        src_ref=edge_out, dst_ref=edge_in, send_sem=esend, recv_sem=erecv,
        device_id={"row": mate}, device_id_type=MESH,
    )

    def far_step(t, i):
        qbuf[i] = product("far", t)
        mate_copy(qbuf, rin, qsend, rrecv, i).start()
        refill("far", t)

    def across_step(t, i):
        term = product("across", t)
        refill("across", t)
        mate_copy(qbuf, rin, qsend, rrecv, i).wait_recv()
        rbuf[i] = term + rin[i]

    def mate_step(i):
        pbuf[i] = product("mate", i)
        mate_copy(pbuf, lin, psend, lrecv, i).start()
        refill("mate", i)

    def own_step(i):
        lbuf[i] = product("own", i)
        refill("own", i)

    turn = lax.rem(LANES - shift, LANES)
    keep = lane < LANES - shift

    def arrive(i, first, last):
        mate_copy(pbuf, lin, psend, lrecv, i).wait_recv()
        if first:
            for k in range(3):
                first_copy(k).wait_recv()
        elif last:
            @pl.when(core == 0)
            def _():
                qx_copy.wait_recv()

            @pl.when(core == 1)
            def _():
                across_copy(final, end).wait_recv()
        else:
            for k in range(1, final):
                for sem, where in pieces(k):
                    @pl.when(i == where.start)
                    def _():
                        across_copy(sem, where).wait_recv()

            @pl.when(i == RELAY)
            def _():
                each_single(lambda copy: copy.wait_recv())

                @pl.when(col == 3)
                def _():
                    relay_copy(2).wait_recv()
        full = lbuf[i] + lin[i] + yin[i]
        parts = [full[:, k * LANES:(k + 1) * LANES] for k in range(TILES)]
        if first:
            parts[0] = parts[0] + first_in[...]
            edge_out[...] = parts[0]

            @pl.when(core == 1)
            def _():
                edge_copy.start()
        if last:
            @pl.when(core == 0)
            def _():
                edge_copy.wait_recv()

            parts[-1] = jnp.where(core == 0, edge_in[...], parts[-1])
        rolled = [pltpu.roll(part, turn, 1) for part in parts]
        tiles = [jnp.where(keep, rolled[k], rolled[k + 1]) for k in range(TILES - 1)]
        at = 0
        if not first:
            tiles = [jnp.where(keep, carry[...], rolled[0])] + tiles
            at = pl.multiple_of(i * CHUNK - LANES, LANES)
        carry[...] = rolled[-1]
        z_ref[:, pl.ds(at, LANES * len(tiles))] = jnp.concatenate(tiles, axis=1)
        top = tiles[0]
        for tile in tiles[1:]:
            top = jnp.maximum(top, tile)
        if not first:
            top = jnp.maximum(top, m_ref[...])
        mass = jnp.exp(tiles[0] - top)
        for tile in tiles[1:]:
            mass = mass + jnp.exp(tile - top)
        if not first:
            mass = mass + s_ref[...] * jnp.exp(m_ref[...] - top)
        m_ref[...] = top
        s_ref[...] = mass

    far_step(0, 0)
    first_copy(0).start()
    rbuf[0] = product("across", 0)
    first_copy(1).start()
    refill("across", 0)

    @pl.when(col < 3)
    def _():
        pl.semaphore_wait(hops.at[0], 1)

    tell_columns(hops.at[1])
    far_step(1, RELAY)
    mate_copy(qbuf, rin, qsend, rrecv, 0).wait_recv()
    rbuf[0, :, LANES:] = rbuf[0, :, LANES:] + rin[0, :, LANES:]
    first_copy(2).start()
    far_step(2, 1)
    pl.semaphore_wait(hops.at[1], beside)
    tell_columns(hops.at[2])
    far_step(3, 2)
    across_step(1, RELAY)
    pl.semaphore_wait(hops.at[2], beside)
    tell_columns(hops.at[3])
    each_single(lambda copy: copy.start())

    @pl.when(col == 3)
    def _():
        relay_copy(0).start()

    @pl.loop(2, end)
    def _(t):
        @pl.when(t < end - 1)
        def _():
            far_step(t + 2, chunk_at(t + 2))

        i = chunk_at(t)
        across_step(t, i)
        for k in range(1, final):
            for sem, where in pieces(k):
                @pl.when(i == where.start + where.size - 1)
                def _():
                    across_copy(sem, where).start()

        @pl.when((t == RELAY_AT) & (col == 0))
        def _():
            relay_copy(0).wait_recv()
            relay_copy(1).start()

    last_step()

    @pl.loop(0, count)
    def _(i):
        mate_step(i)
        own_step(i)

    @pl.when(col == 0)
    def _():
        relay_copy(1).wait_recv()
        relay_copy(2).start()

    pl.semaphore_wait(hops.at[3], beside)
    arrive(0, True, False)

    @pl.loop(1, end)
    def _(i):
        arrive(i, False, False)

    arrive(end, False, True)

    last = carry[...]
    z_ref[:, stride:] = last[:, :rest]
    last = jnp.where(lane < rest, last, -jnp.inf)
    top = jnp.maximum(m_ref[...], last)
    mass = s_ref[...] * jnp.exp(m_ref[...] - top) + jnp.exp(last - top)
    top = jnp.transpose(jnp.concatenate([top, top], axis=0))
    mass = jnp.transpose(jnp.concatenate([mass, mass], axis=0))
    peak = jnp.max(top, axis=0, keepdims=True)
    mass = jnp.sum(mass * jnp.exp(top - peak), axis=0, keepdims=True)
    me = col * 4 + row
    fst[me] = jnp.where(lane[:1] < rows, peak, mass)

    def stat_copy(c, dr, slot):
        return pltpu.make_async_remote_copy(
            src_ref=fst.at[slot], dst_ref=fst.at[slot], send_sem=fsend.at[c * 4 + dr], recv_sem=frecv.at[slot],
            device_id={"col": c, "row": lax.rem(row + dr, 4)}, device_id_type=MESH,
        )

    def each_peer(act):
        for c in range(4):
            for dr in (2, 3, 1):
                act(c, dr)

            @pl.when(col != c)
            def _():
                act(c, 0)

    each_peer(lambda c, dr: stat_copy(c, dr, me).start())
    each_peer(lambda c, dr: stat_copy(c, dr, c * 4 + lax.rem(row + dr, 4)).wait_recv())
    stats = fst[...]
    swapped = pltpu.roll(stats, LANES // 2, 2)
    peak = jnp.max(stats, axis=0)
    mass = jnp.sum(swapped * jnp.exp(stats - peak), axis=0)
    lse_ref[...] = peak + jnp.log(mass)

    for k in range(1, 4):
        norm_copy(k).wait_send()
    for src, dst, send, recv in ((qbuf, rin, qsend, rrecv), (pbuf, lin, psend, lrecv)):
        pltpu.make_async_remote_copy(
            src_ref=src, dst_ref=dst, send_sem=send, recv_sem=recv.at[0],
            device_id={"row": mate}, device_id_type=MESH,
        ).wait_send()
    for k in range(3):
        first_copy(k).wait_send()
    for k in range(1, final):
        each_group(k, lambda copy: copy.wait_send())
    each_single(lambda copy: copy.wait_send())

    @pl.when(core == 0)
    def _():
        rx_copy.wait_send()

    @pl.when(core == 1)
    def _():
        qx_copy.wait_send()
        across_copy(final, end).wait_send()

    @pl.when(col == 3)
    def _():
        relay_copy(0).wait_send()

    @pl.when(col == 0)
    def _():
        relay_copy(1).wait_send()
        relay_copy(2).wait_send()

    @pl.when(core == 1)
    def _():
        edge_copy.wait_send()

    each_peer(lambda c, dr: stat_copy(c, dr, me).wait_send())


def solution(mesh):
    def local_head(hidden, norm_gain, w_head):
        rows, feats = hidden.shape
        width = w_head.shape[1] // 4
        count = (width // LANES + 1) // TILES
        block = (count, rows, CHUNK)
        dma = pltpu.SemaphoreType.DMA

        def body(*refs):
            head_kernel(count, width, feats * 4, *refs)

        z, lse = pl.pallas_call(
            body,
            out_shape=(
                jax.ShapeDtypeStruct((rows, width), jnp.float32),
                jax.ShapeDtypeStruct((1, LANES), jnp.float32),
            ),
            in_specs=[
                pl.BlockSpec(memory_space=pltpu.HBM),
                pl.BlockSpec(memory_space=pltpu.HBM),
                pl.BlockSpec(memory_space=pltpu.HBM),
            ],
            out_specs=(pl.BlockSpec(memory_space=pltpu.VMEM), pl.BlockSpec(memory_space=pltpu.VMEM)),
            scratch_shapes=[
                pltpu.VMEM((rows, feats), hidden.dtype),
                pltpu.VMEM((feats,), jnp.float32),
                *[pltpu.VMEM((SLOTS, feats, CHUNK), jnp.bfloat16) for _ in range(4)],
                pltpu.VMEM((rows, feats), jnp.bfloat16),
                *[pltpu.VMEM(block, jnp.float32) for _ in range(7)],
                pltpu.VMEM((4, 1, LANES), jnp.float32),
                pltpu.VMEM((16, 1, LANES), jnp.float32),
                *[pltpu.VMEM((rows, LANES), jnp.float32) for _ in range(5)],
                *[pltpu.VMEM((rows, (TILES - 1) * LANES), jnp.float32) for _ in range(4)],
                pltpu.VMEM((rows, LANES), jnp.float32),
                dma, dma, pltpu.SemaphoreType.REGULAR((4,)),
                *[dma((SLOTS,)) for _ in range(4)], dma((4,)), dma((4,)),
                dma, dma, dma((len(GROUPS) + 2,)), dma((count,)), dma((count,)), dma((len(GROUPS) + 2,)), dma((16,)), dma((16,)), dma, dma, dma((3,)), dma((3,)), dma, dma, dma,
                dma((3,)), dma((3,)),
            ],
            compiler_params=pltpu.CompilerParams(
                collective_id=0, has_side_effects=True, vmem_limit_bytes=48 * 1024 * 1024
            ),
            name="head",
        )(pltpu.with_memory_space_constraint(hidden, pltpu.HBM), pltpu.with_memory_space_constraint(norm_gain, pltpu.HBM), w_head)
        log_norm = lse[0, :rows]
        return z - log_norm[:, None], log_norm

    return jax.shard_map(
        local_head,
        mesh=mesh,
        in_specs=(P("dp", "row"), P("row"), P("row", "col")),
        out_specs=(P("dp", ("col", "row")), P("dp")),
        check_vma=False,
    )
```

```python
import jax
import jax.numpy as jnp
from jax import lax
from jax.experimental import pallas as pl
from jax.experimental.pallas import tpu as pltpu
from jax.sharding import PartitionSpec as P

EPS = 1e-5
MESH = pl.DeviceIdType.MESH
LANES = 128
TILES = 3
CHUNK = TILES * LANES
SLOTS = 4
GROUPS = ((0,), (1, 2), (3, 7), (8, 17), (18, 23), (24,))
RELAY = 12
RELAY_AT = 14


def head_kernel(
    count, width, hidden_size,
    h_hbm, g_hbm, w_ref, z_ref, lse_ref,
    h_ref, g_ref, wq, wr, wp, wl, x_ref, qbuf, rbuf, pbuf, lbuf, rin, lin, yin, nst, fst, m_ref, s_ref, carry, edge_out, edge_in, relay_in, relay_mid, rx, qx, first_in,
    h_sem, g_sem, hops, wq_sem, wr_sem, wp_sem, wl_sem, nsend, nrecv, qsend, psend, ysend, rrecv, lrecv, yrecv, fsend, frecv, esend, erecv, relay_send, relay_recv, rx_send, rx_recv, qx_send, first_send, first_recv,
):
    rows, feats = h_ref.shape
    stride = (width // LANES) * LANES
    rest = width - stride
    col = lax.axis_index("col")
    row = lax.axis_index("row")
    core = lax.rem(row, 2)
    mate = row + 1 - 2 * core
    across = lax.rem(row + 2, 4)
    far = 3 - row
    shift = row * rest

    end = count - 1

    streams = {
        "far": (far, wq, wq_sem), "across": (across, wr, wr_sem), "mate": (mate, wp, wp_sem), "own": (row, wl, wl_sem)
    }

    def chunk_at(t):
        if isinstance(t, int) and t < 2:
            return t * RELAY
        return t - 1 + t // (RELAY + 1)

    def fetch(name, t):
        part, buf, sem = streams[name]
        chunk = t
        if name in ("far", "across"):
            chunk = chunk_at(t)
        start = pl.multiple_of(stride * part + CHUNK * chunk, LANES)
        slot = lax.rem(t, SLOTS)
        return pltpu.make_async_copy(w_ref.at[:, pl.ds(start, CHUNK)], buf.at[slot], sem.at[slot])

    barrier = pltpu.get_barrier_semaphore()

    def tell_column(sem, step):
        @pl.when((col + step >= 0) & (col + step < 4))
        def _():
            pl.semaphore_signal(sem, inc=1, device_id_type=MESH, device_id={"col": col + step})

    def tell_columns(sem):
        tell_column(sem, -1)
        tell_column(sem, 1)

    for k in (2, 3, 1):
        pl.semaphore_signal(barrier, inc=1, device_id_type=MESH, device_id={"row": lax.rem(row + k, 4)})
    tell_column(barrier, 1)
    below = (col + 2) // 3
    above = (5 - col) // 3
    beside = below + above

    h_copy = pltpu.make_async_copy(h_hbm, h_ref, h_sem)
    g_copy = pltpu.make_async_copy(g_hbm, g_ref, g_sem)
    h_copy.start()
    g_copy.start()
    h_copy.wait()
    for name, t in (("far", 0), ("far", 1), ("across", 0)):
        fetch(name, t).start()

    lane = lax.broadcasted_iota(jnp.int32, (rows, LANES), 1)
    sq = jnp.zeros((rows, LANES), jnp.float32)
    for j in range(feats // LANES):
        part = h_ref[:, j * LANES:(j + 1) * LANES].astype(jnp.float32)
        sq = sq + part * part
    sq = jnp.transpose(jnp.concatenate([sq, sq], axis=0))
    nst[row] = jnp.sum(sq, axis=0, keepdims=True)
    pl.semaphore_wait(barrier, 3 + below)
    tell_column(hops.at[0], -1)

    def norm_copy(k):
        return pltpu.make_async_remote_copy(
            src_ref=nst.at[row], dst_ref=nst.at[row], send_sem=nsend.at[k], recv_sem=nrecv.at[row],
            device_id={"row": lax.rem(row + k, 4)}, device_id_type=MESH,
        )

    for k in (2, 3, 1):
        norm_copy(k).start()
    for name, t in (
        *[(n, t) for t in range(1, SLOTS) for n in ("far", "across") if n == "across" or t > 1], *[(n, t) for t in range(SLOTS) for n in ("mate", "own")]
    ):
        fetch(name, t).start()
    for k in range(1, 4):
        peer = lax.rem(row + k, 4)
        pltpu.make_async_remote_copy(
            src_ref=nst.at[peer], dst_ref=nst.at[peer], send_sem=nsend.at[k], recv_sem=nrecv.at[peer],
            device_id={"row": peer}, device_id_type=MESH,
        ).wait_recv()
    g_copy.wait()
    total = nst[0] + nst[1] + nst[2] + nst[3]
    scale = lax.rsqrt(total / hidden_size + EPS)
    scale = jnp.transpose(jnp.broadcast_to(scale, (LANES, LANES)))[:rows]
    for j in range(feats // LANES):
        cols = slice(j * LANES, (j + 1) * LANES)
        x_ref[:, cols] = (h_ref[:, cols].astype(jnp.float32) * scale * g_ref[cols].reshape(1, LANES)).astype(jnp.bfloat16)

    def product(name, t):
        fetch(name, t).wait()
        return jnp.dot(x_ref[...], streams[name][1][lax.rem(t, SLOTS)], preferred_element_type=jnp.float32)

    def refill(name, t):
        @pl.when(t + SLOTS < count)
        def _():
            fetch(name, t + SLOTS).start()

    def mate_copy(src, dst, send, recv, i):
        return pltpu.make_async_remote_copy(
            src_ref=src.at[i], dst_ref=dst.at[i], send_sem=send, recv_sem=recv.at[i],
            device_id={"row": mate}, device_id_type=MESH,
        )

    most = pl.ds(0, (TILES - 1) * LANES)
    final = len(GROUPS) - 1

    def across_copy(k, where):
        return pltpu.make_async_remote_copy(
            src_ref=rbuf.at[where], dst_ref=yin.at[where], send_sem=ysend.at[k], recv_sem=yrecv.at[k],
            device_id={"row": across}, device_id_type=MESH,
        )

    def pieces(k):
        lo, hi = GROUPS[k][0], GROUPS[k][-1]
        if lo <= RELAY <= hi:
            return [(k, pl.ds(lo, RELAY - lo)), (len(GROUPS), pl.ds(RELAY + 1, hi - RELAY))]
        return [(k, pl.ds(lo, hi - lo + 1))]

    rx_copy = pltpu.make_async_remote_copy(
        src_ref=rbuf.at[end, :, most], dst_ref=rx, send_sem=rx_send, recv_sem=rx_recv,
        device_id={"row": mate}, device_id_type=MESH,
    )
    qx_copy = pltpu.make_async_remote_copy(
        src_ref=qx, dst_ref=yin.at[end, :, most], send_sem=qx_send, recv_sem=yrecv.at[final],
        device_id={"row": far}, device_id_type=MESH,
    )

    lead = pl.ds(0, LANES)
    rest_of = pl.ds(LANES, (TILES - 1) * LANES)

    def first_copy(k):
        src, dst, device = (
            (qbuf.at[0, :, lead], first_in, far),
            (rbuf.at[0, :, lead], yin.at[0, :, lead], across),
            (rbuf.at[0, :, rest_of], yin.at[0, :, rest_of], across),
        )[k]
        return pltpu.make_async_remote_copy(
            src_ref=src, dst_ref=dst, send_sem=first_send.at[k], recv_sem=first_recv.at[k],
            device_id={"row": device}, device_id_type=MESH,
        )

    def last_step():
        rbuf[end] = product("across", end)

        @pl.when(core == 0)
        def _():
            rx_copy.start()

        mate_copy(qbuf, rin, qsend, rrecv, end).wait_recv()

        @pl.when(core == 1)
        def _():
            rx_copy.wait_recv()
            qx[...] = qbuf[end, :, most] + rx[...]
            qx_copy.start()
            rbuf[end] = rbuf[end] + rin[end]
            across_copy(final, end).start()

    def each_group(k, act):
        for sem, where in pieces(k):
            act(across_copy(sem, where))

    def each_single(act):
        @pl.when(col < 3)
        def _():
            act(across_copy(len(GROUPS) + 1, RELAY))

        @pl.when(col == 3)
        def _():
            act(across_copy(len(GROUPS) + 1, (RELAY, slice(None), pl.ds((TILES - 1) * LANES, LANES))))

    def relay_copy(k):
        src, dst, device = (
            (rbuf.at[RELAY, :, most], relay_in, {"col": core}),
            (relay_in, relay_mid, {"row": across}),
            (relay_mid, yin.at[RELAY, :, most], {"col": 3}),
        )[k]
        return pltpu.make_async_remote_copy(
            src_ref=src, dst_ref=dst, send_sem=relay_send.at[k], recv_sem=relay_recv.at[k],
            device_id=device, device_id_type=MESH,
        )

    edge_copy = pltpu.make_async_remote_copy(
        src_ref=edge_out, dst_ref=edge_in, send_sem=esend, recv_sem=erecv,
        device_id={"row": mate}, device_id_type=MESH,
    )

    def far_step(t, i):
        qbuf[i] = product("far", t)
        mate_copy(qbuf, rin, qsend, rrecv, i).start()
        refill("far", t)

    def across_step(t, i):
        term = product("across", t)
        refill("across", t)
        mate_copy(qbuf, rin, qsend, rrecv, i).wait_recv()
        rbuf[i] = term + rin[i]

    def mate_step(i):
        pbuf[i] = product("mate", i)
        mate_copy(pbuf, lin, psend, lrecv, i).start()
        refill("mate", i)

    def own_step(i):
        lbuf[i] = product("own", i)
        refill("own", i)

    turn = lax.rem(LANES - shift, LANES)
    keep = lane < LANES - shift

    def arrive(i, first, last):
        mate_copy(pbuf, lin, psend, lrecv, i).wait_recv()
        if first:
            for k in range(3):
                first_copy(k).wait_recv()
        elif last:
            @pl.when(core == 0)
            def _():
                qx_copy.wait_recv()

            @pl.when(core == 1)
            def _():
                across_copy(final, end).wait_recv()
        else:
            for k in range(1, final):
                for sem, where in pieces(k):
                    @pl.when(i == where.start)
                    def _():
                        across_copy(sem, where).wait_recv()

            @pl.when(i == RELAY)
            def _():
                each_single(lambda copy: copy.wait_recv())

                @pl.when(col == 3)
                def _():
                    relay_copy(2).wait_recv()
        full = lbuf[i] + lin[i] + yin[i]
        parts = [full[:, k * LANES:(k + 1) * LANES] for k in range(TILES)]
        if first:
            parts[0] = parts[0] + first_in[...]
            edge_out[...] = parts[0]

            @pl.when(core == 1)
            def _():
                edge_copy.start()
        if last:
            @pl.when(core == 0)
            def _():
                edge_copy.wait_recv()

            parts[-1] = jnp.where(core == 0, edge_in[...], parts[-1])
        rolled = [pltpu.roll(part, turn, 1) for part in parts]
        tiles = [jnp.where(keep, rolled[k], rolled[k + 1]) for k in range(TILES - 1)]
        at = 0
        if not first:
            tiles = [jnp.where(keep, carry[...], rolled[0])] + tiles
            at = pl.multiple_of(i * CHUNK - LANES, LANES)
        carry[...] = rolled[-1]
        z_ref[:, pl.ds(at, LANES * len(tiles))] = jnp.concatenate(tiles, axis=1)
        top = tiles[0]
        for tile in tiles[1:]:
            top = jnp.maximum(top, tile)
        if not first:
            top = jnp.maximum(top, m_ref[...])
        mass = jnp.exp(tiles[0] - top)
        for tile in tiles[1:]:
            mass = mass + jnp.exp(tile - top)
        if not first:
            mass = mass + s_ref[...] * jnp.exp(m_ref[...] - top)
        m_ref[...] = top
        s_ref[...] = mass

    far_step(0, 0)
    first_copy(0).start()
    rbuf[0] = product("across", 0)
    first_copy(1).start()
    refill("across", 0)

    @pl.when(col < 3)
    def _():
        pl.semaphore_wait(hops.at[0], 1)

    tell_columns(hops.at[1])
    far_step(1, RELAY)
    mate_copy(qbuf, rin, qsend, rrecv, 0).wait_recv()
    rbuf[0, :, LANES:] = rbuf[0, :, LANES:] + rin[0, :, LANES:]
    first_copy(2).start()
    far_step(2, 1)
    pl.semaphore_wait(hops.at[1], beside)
    tell_columns(hops.at[2])
    far_step(3, 2)
    across_step(1, RELAY)
    pl.semaphore_wait(hops.at[2], beside)
    tell_columns(hops.at[3])
    each_single(lambda copy: copy.start())

    @pl.when(col == 3)
    def _():
        relay_copy(0).start()

    @pl.loop(2, end)
    def _(t):
        @pl.when(t < end - 1)
        def _():
            far_step(t + 2, chunk_at(t + 2))

        i = chunk_at(t)
        across_step(t, i)
        for k in range(1, final):
            for sem, where in pieces(k):
                @pl.when(i == where.start + where.size - 1)
                def _():
                    across_copy(sem, where).start()

        @pl.when((t == RELAY_AT) & (col == core))
        def _():
            relay_copy(0).wait_recv()
            relay_copy(1).start()

    last_step()

    @pl.loop(0, count)
    def _(i):
        mate_step(i)
        own_step(i)

    @pl.when(col == core)
    def _():
        relay_copy(1).wait_recv()
        relay_copy(2).start()

    pl.semaphore_wait(hops.at[3], beside)
    arrive(0, True, False)

    @pl.loop(1, end)
    def _(i):
        arrive(i, False, False)

    arrive(end, False, True)

    last = carry[...]
    z_ref[:, stride:] = last[:, :rest]
    last = jnp.where(lane < rest, last, -jnp.inf)
    top = jnp.maximum(m_ref[...], last)
    mass = s_ref[...] * jnp.exp(m_ref[...] - top) + jnp.exp(last - top)
    top = jnp.transpose(jnp.concatenate([top, top], axis=0))
    mass = jnp.transpose(jnp.concatenate([mass, mass], axis=0))
    peak = jnp.max(top, axis=0, keepdims=True)
    mass = jnp.sum(mass * jnp.exp(top - peak), axis=0, keepdims=True)
    me = col * 4 + row
    fst[me] = jnp.where(lane[:1] < rows, peak, mass)

    def stat_copy(c, dr, slot):
        return pltpu.make_async_remote_copy(
            src_ref=fst.at[slot], dst_ref=fst.at[slot], send_sem=fsend.at[c * 4 + dr], recv_sem=frecv.at[slot],
            device_id={"col": c, "row": lax.rem(row + dr, 4)}, device_id_type=MESH,
        )

    def each_peer(act):
        for c in range(4):
            for dr in (2, 3, 1):
                act(c, dr)

            @pl.when(col != c)
            def _():
                act(c, 0)

    each_peer(lambda c, dr: stat_copy(c, dr, me).start())
    each_peer(lambda c, dr: stat_copy(c, dr, c * 4 + lax.rem(row + dr, 4)).wait_recv())
    stats = fst[...]
    swapped = pltpu.roll(stats, LANES // 2, 2)
    peak = jnp.max(stats, axis=0)
    mass = jnp.sum(swapped * jnp.exp(stats - peak), axis=0)
    lse_ref[...] = peak + jnp.log(mass)

    for k in range(1, 4):
        norm_copy(k).wait_send()
    for src, dst, send, recv in ((qbuf, rin, qsend, rrecv), (pbuf, lin, psend, lrecv)):
        pltpu.make_async_remote_copy(
            src_ref=src, dst_ref=dst, send_sem=send, recv_sem=recv.at[0],
            device_id={"row": mate}, device_id_type=MESH,
        ).wait_send()
    for k in range(3):
        first_copy(k).wait_send()
    for k in range(1, final):
        each_group(k, lambda copy: copy.wait_send())
    each_single(lambda copy: copy.wait_send())

    @pl.when(core == 0)
    def _():
        rx_copy.wait_send()

    @pl.when(core == 1)
    def _():
        qx_copy.wait_send()
        across_copy(final, end).wait_send()

    @pl.when(col == 3)
    def _():
        relay_copy(0).wait_send()

    @pl.when(col == core)
    def _():
        relay_copy(1).wait_send()
        relay_copy(2).wait_send()

    @pl.when(core == 1)
    def _():
        edge_copy.wait_send()

    each_peer(lambda c, dr: stat_copy(c, dr, me).wait_send())


def solution(mesh):
    def local_head(hidden, norm_gain, w_head):
        rows, feats = hidden.shape
        width = w_head.shape[1] // 4
        count = (width // LANES + 1) // TILES
        block = (count, rows, CHUNK)
        dma = pltpu.SemaphoreType.DMA

        def body(*refs):
            head_kernel(count, width, feats * 4, *refs)

        z, lse = pl.pallas_call(
            body,
            out_shape=(
                jax.ShapeDtypeStruct((rows, width), jnp.float32),
                jax.ShapeDtypeStruct((1, LANES), jnp.float32),
            ),
            in_specs=[
                pl.BlockSpec(memory_space=pltpu.HBM),
                pl.BlockSpec(memory_space=pltpu.HBM),
                pl.BlockSpec(memory_space=pltpu.HBM),
            ],
            out_specs=(pl.BlockSpec(memory_space=pltpu.VMEM), pl.BlockSpec(memory_space=pltpu.VMEM)),
            scratch_shapes=[
                pltpu.VMEM((rows, feats), hidden.dtype),
                pltpu.VMEM((feats,), jnp.float32),
                *[pltpu.VMEM((SLOTS, feats, CHUNK), jnp.bfloat16) for _ in range(4)],
                pltpu.VMEM((rows, feats), jnp.bfloat16),
                *[pltpu.VMEM(block, jnp.float32) for _ in range(7)],
                pltpu.VMEM((4, 1, LANES), jnp.float32),
                pltpu.VMEM((16, 1, LANES), jnp.float32),
                *[pltpu.VMEM((rows, LANES), jnp.float32) for _ in range(5)],
                *[pltpu.VMEM((rows, (TILES - 1) * LANES), jnp.float32) for _ in range(4)],
                pltpu.VMEM((rows, LANES), jnp.float32),
                dma, dma, pltpu.SemaphoreType.REGULAR((4,)),
                *[dma((SLOTS,)) for _ in range(4)], dma((4,)), dma((4,)),
                dma, dma, dma((len(GROUPS) + 2,)), dma((count,)), dma((count,)), dma((len(GROUPS) + 2,)), dma((16,)), dma((16,)), dma, dma, dma((3,)), dma((3,)), dma, dma, dma,
                dma((3,)), dma((3,)),
            ],
            compiler_params=pltpu.CompilerParams(
                collective_id=0, has_side_effects=True, vmem_limit_bytes=48 * 1024 * 1024
            ),
            name="head",
        )(pltpu.with_memory_space_constraint(hidden, pltpu.HBM), pltpu.with_memory_space_constraint(norm_gain, pltpu.HBM), w_head)
        log_norm = lse[0, :rows]
        return z - log_norm[:, None], log_norm

    return jax.shard_map(
        local_head,
        mesh=mesh,
        in_specs=(P("dp", "row"), P("row"), P("row", "col")),
        out_specs=(P("dp", ("col", "row")), P("dp")),
        check_vma=False,
    )
```

```python
import jax
import jax.numpy as jnp
from jax import lax
from jax.experimental import pallas as pl
from jax.experimental.pallas import tpu as pltpu
from jax.sharding import PartitionSpec as P

EPS = 1e-5
MESH = pl.DeviceIdType.MESH
LANES = 128
TILES = 3
CHUNK = TILES * LANES
SLOTS = 4
GROUPS = ((0,), (1, 2), (3, 7), (8, 17), (18, 23), (24,))
RELAY = 12
RELAY_AT = 14


def head_kernel(
    count, width, hidden_size,
    h_hbm, g_hbm, w_ref, z_ref, lse_ref,
    h_ref, g_ref, wq, wr, wp, wl, x_ref, qbuf, rbuf, pbuf, lbuf, rin, lin, yin, nst, fst, m_ref, s_ref, carry, edge_out, edge_in, relay_in, relay_mid, rx, qx, first_in,
    h_sem, g_sem, hops, wq_sem, wr_sem, wp_sem, wl_sem, nsend, nrecv, qsend, psend, ysend, rrecv, lrecv, yrecv, fsend, frecv, esend, erecv, relay_send, relay_recv, rx_send, rx_recv, qx_send, first_send, first_recv,
):
    rows, feats = h_ref.shape
    stride = (width // LANES) * LANES
    rest = width - stride
    col = lax.axis_index("col")
    row = lax.axis_index("row")
    core = lax.rem(row, 2)
    mate = row + 1 - 2 * core
    across = lax.rem(row + 2, 4)
    far = 3 - row
    shift = row * rest

    end = count - 1

    streams = {
        "far": (far, wq, wq_sem), "across": (across, wr, wr_sem), "mate": (mate, wp, wp_sem), "own": (row, wl, wl_sem)
    }

    def chunk_at(t):
        if isinstance(t, int) and t < 2:
            return t * RELAY
        return t - 1 + t // (RELAY + 1)

    def fetch(name, t):
        part, buf, sem = streams[name]
        chunk = t
        if name in ("far", "across"):
            chunk = chunk_at(t)
        start = pl.multiple_of(stride * part + CHUNK * chunk, LANES)
        slot = lax.rem(t, SLOTS)
        return pltpu.make_async_copy(w_ref.at[:, pl.ds(start, CHUNK)], buf.at[slot], sem.at[slot])

    barrier = pltpu.get_barrier_semaphore()

    def tell_column(sem, step):
        @pl.when((col + step >= 0) & (col + step < 4))
        def _():
            pl.semaphore_signal(sem, inc=1, device_id_type=MESH, device_id={"col": col + step})

    def tell_columns(sem):
        tell_column(sem, -1)
        tell_column(sem, 1)

    for k in (2, 3, 1):
        pl.semaphore_signal(barrier, inc=1, device_id_type=MESH, device_id={"row": lax.rem(row + k, 4)})
    tell_column(barrier, 1)
    below = (col + 2) // 3
    above = (5 - col) // 3
    beside = below + above

    h_copy = pltpu.make_async_copy(h_hbm, h_ref, h_sem)
    g_copy = pltpu.make_async_copy(g_hbm, g_ref, g_sem)
    h_copy.start()
    g_copy.start()
    h_copy.wait()
    for name, t in (("far", 0), ("far", 1), ("across", 0)):
        fetch(name, t).start()

    lane = lax.broadcasted_iota(jnp.int32, (rows, LANES), 1)
    sq = jnp.zeros((rows, LANES), jnp.float32)
    for j in range(feats // LANES):
        part = h_ref[:, j * LANES:(j + 1) * LANES].astype(jnp.float32)
        sq = sq + part * part
    sq = jnp.transpose(jnp.concatenate([sq, sq], axis=0))
    nst[row] = jnp.sum(sq, axis=0, keepdims=True)
    pl.semaphore_wait(barrier, 3 + below)
    tell_column(hops.at[0], -1)

    def norm_copy(k):
        return pltpu.make_async_remote_copy(
            src_ref=nst.at[row], dst_ref=nst.at[row], send_sem=nsend.at[k], recv_sem=nrecv.at[row],
            device_id={"row": lax.rem(row + k, 4)}, device_id_type=MESH,
        )

    for k in (2, 3, 1):
        norm_copy(k).start()
    for name, t in (
        *[(n, t) for t in range(1, SLOTS) for n in ("far", "across") if n == "across" or t > 1], *[(n, t) for t in range(SLOTS) for n in ("mate", "own")]
    ):
        fetch(name, t).start()
    for k in range(1, 4):
        peer = lax.rem(row + k, 4)
        pltpu.make_async_remote_copy(
            src_ref=nst.at[peer], dst_ref=nst.at[peer], send_sem=nsend.at[k], recv_sem=nrecv.at[peer],
            device_id={"row": peer}, device_id_type=MESH,
        ).wait_recv()
    g_copy.wait()
    total = nst[0] + nst[1] + nst[2] + nst[3]
    scale = lax.rsqrt(total / hidden_size + EPS)
    scale = jnp.transpose(jnp.broadcast_to(scale, (LANES, LANES)))[:rows]
    for j in range(feats // LANES):
        cols = slice(j * LANES, (j + 1) * LANES)
        x_ref[:, cols] = (h_ref[:, cols].astype(jnp.float32) * scale * g_ref[cols].reshape(1, LANES)).astype(jnp.bfloat16)

    def product(name, t):
        fetch(name, t).wait()
        return jnp.dot(x_ref[...], streams[name][1][lax.rem(t, SLOTS)], preferred_element_type=jnp.float32)

    def refill(name, t):
        @pl.when(t + SLOTS < count)
        def _():
            fetch(name, t + SLOTS).start()

    def mate_copy(src, dst, send, recv, i):
        return pltpu.make_async_remote_copy(
            src_ref=src.at[i], dst_ref=dst.at[i], send_sem=send, recv_sem=recv.at[i],
            device_id={"row": mate}, device_id_type=MESH,
        )

    most = pl.ds(0, (TILES - 1) * LANES)
    final = len(GROUPS) - 1

    def across_copy(k, where):
        return pltpu.make_async_remote_copy(
            src_ref=rbuf.at[where], dst_ref=yin.at[where], send_sem=ysend.at[k], recv_sem=yrecv.at[k],
            device_id={"row": across}, device_id_type=MESH,
        )

    def pieces(k):
        lo, hi = GROUPS[k][0], GROUPS[k][-1]
        if lo <= RELAY <= hi:
            return [(k, pl.ds(lo, RELAY - lo)), (len(GROUPS), pl.ds(RELAY + 1, hi - RELAY))]
        return [(k, pl.ds(lo, hi - lo + 1))]

    rx_copy = pltpu.make_async_remote_copy(
        src_ref=rbuf.at[end, :, most], dst_ref=rx, send_sem=rx_send, recv_sem=rx_recv,
        device_id={"row": mate}, device_id_type=MESH,
    )
    qx_copy = pltpu.make_async_remote_copy(
        src_ref=qx, dst_ref=yin.at[end, :, most], send_sem=qx_send, recv_sem=yrecv.at[final],
        device_id={"row": far}, device_id_type=MESH,
    )

    lead = pl.ds(0, LANES)
    rest_of = pl.ds(LANES, (TILES - 1) * LANES)

    def first_copy(k):
        src, dst, device = (
            (qbuf.at[0, :, lead], first_in, far),
            (rbuf.at[0, :, lead], yin.at[0, :, lead], across),
            (rbuf.at[0, :, rest_of], yin.at[0, :, rest_of], across),
        )[k]
        return pltpu.make_async_remote_copy(
            src_ref=src, dst_ref=dst, send_sem=first_send.at[k], recv_sem=first_recv.at[k],
            device_id={"row": device}, device_id_type=MESH,
        )

    def last_step():
        rbuf[end] = product("across", end)

        @pl.when(core == 0)
        def _():
            rx_copy.start()

        mate_copy(qbuf, rin, qsend, rrecv, end).wait_recv()

        @pl.when(core == 1)
        def _():
            rx_copy.wait_recv()
            qx[...] = qbuf[end, :, most] + rx[...]
            qx_copy.start()
            rbuf[end] = rbuf[end] + rin[end]
            across_copy(final, end).start()

    def each_group(k, act):
        for sem, where in pieces(k):
            act(across_copy(sem, where))

    late = col >= 3 - core
    early = col <= core

    def each_single(act):
        @pl.when(jnp.logical_not(late))
        def _():
            act(across_copy(len(GROUPS) + 1, RELAY))

        @pl.when(late)
        def _():
            act(across_copy(len(GROUPS) + 1, (RELAY, slice(None), pl.ds((TILES - 1) * LANES, LANES))))

    def relay_copy(k):
        src, dst, device = (
            (rbuf.at[RELAY, :, most], relay_in, {"col": core * (col - 2)}),
            (relay_in, relay_mid, {"row": across}),
            (relay_mid, yin.at[RELAY, :, most], {"col": 3 + core * (col - 1)}),
        )[k]
        return pltpu.make_async_remote_copy(
            src_ref=src, dst_ref=dst, send_sem=relay_send.at[k], recv_sem=relay_recv.at[k],
            device_id=device, device_id_type=MESH,
        )

    edge_copy = pltpu.make_async_remote_copy(
        src_ref=edge_out, dst_ref=edge_in, send_sem=esend, recv_sem=erecv,
        device_id={"row": mate}, device_id_type=MESH,
    )

    def far_step(t, i):
        qbuf[i] = product("far", t)
        mate_copy(qbuf, rin, qsend, rrecv, i).start()
        refill("far", t)

    def across_step(t, i):
        term = product("across", t)
        refill("across", t)
        mate_copy(qbuf, rin, qsend, rrecv, i).wait_recv()
        rbuf[i] = term + rin[i]

    def mate_step(i):
        pbuf[i] = product("mate", i)
        mate_copy(pbuf, lin, psend, lrecv, i).start()
        refill("mate", i)

    def own_step(i):
        lbuf[i] = product("own", i)
        refill("own", i)

    turn = lax.rem(LANES - shift, LANES)
    keep = lane < LANES - shift

    def arrive(i, first, last):
        mate_copy(pbuf, lin, psend, lrecv, i).wait_recv()
        if first:
            for k in range(3):
                first_copy(k).wait_recv()
        elif last:
            @pl.when(core == 0)
            def _():
                qx_copy.wait_recv()

            @pl.when(core == 1)
            def _():
                across_copy(final, end).wait_recv()
        else:
            for k in range(1, final):
                for sem, where in pieces(k):
                    @pl.when(i == where.start)
                    def _():
                        across_copy(sem, where).wait_recv()

            @pl.when(i == RELAY)
            def _():
                each_single(lambda copy: copy.wait_recv())

                @pl.when(late)
                def _():
                    relay_copy(2).wait_recv()
        full = lbuf[i] + lin[i] + yin[i]
        parts = [full[:, k * LANES:(k + 1) * LANES] for k in range(TILES)]
        if first:
            parts[0] = parts[0] + first_in[...]
            edge_out[...] = parts[0]

            @pl.when(core == 1)
            def _():
                edge_copy.start()
        if last:
            @pl.when(core == 0)
            def _():
                edge_copy.wait_recv()

            parts[-1] = jnp.where(core == 0, edge_in[...], parts[-1])
        rolled = [pltpu.roll(part, turn, 1) for part in parts]
        tiles = [jnp.where(keep, rolled[k], rolled[k + 1]) for k in range(TILES - 1)]
        at = 0
        if not first:
            tiles = [jnp.where(keep, carry[...], rolled[0])] + tiles
            at = pl.multiple_of(i * CHUNK - LANES, LANES)
        carry[...] = rolled[-1]
        z_ref[:, pl.ds(at, LANES * len(tiles))] = jnp.concatenate(tiles, axis=1)
        top = tiles[0]
        for tile in tiles[1:]:
            top = jnp.maximum(top, tile)
        if not first:
            top = jnp.maximum(top, m_ref[...])
        mass = jnp.exp(tiles[0] - top)
        for tile in tiles[1:]:
            mass = mass + jnp.exp(tile - top)
        if not first:
            mass = mass + s_ref[...] * jnp.exp(m_ref[...] - top)
        m_ref[...] = top
        s_ref[...] = mass

    far_step(0, 0)
    first_copy(0).start()
    rbuf[0] = product("across", 0)
    first_copy(1).start()
    refill("across", 0)

    @pl.when(col < 3)
    def _():
        pl.semaphore_wait(hops.at[0], 1)

    tell_columns(hops.at[1])
    far_step(1, RELAY)
    mate_copy(qbuf, rin, qsend, rrecv, 0).wait_recv()
    rbuf[0, :, LANES:] = rbuf[0, :, LANES:] + rin[0, :, LANES:]
    first_copy(2).start()
    far_step(2, 1)
    pl.semaphore_wait(hops.at[1], beside)
    tell_columns(hops.at[2])
    far_step(3, 2)
    across_step(1, RELAY)
    pl.semaphore_wait(hops.at[2], beside)
    tell_columns(hops.at[3])
    each_single(lambda copy: copy.start())

    @pl.when(late)
    def _():
        relay_copy(0).start()

    @pl.loop(2, end)
    def _(t):
        @pl.when(t < end - 1)
        def _():
            far_step(t + 2, chunk_at(t + 2))

        i = chunk_at(t)
        across_step(t, i)
        for k in range(1, final):
            for sem, where in pieces(k):
                @pl.when(i == where.start + where.size - 1)
                def _():
                    across_copy(sem, where).start()

        @pl.when((t == RELAY_AT) & early)
        def _():
            relay_copy(0).wait_recv()
            relay_copy(1).start()

    last_step()

    @pl.loop(0, count)
    def _(i):
        mate_step(i)
        own_step(i)

    @pl.when(early)
    def _():
        relay_copy(1).wait_recv()
        relay_copy(2).start()

    pl.semaphore_wait(hops.at[3], beside)
    arrive(0, True, False)

    @pl.loop(1, end)
    def _(i):
        arrive(i, False, False)

    arrive(end, False, True)

    last = carry[...]
    z_ref[:, stride:] = last[:, :rest]
    last = jnp.where(lane < rest, last, -jnp.inf)
    top = jnp.maximum(m_ref[...], last)
    mass = s_ref[...] * jnp.exp(m_ref[...] - top) + jnp.exp(last - top)
    top = jnp.transpose(jnp.concatenate([top, top], axis=0))
    mass = jnp.transpose(jnp.concatenate([mass, mass], axis=0))
    peak = jnp.max(top, axis=0, keepdims=True)
    mass = jnp.sum(mass * jnp.exp(top - peak), axis=0, keepdims=True)
    me = col * 4 + row
    fst[me] = jnp.where(lane[:1] < rows, peak, mass)

    def stat_copy(c, r, slot):
        return pltpu.make_async_remote_copy(
            src_ref=fst.at[slot], dst_ref=fst.at[slot], send_sem=fsend.at[c * 4 + r], recv_sem=frecv.at[slot],
            device_id={"col": c, "row": r}, device_id_type=MESH,
        )

    def each_peer(act):
        for c in range(4):
            for r in range(4):
                @pl.when(me != c * 4 + r)
                def _():
                    act(c, r)

    each_peer(lambda c, r: stat_copy(c, r, me).start())
    each_peer(lambda c, r: stat_copy(c, r, c * 4 + r).wait_recv())
    stats = fst[...]
    swapped = pltpu.roll(stats, LANES // 2, 2)
    peak = jnp.max(stats, axis=0)
    mass = jnp.sum(swapped * jnp.exp(stats - peak), axis=0)
    lse_ref[...] = peak + jnp.log(mass)

    for k in range(1, 4):
        norm_copy(k).wait_send()
    for src, dst, send, recv in ((qbuf, rin, qsend, rrecv), (pbuf, lin, psend, lrecv)):
        pltpu.make_async_remote_copy(
            src_ref=src, dst_ref=dst, send_sem=send, recv_sem=recv.at[0],
            device_id={"row": mate}, device_id_type=MESH,
        ).wait_send()
    for k in range(3):
        first_copy(k).wait_send()
    for k in range(1, final):
        each_group(k, lambda copy: copy.wait_send())
    each_single(lambda copy: copy.wait_send())

    @pl.when(core == 0)
    def _():
        rx_copy.wait_send()

    @pl.when(core == 1)
    def _():
        qx_copy.wait_send()
        across_copy(final, end).wait_send()

    @pl.when(late)
    def _():
        relay_copy(0).wait_send()

    @pl.when(early)
    def _():
        relay_copy(1).wait_send()
        relay_copy(2).wait_send()

    @pl.when(core == 1)
    def _():
        edge_copy.wait_send()

    each_peer(lambda c, r: stat_copy(c, r, me).wait_send())


def solution(mesh):
    def local_head(hidden, norm_gain, w_head):
        rows, feats = hidden.shape
        width = w_head.shape[1] // 4
        count = (width // LANES + 1) // TILES
        block = (count, rows, CHUNK)
        dma = pltpu.SemaphoreType.DMA

        def body(*refs):
            head_kernel(count, width, feats * 4, *refs)

        z, lse = pl.pallas_call(
            body,
            out_shape=(
                jax.ShapeDtypeStruct((rows, width), jnp.float32),
                jax.ShapeDtypeStruct((1, LANES), jnp.float32),
            ),
            in_specs=[
                pl.BlockSpec(memory_space=pltpu.HBM),
                pl.BlockSpec(memory_space=pltpu.HBM),
                pl.BlockSpec(memory_space=pltpu.HBM),
            ],
            out_specs=(pl.BlockSpec(memory_space=pltpu.VMEM), pl.BlockSpec(memory_space=pltpu.VMEM)),
            scratch_shapes=[
                pltpu.VMEM((rows, feats), hidden.dtype),
                pltpu.VMEM((feats,), jnp.float32),
                *[pltpu.VMEM((SLOTS, feats, CHUNK), jnp.bfloat16) for _ in range(4)],
                pltpu.VMEM((rows, feats), jnp.bfloat16),
                *[pltpu.VMEM(block, jnp.float32) for _ in range(7)],
                pltpu.VMEM((4, 1, LANES), jnp.float32),
                pltpu.VMEM((16, 1, LANES), jnp.float32),
                *[pltpu.VMEM((rows, LANES), jnp.float32) for _ in range(5)],
                *[pltpu.VMEM((rows, (TILES - 1) * LANES), jnp.float32) for _ in range(4)],
                pltpu.VMEM((rows, LANES), jnp.float32),
                dma, dma, pltpu.SemaphoreType.REGULAR((4,)),
                *[dma((SLOTS,)) for _ in range(4)], dma((4,)), dma((4,)),
                dma, dma, dma((len(GROUPS) + 2,)), dma((count,)), dma((count,)), dma((len(GROUPS) + 2,)), dma((16,)), dma((16,)), dma, dma, dma((3,)), dma((3,)), dma, dma, dma,
                dma((3,)), dma((3,)),
            ],
            compiler_params=pltpu.CompilerParams(
                collective_id=0, has_side_effects=True, vmem_limit_bytes=48 * 1024 * 1024
            ),
            name="head",
        )(pltpu.with_memory_space_constraint(hidden, pltpu.HBM), pltpu.with_memory_space_constraint(norm_gain, pltpu.HBM), w_head)
        log_norm = lse[0, :rows]
        return z - log_norm[:, None], log_norm

    return jax.shard_map(
        local_head,
        mesh=mesh,
        in_specs=(P("dp", "row"), P("row"), P("row", "col")),
        out_specs=(P("dp", ("col", "row")), P("dp")),
        check_vma=False,
    )
```

```python
import jax
import jax.numpy as jnp
from jax import lax
from jax.experimental import pallas as pl
from jax.experimental.pallas import tpu as pltpu
from jax.sharding import PartitionSpec as P

EPS = 1e-5
MESH = pl.DeviceIdType.MESH
LANES = 128
TILES = 3
CHUNK = TILES * LANES
SLOTS = 4
GROUPS = ((0,), (1, 2), (3, 7), (8, 17), (18, 22), (23,), (24,))
RELAY = 12
RELAY_AT = 14


def head_kernel(
    count, width, hidden_size,
    h_hbm, g_hbm, w_ref, z_ref, lse_ref,
    h_ref, g_ref, wq, wr, wp, wl, x_ref, qbuf, rbuf, pbuf, lbuf, rin, lin, yin, nst, fst, m_ref, s_ref, carry, edge_out, edge_in, relay_in, relay_mid, rx, qx, first_in,
    h_sem, g_sem, hops, wq_sem, wr_sem, wp_sem, wl_sem, nsend, nrecv, qsend, psend, ysend, rrecv, lrecv, yrecv, fsend, frecv, esend, erecv, relay_send, relay_recv, rx_send, rx_recv, qx_send, first_send, first_recv,
):
    rows, feats = h_ref.shape
    stride = (width // LANES) * LANES
    rest = width - stride
    col = lax.axis_index("col")
    row = lax.axis_index("row")
    core = lax.rem(row, 2)
    mate = row + 1 - 2 * core
    across = lax.rem(row + 2, 4)
    far = 3 - row
    shift = row * rest

    end = count - 1

    streams = {
        "far": (far, wq, wq_sem), "across": (across, wr, wr_sem), "mate": (mate, wp, wp_sem), "own": (row, wl, wl_sem)
    }

    def chunk_at(t):
        if isinstance(t, int) and t < 2:
            return t * RELAY
        return t - 1 + t // (RELAY + 1)

    def fetch(name, t):
        part, buf, sem = streams[name]
        chunk = t
        if name in ("far", "across"):
            chunk = chunk_at(t)
        start = pl.multiple_of(stride * part + CHUNK * chunk, LANES)
        slot = lax.rem(t, SLOTS)
        return pltpu.make_async_copy(w_ref.at[:, pl.ds(start, CHUNK)], buf.at[slot], sem.at[slot])

    barrier = pltpu.get_barrier_semaphore()

    def tell_column(sem, step):
        @pl.when((col + step >= 0) & (col + step < 4))
        def _():
            pl.semaphore_signal(sem, inc=1, device_id_type=MESH, device_id={"col": col + step})

    def tell_columns(sem):
        tell_column(sem, -1)
        tell_column(sem, 1)

    for k in (2, 3, 1):
        pl.semaphore_signal(barrier, inc=1, device_id_type=MESH, device_id={"row": lax.rem(row + k, 4)})
    tell_column(barrier, 1)
    below = (col + 2) // 3
    above = (5 - col) // 3
    beside = below + above

    h_copy = pltpu.make_async_copy(h_hbm, h_ref, h_sem)
    g_copy = pltpu.make_async_copy(g_hbm, g_ref, g_sem)
    h_copy.start()
    g_copy.start()
    h_copy.wait()
    for name, t in (("far", 0), ("far", 1), ("across", 0)):
        fetch(name, t).start()

    lane = lax.broadcasted_iota(jnp.int32, (rows, LANES), 1)
    sq = jnp.zeros((rows, LANES), jnp.float32)
    for j in range(feats // LANES):
        part = h_ref[:, j * LANES:(j + 1) * LANES].astype(jnp.float32)
        sq = sq + part * part
    sq = jnp.transpose(jnp.concatenate([sq, sq], axis=0))
    nst[row] = jnp.sum(sq, axis=0, keepdims=True)
    pl.semaphore_wait(barrier, 3 + below)
    tell_column(hops.at[0], -1)

    def norm_copy(k):
        return pltpu.make_async_remote_copy(
            src_ref=nst.at[row], dst_ref=nst.at[row], send_sem=nsend.at[k], recv_sem=nrecv.at[row],
            device_id={"row": lax.rem(row + k, 4)}, device_id_type=MESH,
        )

    for k in (2, 3, 1):
        norm_copy(k).start()
    for name, t in (
        *[(n, t) for t in range(1, SLOTS) for n in ("far", "across") if n == "across" or t > 1], *[(n, t) for t in range(SLOTS) for n in ("mate", "own")]
    ):
        fetch(name, t).start()
    for k in range(1, 4):
        peer = lax.rem(row + k, 4)
        pltpu.make_async_remote_copy(
            src_ref=nst.at[peer], dst_ref=nst.at[peer], send_sem=nsend.at[k], recv_sem=nrecv.at[peer],
            device_id={"row": peer}, device_id_type=MESH,
        ).wait_recv()
    g_copy.wait()
    total = nst[0] + nst[1] + nst[2] + nst[3]
    scale = lax.rsqrt(total / hidden_size + EPS)
    scale = jnp.transpose(jnp.broadcast_to(scale, (LANES, LANES)))[:rows]
    for j in range(feats // LANES):
        cols = slice(j * LANES, (j + 1) * LANES)
        x_ref[:, cols] = (h_ref[:, cols].astype(jnp.float32) * scale * g_ref[cols].reshape(1, LANES)).astype(jnp.bfloat16)

    def product(name, t):
        fetch(name, t).wait()
        return jnp.dot(x_ref[...], streams[name][1][lax.rem(t, SLOTS)], preferred_element_type=jnp.float32)

    def refill(name, t):
        @pl.when(t + SLOTS < count)
        def _():
            fetch(name, t + SLOTS).start()

    def mate_copy(src, dst, send, recv, i):
        return pltpu.make_async_remote_copy(
            src_ref=src.at[i], dst_ref=dst.at[i], send_sem=send, recv_sem=recv.at[i],
            device_id={"row": mate}, device_id_type=MESH,
        )

    most = pl.ds(0, (TILES - 1) * LANES)
    final = len(GROUPS) - 1

    def across_copy(k, where):
        return pltpu.make_async_remote_copy(
            src_ref=rbuf.at[where], dst_ref=yin.at[where], send_sem=ysend.at[k], recv_sem=yrecv.at[k],
            device_id={"row": across}, device_id_type=MESH,
        )

    def pieces(k):
        lo, hi = GROUPS[k][0], GROUPS[k][-1]
        if lo <= RELAY <= hi:
            return [(k, pl.ds(lo, RELAY - lo)), (len(GROUPS), pl.ds(RELAY + 1, hi - RELAY))]
        return [(k, pl.ds(lo, hi - lo + 1))]

    rx_copy = pltpu.make_async_remote_copy(
        src_ref=rbuf.at[end, :, most], dst_ref=rx, send_sem=rx_send, recv_sem=rx_recv,
        device_id={"row": mate}, device_id_type=MESH,
    )
    qx_copy = pltpu.make_async_remote_copy(
        src_ref=qx, dst_ref=yin.at[end, :, most], send_sem=qx_send, recv_sem=yrecv.at[final],
        device_id={"row": far}, device_id_type=MESH,
    )

    lead = pl.ds(0, LANES)
    rest_of = pl.ds(LANES, (TILES - 1) * LANES)

    def first_copy(k):
        src, dst, device = (
            (qbuf.at[0, :, lead], first_in, far),
            (rbuf.at[0, :, lead], yin.at[0, :, lead], across),
            (rbuf.at[0, :, rest_of], yin.at[0, :, rest_of], across),
        )[k]
        return pltpu.make_async_remote_copy(
            src_ref=src, dst_ref=dst, send_sem=first_send.at[k], recv_sem=first_recv.at[k],
            device_id={"row": device}, device_id_type=MESH,
        )

    def last_step():
        rbuf[end] = product("across", end)

        @pl.when(core == 0)
        def _():
            rx_copy.start()

        mate_copy(qbuf, rin, qsend, rrecv, end).wait_recv()

        @pl.when(core == 1)
        def _():
            rx_copy.wait_recv()
            qx[...] = qbuf[end, :, most] + rx[...]
            qx_copy.start()
            rbuf[end] = rbuf[end] + rin[end]
            across_copy(final, end).start()

    def each_group(k, act):
        for sem, where in pieces(k):
            act(across_copy(sem, where))

    late = col >= 3 - core
    early = col <= core

    def each_single(act):
        @pl.when(jnp.logical_not(late))
        def _():
            act(across_copy(len(GROUPS) + 1, RELAY))

        @pl.when(late)
        def _():
            act(across_copy(len(GROUPS) + 1, (RELAY, slice(None), pl.ds((TILES - 1) * LANES, LANES))))

    def relay_copy(k):
        src, dst, device = (
            (rbuf.at[RELAY, :, most], relay_in, {"col": core * (col - 2)}),
            (relay_in, relay_mid, {"row": across}),
            (relay_mid, yin.at[RELAY, :, most], {"col": 3 + core * (col - 1)}),
        )[k]
        return pltpu.make_async_remote_copy(
            src_ref=src, dst_ref=dst, send_sem=relay_send.at[k], recv_sem=relay_recv.at[k],
            device_id=device, device_id_type=MESH,
        )

    edge_copy = pltpu.make_async_remote_copy(
        src_ref=edge_out, dst_ref=edge_in, send_sem=esend, recv_sem=erecv,
        device_id={"row": mate}, device_id_type=MESH,
    )

    def far_step(t, i):
        qbuf[i] = product("far", t)
        mate_copy(qbuf, rin, qsend, rrecv, i).start()
        refill("far", t)

    def across_step(t, i):
        term = product("across", t)
        refill("across", t)
        mate_copy(qbuf, rin, qsend, rrecv, i).wait_recv()
        rbuf[i] = term + rin[i]

    def mate_step(i):
        pbuf[i] = product("mate", i)
        mate_copy(pbuf, lin, psend, lrecv, i).start()
        refill("mate", i)

    def own_step(i):
        lbuf[i] = product("own", i)
        refill("own", i)

    turn = lax.rem(LANES - shift, LANES)
    keep = lane < LANES - shift

    def arrive(i, first, last):
        mate_copy(pbuf, lin, psend, lrecv, i).wait_recv()
        if first:
            for k in range(3):
                first_copy(k).wait_recv()
        elif last:
            @pl.when(core == 0)
            def _():
                qx_copy.wait_recv()

            @pl.when(core == 1)
            def _():
                across_copy(final, end).wait_recv()
        else:
            for k in range(1, final):
                for sem, where in pieces(k):
                    @pl.when(i == where.start)
                    def _():
                        across_copy(sem, where).wait_recv()

            @pl.when(i == RELAY)
            def _():
                each_single(lambda copy: copy.wait_recv())

                @pl.when(late)
                def _():
                    relay_copy(2).wait_recv()
        full = lbuf[i] + lin[i] + yin[i]
        parts = [full[:, k * LANES:(k + 1) * LANES] for k in range(TILES)]
        if first:
            parts[0] = parts[0] + first_in[...]
            edge_out[...] = parts[0]

            @pl.when(core == 1)
            def _():
                edge_copy.start()
        if last:
            @pl.when(core == 0)
            def _():
                edge_copy.wait_recv()

            parts[-1] = jnp.where(core == 0, edge_in[...], parts[-1])
        rolled = [pltpu.roll(part, turn, 1) for part in parts]
        tiles = [jnp.where(keep, rolled[k], rolled[k + 1]) for k in range(TILES - 1)]
        at = 0
        if not first:
            tiles = [jnp.where(keep, carry[...], rolled[0])] + tiles
            at = pl.multiple_of(i * CHUNK - LANES, LANES)
        carry[...] = rolled[-1]
        z_ref[:, pl.ds(at, LANES * len(tiles))] = jnp.concatenate(tiles, axis=1)
        top = tiles[0]
        for tile in tiles[1:]:
            top = jnp.maximum(top, tile)
        if not first:
            top = jnp.maximum(top, m_ref[...])
        mass = jnp.exp(tiles[0] - top)
        for tile in tiles[1:]:
            mass = mass + jnp.exp(tile - top)
        if not first:
            mass = mass + s_ref[...] * jnp.exp(m_ref[...] - top)
        m_ref[...] = top
        s_ref[...] = mass

    far_step(0, 0)
    first_copy(0).start()
    rbuf[0] = product("across", 0)
    first_copy(1).start()
    refill("across", 0)

    @pl.when(col < 3)
    def _():
        pl.semaphore_wait(hops.at[0], 1)

    tell_columns(hops.at[1])
    far_step(1, RELAY)
    mate_copy(qbuf, rin, qsend, rrecv, 0).wait_recv()
    rbuf[0, :, LANES:] = rbuf[0, :, LANES:] + rin[0, :, LANES:]
    first_copy(2).start()
    far_step(2, 1)
    pl.semaphore_wait(hops.at[1], beside)
    tell_columns(hops.at[2])
    far_step(3, 2)
    across_step(1, RELAY)
    each_single(lambda copy: copy.start())

    @pl.when(late)
    def _():
        pl.semaphore_wait(hops.at[2], beside)
        relay_copy(0).start()

    @pl.loop(2, end)
    def _(t):
        @pl.when(t < end - 1)
        def _():
            far_step(t + 2, chunk_at(t + 2))

        i = chunk_at(t)
        across_step(t, i)
        for k in range(1, final):
            for sem, where in pieces(k):
                @pl.when(i == where.start + where.size - 1)
                def _():
                    across_copy(sem, where).start()

        @pl.when((t == RELAY_AT) & early)
        def _():
            relay_copy(0).wait_recv()
            relay_copy(1).start()

    last_step()

    @pl.when(jnp.logical_not(late))
    def _():
        pl.semaphore_wait(hops.at[2], beside)

    tell_columns(hops.at[3])

    @pl.loop(0, count)
    def _(i):
        mate_step(i)
        own_step(i)

    @pl.when(early)
    def _():
        relay_copy(1).wait_recv()
        relay_copy(2).start()

    pl.semaphore_wait(hops.at[3], beside)
    arrive(0, True, False)

    @pl.loop(1, end)
    def _(i):
        arrive(i, False, False)

    arrive(end, False, True)

    last = carry[...]
    z_ref[:, stride:] = last[:, :rest]
    last = jnp.where(lane < rest, last, -jnp.inf)
    top = jnp.maximum(m_ref[...], last)
    mass = s_ref[...] * jnp.exp(m_ref[...] - top) + jnp.exp(last - top)
    top = jnp.transpose(jnp.concatenate([top, top], axis=0))
    mass = jnp.transpose(jnp.concatenate([mass, mass], axis=0))
    peak = jnp.max(top, axis=0, keepdims=True)
    mass = jnp.sum(mass * jnp.exp(top - peak), axis=0, keepdims=True)
    me = col * 4 + row
    fst[me] = jnp.where(lane[:1] < rows, peak, mass)

    def stat_copy(c, r, slot):
        return pltpu.make_async_remote_copy(
            src_ref=fst.at[slot], dst_ref=fst.at[slot], send_sem=fsend.at[c * 4 + r], recv_sem=frecv.at[slot],
            device_id={"col": c, "row": r}, device_id_type=MESH,
        )

    def each_peer(act):
        for c in range(4):
            for r in range(4):
                @pl.when(me != c * 4 + r)
                def _():
                    act(c, r)

    each_peer(lambda c, r: stat_copy(c, r, me).start())
    each_peer(lambda c, r: stat_copy(c, r, c * 4 + r).wait_recv())
    stats = fst[...]
    swapped = pltpu.roll(stats, LANES // 2, 2)
    peak = jnp.max(stats, axis=0)
    mass = jnp.sum(swapped * jnp.exp(stats - peak), axis=0)
    lse_ref[...] = peak + jnp.log(mass)

    for k in range(1, 4):
        norm_copy(k).wait_send()
    for src, dst, send, recv in ((qbuf, rin, qsend, rrecv), (pbuf, lin, psend, lrecv)):
        pltpu.make_async_remote_copy(
            src_ref=src, dst_ref=dst, send_sem=send, recv_sem=recv.at[0],
            device_id={"row": mate}, device_id_type=MESH,
        ).wait_send()
    for k in range(3):
        first_copy(k).wait_send()
    for k in range(1, final):
        each_group(k, lambda copy: copy.wait_send())
    each_single(lambda copy: copy.wait_send())

    @pl.when(core == 0)
    def _():
        rx_copy.wait_send()

    @pl.when(core == 1)
    def _():
        qx_copy.wait_send()
        across_copy(final, end).wait_send()

    @pl.when(late)
    def _():
        relay_copy(0).wait_send()

    @pl.when(early)
    def _():
        relay_copy(1).wait_send()
        relay_copy(2).wait_send()

    @pl.when(core == 1)
    def _():
        edge_copy.wait_send()

    each_peer(lambda c, r: stat_copy(c, r, me).wait_send())


def solution(mesh):
    def local_head(hidden, norm_gain, w_head):
        rows, feats = hidden.shape
        width = w_head.shape[1] // 4
        count = (width // LANES + 1) // TILES
        block = (count, rows, CHUNK)
        dma = pltpu.SemaphoreType.DMA

        def body(*refs):
            head_kernel(count, width, feats * 4, *refs)

        z, lse = pl.pallas_call(
            body,
            out_shape=(
                jax.ShapeDtypeStruct((rows, width), jnp.float32),
                jax.ShapeDtypeStruct((1, LANES), jnp.float32),
            ),
            in_specs=[
                pl.BlockSpec(memory_space=pltpu.HBM),
                pl.BlockSpec(memory_space=pltpu.HBM),
                pl.BlockSpec(memory_space=pltpu.HBM),
            ],
            out_specs=(pl.BlockSpec(memory_space=pltpu.VMEM), pl.BlockSpec(memory_space=pltpu.VMEM)),
            scratch_shapes=[
                pltpu.VMEM((rows, feats), hidden.dtype),
                pltpu.VMEM((feats,), jnp.float32),
                *[pltpu.VMEM((SLOTS, feats, CHUNK), jnp.bfloat16) for _ in range(4)],
                pltpu.VMEM((rows, feats), jnp.bfloat16),
                *[pltpu.VMEM(block, jnp.float32) for _ in range(7)],
                pltpu.VMEM((4, 1, LANES), jnp.float32),
                pltpu.VMEM((16, 1, LANES), jnp.float32),
                *[pltpu.VMEM((rows, LANES), jnp.float32) for _ in range(5)],
                *[pltpu.VMEM((rows, (TILES - 1) * LANES), jnp.float32) for _ in range(4)],
                pltpu.VMEM((rows, LANES), jnp.float32),
                dma, dma, pltpu.SemaphoreType.REGULAR((4,)),
                *[dma((SLOTS,)) for _ in range(4)], dma((4,)), dma((4,)),
                dma, dma, dma((len(GROUPS) + 2,)), dma((count,)), dma((count,)), dma((len(GROUPS) + 2,)), dma((16,)), dma((16,)), dma, dma, dma((3,)), dma((3,)), dma, dma, dma,
                dma((3,)), dma((3,)),
            ],
            compiler_params=pltpu.CompilerParams(
                collective_id=0, has_side_effects=True, vmem_limit_bytes=48 * 1024 * 1024
            ),
            name="head",
        )(pltpu.with_memory_space_constraint(hidden, pltpu.HBM), pltpu.with_memory_space_constraint(norm_gain, pltpu.HBM), w_head)
        log_norm = lse[0, :rows]
        return z - log_norm[:, None], log_norm

    return jax.shard_map(
        local_head,
        mesh=mesh,
        in_specs=(P("dp", "row"), P("row"), P("row", "col")),
        out_specs=(P("dp", ("col", "row")), P("dp")),
        check_vma=False,
    )
```

```python
import jax
import jax.numpy as jnp
from jax import lax
from jax.experimental import pallas as pl
from jax.experimental.pallas import tpu as pltpu
from jax.sharding import PartitionSpec as P

EPS = 1e-5
MESH = pl.DeviceIdType.MESH
LANES = 128
TILES = 3
CHUNK = TILES * LANES
SLOTS = 4
GROUPS = ((0,), (1, 2), (3, 7), (8, 17), (18, 22), (23,), (24,))
RELAY = 12
RELAY_AT = 14


def head_kernel(
    count, width, hidden_size,
    h_hbm, g_hbm, w_ref, z_ref, lse_ref,
    h_ref, g_ref, wq, wr, wp, wl, x_ref, qbuf, rbuf, pbuf, lbuf, rin, lin, yin, nst, fst, m_ref, s_ref, carry, edge_out, edge_in, relay_in, relay_mid, rx, qx, first_in,
    h_sem, g_sem, hops, wq_sem, wr_sem, wp_sem, wl_sem, nsend, nrecv, qsend, psend, ysend, rrecv, lrecv, yrecv, fsend, frecv, esend, erecv, relay_send, relay_recv, rx_send, rx_recv, qx_send, first_send, first_recv,
):
    h_copy = pltpu.make_async_copy(h_hbm, h_ref, h_sem)
    g_copy = pltpu.make_async_copy(g_hbm, g_ref, g_sem)
    h_copy.start()
    g_copy.start()
    rows, feats = h_ref.shape
    stride = (width // LANES) * LANES
    rest = width - stride
    col = lax.axis_index("col")
    row = lax.axis_index("row")
    core = lax.rem(row, 2)
    mate = row + 1 - 2 * core
    across = lax.rem(row + 2, 4)
    far = 3 - row
    shift = row * rest

    end = count - 1

    streams = {
        "far": (far, wq, wq_sem), "across": (across, wr, wr_sem), "mate": (mate, wp, wp_sem), "own": (row, wl, wl_sem)
    }

    def chunk_at(t):
        if isinstance(t, int) and t < 2:
            return t * RELAY
        return t - 1 + t // (RELAY + 1)

    def fetch(name, t):
        part, buf, sem = streams[name]
        chunk = t
        if name in ("far", "across"):
            chunk = chunk_at(t)
        start = pl.multiple_of(stride * part + CHUNK * chunk, LANES)
        slot = lax.rem(t, SLOTS)
        return pltpu.make_async_copy(w_ref.at[:, pl.ds(start, CHUNK)], buf.at[slot], sem.at[slot])

    barrier = pltpu.get_barrier_semaphore()

    def tell_column(sem, step):
        @pl.when((col + step >= 0) & (col + step < 4))
        def _():
            pl.semaphore_signal(sem, inc=1, device_id_type=MESH, device_id={"col": col + step})

    def tell_columns(sem):
        tell_column(sem, -1)
        tell_column(sem, 1)

    for k in (2, 3, 1):
        pl.semaphore_signal(barrier, inc=1, device_id_type=MESH, device_id={"row": lax.rem(row + k, 4)})
    tell_column(barrier, 1)
    below = (col + 2) // 3
    above = (5 - col) // 3
    beside = below + above

    h_copy.wait()
    for name, t in (("far", 0), ("far", 1), ("across", 0)):
        fetch(name, t).start()

    lane = lax.broadcasted_iota(jnp.int32, (rows, LANES), 1)
    sq = jnp.zeros((rows, LANES), jnp.float32)
    for j in range(feats // LANES):
        part = h_ref[:, j * LANES:(j + 1) * LANES].astype(jnp.float32)
        sq = sq + part * part
    sq = jnp.transpose(jnp.concatenate([sq, sq], axis=0))
    nst[row] = jnp.sum(sq, axis=0, keepdims=True)
    pl.semaphore_wait(barrier, 3 + below)
    tell_column(hops.at[0], -1)

    def norm_copy(k):
        return pltpu.make_async_remote_copy(
            src_ref=nst.at[row], dst_ref=nst.at[row], send_sem=nsend.at[k], recv_sem=nrecv.at[row],
            device_id={"row": lax.rem(row + k, 4)}, device_id_type=MESH,
        )

    for k in (2, 3, 1):
        norm_copy(k).start()
    for name, t in (
        *[(n, t) for t in range(1, SLOTS) for n in ("far", "across") if n == "across" or t > 1], *[(n, t) for t in range(SLOTS) for n in ("mate", "own")]
    ):
        fetch(name, t).start()
    for k in range(1, 4):
        peer = lax.rem(row + k, 4)
        pltpu.make_async_remote_copy(
            src_ref=nst.at[peer], dst_ref=nst.at[peer], send_sem=nsend.at[k], recv_sem=nrecv.at[peer],
            device_id={"row": peer}, device_id_type=MESH,
        ).wait_recv()
    g_copy.wait()
    total = nst[0] + nst[1] + nst[2] + nst[3]
    scale = lax.rsqrt(total / hidden_size + EPS)
    scale = jnp.transpose(jnp.broadcast_to(scale, (LANES, LANES)))[:rows]
    for j in range(feats // LANES):
        cols = slice(j * LANES, (j + 1) * LANES)
        x_ref[:, cols] = (h_ref[:, cols].astype(jnp.float32) * scale * g_ref[cols].reshape(1, LANES)).astype(jnp.bfloat16)

    def product(name, t):
        fetch(name, t).wait()
        return jnp.dot(x_ref[...], streams[name][1][lax.rem(t, SLOTS)], preferred_element_type=jnp.float32)

    def refill(name, t):
        @pl.when(t + SLOTS < count)
        def _():
            fetch(name, t + SLOTS).start()

    def mate_copy(src, dst, send, recv, i):
        return pltpu.make_async_remote_copy(
            src_ref=src.at[i], dst_ref=dst.at[i], send_sem=send, recv_sem=recv.at[i],
            device_id={"row": mate}, device_id_type=MESH,
        )

    most = pl.ds(0, (TILES - 1) * LANES)
    final = len(GROUPS) - 1

    def across_copy(k, where):
        return pltpu.make_async_remote_copy(
            src_ref=rbuf.at[where], dst_ref=yin.at[where], send_sem=ysend.at[k], recv_sem=yrecv.at[k],
            device_id={"row": across}, device_id_type=MESH,
        )

    def pieces(k):
        lo, hi = GROUPS[k][0], GROUPS[k][-1]
        if lo <= RELAY <= hi:
            return [(k, pl.ds(lo, RELAY - lo)), (len(GROUPS), pl.ds(RELAY + 1, hi - RELAY))]
        return [(k, pl.ds(lo, hi - lo + 1))]

    rx_copy = pltpu.make_async_remote_copy(
        src_ref=rbuf.at[end, :, most], dst_ref=rx, send_sem=rx_send, recv_sem=rx_recv,
        device_id={"row": mate}, device_id_type=MESH,
    )
    qx_copy = pltpu.make_async_remote_copy(
        src_ref=qx, dst_ref=yin.at[end, :, most], send_sem=qx_send, recv_sem=yrecv.at[final],
        device_id={"row": far}, device_id_type=MESH,
    )

    lead = pl.ds(0, LANES)
    rest_of = pl.ds(LANES, (TILES - 1) * LANES)

    def first_copy(k):
        src, dst, device = (
            (qbuf.at[0, :, lead], first_in, far),
            (rbuf.at[0, :, lead], yin.at[0, :, lead], across),
            (rbuf.at[0, :, rest_of], yin.at[0, :, rest_of], across),
        )[k]
        return pltpu.make_async_remote_copy(
            src_ref=src, dst_ref=dst, send_sem=first_send.at[k], recv_sem=first_recv.at[k],
            device_id={"row": device}, device_id_type=MESH,
        )

    def last_step():
        rbuf[end] = product("across", end)

        @pl.when(core == 0)
        def _():
            rx_copy.start()

        mate_copy(qbuf, rin, qsend, rrecv, end).wait_recv()

        @pl.when(core == 1)
        def _():
            rx_copy.wait_recv()
            qx[...] = qbuf[end, :, most] + rx[...]
            qx_copy.start()
            rbuf[end] = rbuf[end] + rin[end]
            across_copy(final, end).start()

    def each_group(k, act):
        for sem, where in pieces(k):
            act(across_copy(sem, where))

    late = col >= 3 - core
    early = col <= core

    def each_single(act):
        @pl.when(jnp.logical_not(late))
        def _():
            act(across_copy(len(GROUPS) + 1, RELAY))

        @pl.when(late)
        def _():
            act(across_copy(len(GROUPS) + 1, (RELAY, slice(None), pl.ds((TILES - 1) * LANES, LANES))))

    def relay_copy(k):
        src, dst, device = (
            (rbuf.at[RELAY, :, most], relay_in, {"col": core * (col - 2)}),
            (relay_in, relay_mid, {"row": across}),
            (relay_mid, yin.at[RELAY, :, most], {"col": 3 + core * (col - 1)}),
        )[k]
        return pltpu.make_async_remote_copy(
            src_ref=src, dst_ref=dst, send_sem=relay_send.at[k], recv_sem=relay_recv.at[k],
            device_id=device, device_id_type=MESH,
        )

    edge_copy = pltpu.make_async_remote_copy(
        src_ref=edge_out, dst_ref=edge_in, send_sem=esend, recv_sem=erecv,
        device_id={"row": mate}, device_id_type=MESH,
    )

    def far_step(t, i):
        qbuf[i] = product("far", t)
        mate_copy(qbuf, rin, qsend, rrecv, i).start()
        refill("far", t)

    def across_step(t, i):
        term = product("across", t)
        refill("across", t)
        mate_copy(qbuf, rin, qsend, rrecv, i).wait_recv()
        rbuf[i] = term + rin[i]

    def mate_step(i):
        pbuf[i] = product("mate", i)
        mate_copy(pbuf, lin, psend, lrecv, i).start()
        refill("mate", i)

    def own_step(i):
        lbuf[i] = product("own", i)
        refill("own", i)

    turn = lax.rem(LANES - shift, LANES)
    keep = lane < LANES - shift

    def arrive(i, first, last):
        mate_copy(pbuf, lin, psend, lrecv, i).wait_recv()
        if first:
            for k in range(3):
                first_copy(k).wait_recv()
        elif last:
            @pl.when(core == 0)
            def _():
                qx_copy.wait_recv()

            @pl.when(core == 1)
            def _():
                across_copy(final, end).wait_recv()
        else:
            for k in range(1, final):
                for sem, where in pieces(k):
                    @pl.when(i == where.start)
                    def _():
                        across_copy(sem, where).wait_recv()

            @pl.when(i == RELAY)
            def _():
                each_single(lambda copy: copy.wait_recv())

                @pl.when(late)
                def _():
                    relay_copy(2).wait_recv()
        full = lbuf[i] + lin[i] + yin[i]
        parts = [full[:, k * LANES:(k + 1) * LANES] for k in range(TILES)]
        if first:
            parts[0] = parts[0] + first_in[...]
            edge_out[...] = parts[0]

            @pl.when(core == 1)
            def _():
                edge_copy.start()
        if last:
            @pl.when(core == 0)
            def _():
                edge_copy.wait_recv()

            parts[-1] = jnp.where(core == 0, edge_in[...], parts[-1])
        rolled = [pltpu.roll(part, turn, 1) for part in parts]
        tiles = [jnp.where(keep, rolled[k], rolled[k + 1]) for k in range(TILES - 1)]
        at = 0
        if not first:
            tiles = [jnp.where(keep, carry[...], rolled[0])] + tiles
            at = pl.multiple_of(i * CHUNK - LANES, LANES)
        carry[...] = rolled[-1]
        z_ref[:, pl.ds(at, LANES * len(tiles))] = jnp.concatenate(tiles, axis=1)
        top = tiles[0]
        for tile in tiles[1:]:
            top = jnp.maximum(top, tile)
        if not first:
            top = jnp.maximum(top, m_ref[...])
        mass = jnp.exp(tiles[0] - top)
        for tile in tiles[1:]:
            mass = mass + jnp.exp(tile - top)
        if not first:
            mass = mass + s_ref[...] * jnp.exp(m_ref[...] - top)
        m_ref[...] = top
        s_ref[...] = mass

    far_step(0, 0)
    first_copy(0).start()
    rbuf[0] = product("across", 0)
    first_copy(1).start()
    refill("across", 0)

    @pl.when(col < 3)
    def _():
        pl.semaphore_wait(hops.at[0], 1)

    tell_columns(hops.at[1])
    far_step(1, RELAY)
    mate_copy(qbuf, rin, qsend, rrecv, 0).wait_recv()
    rbuf[0, :, LANES:] = rbuf[0, :, LANES:] + rin[0, :, LANES:]
    first_copy(2).start()
    far_step(2, 1)
    pl.semaphore_wait(hops.at[1], beside)
    tell_columns(hops.at[2])
    far_step(3, 2)
    across_step(1, RELAY)
    each_single(lambda copy: copy.start())

    @pl.when(late)
    def _():
        pl.semaphore_wait(hops.at[2], beside)
        relay_copy(0).start()

    @pl.loop(2, end)
    def _(t):
        @pl.when(t < end - 1)
        def _():
            far_step(t + 2, chunk_at(t + 2))

        i = chunk_at(t)
        across_step(t, i)
        for k in range(1, final):
            for sem, where in pieces(k):
                @pl.when(i == where.start + where.size - 1)
                def _():
                    across_copy(sem, where).start()

        @pl.when((t == RELAY_AT) & early)
        def _():
            relay_copy(0).wait_recv()
            relay_copy(1).start()

    last_step()

    @pl.when(jnp.logical_not(late))
    def _():
        pl.semaphore_wait(hops.at[2], beside)

    tell_columns(hops.at[3])

    @pl.loop(0, count)
    def _(i):
        mate_step(i)
        own_step(i)

    @pl.when(early)
    def _():
        relay_copy(1).wait_recv()
        relay_copy(2).start()

    pl.semaphore_wait(hops.at[3], beside)
    arrive(0, True, False)

    @pl.loop(1, end)
    def _(i):
        arrive(i, False, False)

    arrive(end, False, True)

    last = carry[...]
    z_ref[:, stride:] = last[:, :rest]
    last = jnp.where(lane < rest, last, -jnp.inf)
    top = jnp.maximum(m_ref[...], last)
    mass = s_ref[...] * jnp.exp(m_ref[...] - top) + jnp.exp(last - top)
    top = jnp.transpose(jnp.concatenate([top, top], axis=0))
    mass = jnp.transpose(jnp.concatenate([mass, mass], axis=0))
    peak = jnp.max(top, axis=0, keepdims=True)
    mass = jnp.sum(mass * jnp.exp(top - peak), axis=0, keepdims=True)
    me = col * 4 + row
    fst[me] = jnp.where(lane[:1] < rows, peak, mass)

    def stat_copy(c, r, slot):
        return pltpu.make_async_remote_copy(
            src_ref=fst.at[slot], dst_ref=fst.at[slot], send_sem=fsend.at[c * 4 + r], recv_sem=frecv.at[slot],
            device_id={"col": c, "row": r}, device_id_type=MESH,
        )

    def each_peer(act):
        for c in range(4):
            for r in range(4):
                @pl.when(me != c * 4 + r)
                def _():
                    act(c, r)

    each_peer(lambda c, r: stat_copy(c, r, me).start())
    for k in range(1, 16):
        peer = lax.rem(me + k, 16)
        stat_copy(col, row, peer).wait_recv()
    stats = fst[...]
    swapped = pltpu.roll(stats, LANES // 2, 2)
    peak = jnp.max(stats, axis=0)
    mass = jnp.sum(swapped * jnp.exp(stats - peak), axis=0)
    lse_ref[...] = peak + jnp.log(mass)

    for k in range(1, 4):
        norm_copy(k).wait_send()
    for src, dst, send, recv in ((qbuf, rin, qsend, rrecv), (pbuf, lin, psend, lrecv)):
        pltpu.make_async_remote_copy(
            src_ref=src, dst_ref=dst, send_sem=send, recv_sem=recv.at[0],
            device_id={"row": mate}, device_id_type=MESH,
        ).wait_send()
    for k in range(3):
        first_copy(k).wait_send()
    for k in range(1, final):
        each_group(k, lambda copy: copy.wait_send())
    each_single(lambda copy: copy.wait_send())

    @pl.when(core == 0)
    def _():
        rx_copy.wait_send()

    @pl.when(core == 1)
    def _():
        qx_copy.wait_send()
        across_copy(final, end).wait_send()

    @pl.when(late)
    def _():
        relay_copy(0).wait_send()

    @pl.when(early)
    def _():
        relay_copy(1).wait_send()
        relay_copy(2).wait_send()

    @pl.when(core == 1)
    def _():
        edge_copy.wait_send()

    each_peer(lambda c, r: stat_copy(c, r, me).wait_send())


def solution(mesh):
    def local_head(hidden, norm_gain, w_head):
        rows, feats = hidden.shape
        width = w_head.shape[1] // 4
        count = (width // LANES + 1) // TILES
        block = (count, rows, CHUNK)
        dma = pltpu.SemaphoreType.DMA

        def body(*refs):
            head_kernel(count, width, feats * 4, *refs)

        z, lse = pl.pallas_call(
            body,
            out_shape=(
                jax.ShapeDtypeStruct((rows, width), jnp.float32),
                jax.ShapeDtypeStruct((1, LANES), jnp.float32),
            ),
            in_specs=[
                pl.BlockSpec(memory_space=pltpu.HBM),
                pl.BlockSpec(memory_space=pltpu.HBM),
                pl.BlockSpec(memory_space=pltpu.HBM),
            ],
            out_specs=(pl.BlockSpec(memory_space=pltpu.VMEM), pl.BlockSpec(memory_space=pltpu.VMEM)),
            scratch_shapes=[
                pltpu.VMEM((rows, feats), hidden.dtype),
                pltpu.VMEM((feats,), jnp.float32),
                *[pltpu.VMEM((SLOTS, feats, CHUNK), jnp.bfloat16) for _ in range(4)],
                pltpu.VMEM((rows, feats), jnp.bfloat16),
                *[pltpu.VMEM(block, jnp.float32) for _ in range(7)],
                pltpu.VMEM((4, 1, LANES), jnp.float32),
                pltpu.VMEM((16, 1, LANES), jnp.float32),
                *[pltpu.VMEM((rows, LANES), jnp.float32) for _ in range(5)],
                *[pltpu.VMEM((rows, (TILES - 1) * LANES), jnp.float32) for _ in range(4)],
                pltpu.VMEM((rows, LANES), jnp.float32),
                dma, dma, pltpu.SemaphoreType.REGULAR((4,)),
                *[dma((SLOTS,)) for _ in range(4)], dma((4,)), dma((4,)),
                dma, dma, dma((len(GROUPS) + 2,)), dma((count,)), dma((count,)), dma((len(GROUPS) + 2,)), dma((16,)), dma((16,)), dma, dma, dma((3,)), dma((3,)), dma, dma, dma,
                dma((3,)), dma((3,)),
            ],
            compiler_params=pltpu.CompilerParams(
                collective_id=0, has_side_effects=True, vmem_limit_bytes=48 * 1024 * 1024
            ),
            name="head",
        )(pltpu.with_memory_space_constraint(hidden, pltpu.HBM), pltpu.with_memory_space_constraint(norm_gain, pltpu.HBM), w_head)
        log_norm = lse[0, :rows]
        return z - log_norm[:, None], log_norm

    return jax.shard_map(
        local_head,
        mesh=mesh,
        in_specs=(P("dp", "row"), P("row"), P("row", "col")),
        out_specs=(P("dp", ("col", "row")), P("dp")),
        check_vma=False,
    )
```

```python
import jax
import jax.numpy as jnp
from jax import lax
from jax.experimental import pallas as pl
from jax.experimental.pallas import tpu as pltpu
from jax.sharding import PartitionSpec as P

EPS = 1e-5
MESH = pl.DeviceIdType.MESH
LANES = 128
TILES = 3
CHUNK = TILES * LANES
SLOTS = 4
GROUPS = ((0,), (1, 2), (3, 6), (8, 17), (18, 22), (23,), (24,))
RELAY = 7
RELAY_AT = 14


def head_kernel(
    count, width, hidden_size,
    h_hbm, g_hbm, w_ref, z_ref, lse_ref,
    h_ref, g_ref, wq, wr, wp, wl, x_ref, qbuf, rbuf, pbuf, lbuf, rin, lin, yin, nst, fst, m_ref, s_ref, carry, edge_out, edge_in, relay_in, relay_mid, rx, qx, first_in,
    h_sem, g_sem, hops, wq_sem, wr_sem, wp_sem, wl_sem, nsend, nrecv, qsend, psend, ysend, rrecv, lrecv, yrecv, fsend, frecv, esend, erecv, relay_send, relay_recv, rx_send, rx_recv, qx_send, first_send, first_recv,
):
    h_copy = pltpu.make_async_copy(h_hbm, h_ref, h_sem)
    g_copy = pltpu.make_async_copy(g_hbm, g_ref, g_sem)
    h_copy.start()
    g_copy.start()
    rows, feats = h_ref.shape
    stride = (width // LANES) * LANES
    rest = width - stride
    col = lax.axis_index("col")
    row = lax.axis_index("row")
    core = lax.rem(row, 2)
    mate = row + 1 - 2 * core
    across = lax.rem(row + 2, 4)
    far = 3 - row
    shift = row * rest

    end = count - 1

    streams = {
        "far": (far, wq, wq_sem), "across": (across, wr, wr_sem), "mate": (mate, wp, wp_sem), "own": (row, wl, wl_sem)
    }

    def chunk_at(t):
        if isinstance(t, int) and t < 2:
            return t * RELAY
        return t - 1 + (t + end - RELAY) // count

    def fetch(name, t):
        part, buf, sem = streams[name]
        chunk = t
        if name in ("far", "across"):
            chunk = chunk_at(t)
        start = pl.multiple_of(stride * part + CHUNK * chunk, LANES)
        slot = lax.rem(t, SLOTS)
        return pltpu.make_async_copy(w_ref.at[:, pl.ds(start, CHUNK)], buf.at[slot], sem.at[slot])

    barrier = pltpu.get_barrier_semaphore()

    def tell_column(sem, step):
        @pl.when((col + step >= 0) & (col + step < 4))
        def _():
            pl.semaphore_signal(sem, inc=1, device_id_type=MESH, device_id={"col": col + step})

    def tell_columns(sem):
        tell_column(sem, -1)
        tell_column(sem, 1)

    for k in (2, 3, 1):
        pl.semaphore_signal(barrier, inc=1, device_id_type=MESH, device_id={"row": lax.rem(row + k, 4)})
    tell_column(barrier, 1)
    below = (col + 2) // 3
    above = (5 - col) // 3
    beside = below + above

    h_copy.wait()
    for name, t in (("far", 0), ("far", 1), ("across", 0)):
        fetch(name, t).start()

    lane = lax.broadcasted_iota(jnp.int32, (rows, LANES), 1)
    sq = jnp.zeros((rows, LANES), jnp.float32)
    for j in range(feats // LANES):
        part = h_ref[:, j * LANES:(j + 1) * LANES].astype(jnp.float32)
        sq = sq + part * part
    sq = jnp.transpose(jnp.concatenate([sq, sq], axis=0))
    nst[row] = jnp.sum(sq, axis=0, keepdims=True)
    pl.semaphore_wait(barrier, 3 + below)

    def norm_copy(k):
        return pltpu.make_async_remote_copy(
            src_ref=nst.at[row], dst_ref=nst.at[row], send_sem=nsend.at[k], recv_sem=nrecv.at[row],
            device_id={"row": lax.rem(row + k, 4)}, device_id_type=MESH,
        )

    for k in (2, 3, 1):
        norm_copy(k).start()
    tell_column(hops.at[0], -1)
    for name, t in (
        *[(n, t) for t in range(1, SLOTS) for n in ("far", "across") if n == "across" or t > 1], *[(n, t) for t in range(SLOTS) for n in ("mate", "own")]
    ):
        fetch(name, t).start()
    for k in range(1, 4):
        peer = lax.rem(row + k, 4)
        pltpu.make_async_remote_copy(
            src_ref=nst.at[peer], dst_ref=nst.at[peer], send_sem=nsend.at[k], recv_sem=nrecv.at[peer],
            device_id={"row": peer}, device_id_type=MESH,
        ).wait_recv()
    g_copy.wait()
    total = nst[0] + nst[1] + nst[2] + nst[3]
    scale = lax.rsqrt(total / hidden_size + EPS)
    scale = jnp.transpose(jnp.broadcast_to(scale, (LANES, LANES)))[:rows]
    for j in range(feats // LANES):
        cols = slice(j * LANES, (j + 1) * LANES)
        x_ref[:, cols] = (h_ref[:, cols].astype(jnp.float32) * scale * g_ref[cols].reshape(1, LANES)).astype(jnp.bfloat16)

    def product(name, t):
        fetch(name, t).wait()
        return jnp.dot(x_ref[...], streams[name][1][lax.rem(t, SLOTS)], preferred_element_type=jnp.float32)

    def refill(name, t):
        @pl.when(t + SLOTS < count)
        def _():
            fetch(name, t + SLOTS).start()

    def mate_copy(src, dst, send, recv, i):
        return pltpu.make_async_remote_copy(
            src_ref=src.at[i], dst_ref=dst.at[i], send_sem=send, recv_sem=recv.at[i],
            device_id={"row": mate}, device_id_type=MESH,
        )

    most = pl.ds(0, (TILES - 1) * LANES)
    final = len(GROUPS) - 1

    def across_copy(k, where):
        return pltpu.make_async_remote_copy(
            src_ref=rbuf.at[where], dst_ref=yin.at[where], send_sem=ysend.at[k], recv_sem=yrecv.at[k],
            device_id={"row": across}, device_id_type=MESH,
        )

    def pieces(k):
        lo, hi = GROUPS[k][0], GROUPS[k][-1]
        if lo <= RELAY <= hi:
            return [(k, pl.ds(lo, RELAY - lo)), (len(GROUPS), pl.ds(RELAY + 1, hi - RELAY))]
        return [(k, pl.ds(lo, hi - lo + 1))]

    rx_copy = pltpu.make_async_remote_copy(
        src_ref=rbuf.at[end, :, most], dst_ref=rx, send_sem=rx_send, recv_sem=rx_recv,
        device_id={"row": mate}, device_id_type=MESH,
    )
    qx_copy = pltpu.make_async_remote_copy(
        src_ref=qx, dst_ref=yin.at[end, :, most], send_sem=qx_send, recv_sem=yrecv.at[final],
        device_id={"row": far}, device_id_type=MESH,
    )

    lead = pl.ds(0, LANES)
    rest_of = pl.ds(LANES, (TILES - 1) * LANES)

    def first_copy(k):
        src, dst, device = (
            (qbuf.at[0, :, lead], first_in, far),
            (rbuf.at[0, :, lead], yin.at[0, :, lead], across),
            (rbuf.at[0, :, rest_of], yin.at[0, :, rest_of], across),
        )[k]
        return pltpu.make_async_remote_copy(
            src_ref=src, dst_ref=dst, send_sem=first_send.at[k], recv_sem=first_recv.at[k],
            device_id={"row": device}, device_id_type=MESH,
        )

    def last_step():
        rbuf[end] = product("across", end)

        @pl.when(core == 0)
        def _():
            rx_copy.start()

        mate_copy(qbuf, rin, qsend, rrecv, end).wait_recv()

        @pl.when(core == 1)
        def _():
            rx_copy.wait_recv()
            qx[...] = qbuf[end, :, most] + rx[...]
            qx_copy.start()
            rbuf[end] = rbuf[end] + rin[end]
            across_copy(final, end).start()

    def each_group(k, act):
        for sem, where in pieces(k):
            act(across_copy(sem, where))

    late = col >= 3 - core
    early = col <= core

    def each_single(act):
        @pl.when(jnp.logical_not(late))
        def _():
            act(across_copy(len(GROUPS) + 1, RELAY))

        @pl.when(late)
        def _():
            act(across_copy(len(GROUPS) + 1, (RELAY, slice(None), pl.ds((TILES - 1) * LANES, LANES))))

    def relay_copy(k):
        src, dst, device = (
            (rbuf.at[RELAY, :, most], relay_in, {"col": core * (col - 2)}),
            (relay_in, relay_mid, {"row": across}),
            (relay_mid, yin.at[RELAY, :, most], {"col": 3 + core * (col - 1)}),
        )[k]
        return pltpu.make_async_remote_copy(
            src_ref=src, dst_ref=dst, send_sem=relay_send.at[k], recv_sem=relay_recv.at[k],
            device_id=device, device_id_type=MESH,
        )

    edge_copy = pltpu.make_async_remote_copy(
        src_ref=edge_out, dst_ref=edge_in, send_sem=esend, recv_sem=erecv,
        device_id={"row": mate}, device_id_type=MESH,
    )

    def far_step(t, i):
        qbuf[i] = product("far", t)
        mate_copy(qbuf, rin, qsend, rrecv, i).start()
        refill("far", t)

    def across_step(t, i):
        term = product("across", t)
        refill("across", t)
        mate_copy(qbuf, rin, qsend, rrecv, i).wait_recv()
        rbuf[i] = term + rin[i]

    def mate_step(i):
        pbuf[i] = product("mate", i)
        mate_copy(pbuf, lin, psend, lrecv, i).start()
        refill("mate", i)

    def own_step(i):
        lbuf[i] = product("own", i)
        refill("own", i)

    turn = lax.rem(LANES - shift, LANES)
    keep = lane < LANES - shift

    def arrive(i, first, last):
        mate_copy(pbuf, lin, psend, lrecv, i).wait_recv()
        if first:
            for k in range(3):
                first_copy(k).wait_recv()
        elif last:
            @pl.when(core == 0)
            def _():
                qx_copy.wait_recv()

            @pl.when(core == 1)
            def _():
                across_copy(final, end).wait_recv()
        else:
            for k in range(1, final):
                for sem, where in pieces(k):
                    @pl.when(i == where.start)
                    def _():
                        across_copy(sem, where).wait_recv()

            @pl.when(i == RELAY)
            def _():
                each_single(lambda copy: copy.wait_recv())

                @pl.when(late)
                def _():
                    relay_copy(2).wait_recv()
        full = lbuf[i] + lin[i] + yin[i]
        parts = [full[:, k * LANES:(k + 1) * LANES] for k in range(TILES)]
        if first:
            parts[0] = parts[0] + first_in[...]
            edge_out[...] = parts[0]

            @pl.when(core == 1)
            def _():
                edge_copy.start()
        if last:
            @pl.when(core == 0)
            def _():
                edge_copy.wait_recv()

            parts[-1] = jnp.where(core == 0, edge_in[...], parts[-1])
        rolled = [pltpu.roll(part, turn, 1) for part in parts]
        tiles = [jnp.where(keep, rolled[k], rolled[k + 1]) for k in range(TILES - 1)]
        at = 0
        if not first:
            tiles = [jnp.where(keep, carry[...], rolled[0])] + tiles
            at = pl.multiple_of(i * CHUNK - LANES, LANES)
        carry[...] = rolled[-1]
        z_ref[:, pl.ds(at, LANES * len(tiles))] = jnp.concatenate(tiles, axis=1)
        top = tiles[0]
        for tile in tiles[1:]:
            top = jnp.maximum(top, tile)
        if not first:
            top = jnp.maximum(top, m_ref[...])
        mass = jnp.exp(tiles[0] - top)
        for tile in tiles[1:]:
            mass = mass + jnp.exp(tile - top)
        if not first:
            mass = mass + s_ref[...] * jnp.exp(m_ref[...] - top)
        m_ref[...] = top
        s_ref[...] = mass

    far_step(0, 0)
    first_copy(0).start()
    rbuf[0] = product("across", 0)
    first_copy(1).start()
    refill("across", 0)

    @pl.when(col < 3)
    def _():
        pl.semaphore_wait(hops.at[0], 1)

    tell_columns(hops.at[1])
    far_step(1, RELAY)
    mate_copy(qbuf, rin, qsend, rrecv, 0).wait_recv()
    rbuf[0, :, LANES:] = rbuf[0, :, LANES:] + rin[0, :, LANES:]
    first_copy(2).start()
    far_step(2, 1)
    pl.semaphore_wait(hops.at[1], beside)
    tell_columns(hops.at[2])
    far_step(3, 2)
    across_step(1, RELAY)
    each_single(lambda copy: copy.start())

    @pl.when(late)
    def _():
        pl.semaphore_wait(hops.at[2], beside)
        relay_copy(0).start()

    @pl.loop(2, end)
    def _(t):
        @pl.when(t < end - 1)
        def _():
            far_step(t + 2, chunk_at(t + 2))

        i = chunk_at(t)
        across_step(t, i)
        for k in range(1, final):
            for sem, where in pieces(k):
                @pl.when(i == where.start + where.size - 1)
                def _():
                    across_copy(sem, where).start()

        @pl.when((t == RELAY_AT) & early)
        def _():
            relay_copy(0).wait_recv()
            relay_copy(1).start()

    last_step()

    @pl.when(jnp.logical_not(late))
    def _():
        pl.semaphore_wait(hops.at[2], beside)

    tell_columns(hops.at[3])

    @pl.loop(0, count)
    def _(i):
        mate_step(i)
        own_step(i)

    @pl.when(early)
    def _():
        relay_copy(1).wait_recv()
        relay_copy(2).start()

    pl.semaphore_wait(hops.at[3], beside)
    arrive(0, True, False)

    @pl.loop(1, end)
    def _(i):
        arrive(i, False, False)

    arrive(end, False, True)

    last = carry[...]
    z_ref[:, stride:] = last[:, :rest]
    last = jnp.where(lane < rest, last, -jnp.inf)
    top = jnp.maximum(m_ref[...], last)
    mass = s_ref[...] * jnp.exp(m_ref[...] - top) + jnp.exp(last - top)
    top = jnp.transpose(jnp.concatenate([top, top], axis=0))
    mass = jnp.transpose(jnp.concatenate([mass, mass], axis=0))
    peak = jnp.max(top, axis=0, keepdims=True)
    mass = jnp.sum(mass * jnp.exp(top - peak), axis=0, keepdims=True)
    me = col * 4 + row
    fst[me] = jnp.where(lane[:1] < rows, peak, mass)

    def stat_copy(c, r, slot):
        return pltpu.make_async_remote_copy(
            src_ref=fst.at[slot], dst_ref=fst.at[slot], send_sem=fsend.at[c * 4 + r], recv_sem=frecv.at[slot],
            device_id={"col": c, "row": r}, device_id_type=MESH,
        )

    def each_peer(act):
        for c in range(4):
            for r in range(4):
                @pl.when(me != c * 4 + r)
                def _():
                    act(c, r)

    each_peer(lambda c, r: stat_copy(c, r, me).start())
    for k in range(1, 16):
        peer = lax.rem(me + k, 16)
        stat_copy(col, row, peer).wait_recv()
    stats = fst[...]
    swapped = pltpu.roll(stats, LANES // 2, 2)
    peak = jnp.max(stats, axis=0)
    mass = jnp.sum(swapped * jnp.exp(stats - peak), axis=0)
    lse_ref[...] = peak + jnp.log(mass)

    for k in range(1, 4):
        norm_copy(k).wait_send()
    for src, dst, send, recv in ((qbuf, rin, qsend, rrecv), (pbuf, lin, psend, lrecv)):
        pltpu.make_async_remote_copy(
            src_ref=src, dst_ref=dst, send_sem=send, recv_sem=recv.at[0],
            device_id={"row": mate}, device_id_type=MESH,
        ).wait_send()
    for k in range(3):
        first_copy(k).wait_send()
    for k in range(1, final):
        each_group(k, lambda copy: copy.wait_send())
    each_single(lambda copy: copy.wait_send())

    @pl.when(core == 0)
    def _():
        rx_copy.wait_send()

    @pl.when(core == 1)
    def _():
        qx_copy.wait_send()
        across_copy(final, end).wait_send()

    @pl.when(late)
    def _():
        relay_copy(0).wait_send()

    @pl.when(early)
    def _():
        relay_copy(1).wait_send()
        relay_copy(2).wait_send()

    @pl.when(core == 1)
    def _():
        edge_copy.wait_send()

    each_peer(lambda c, r: stat_copy(c, r, me).wait_send())


def solution(mesh):
    def local_head(hidden, norm_gain, w_head):
        rows, feats = hidden.shape
        width = w_head.shape[1] // 4
        count = (width // LANES + 1) // TILES
        block = (count, rows, CHUNK)
        dma = pltpu.SemaphoreType.DMA

        def body(*refs):
            head_kernel(count, width, feats * 4, *refs)

        z, lse = pl.pallas_call(
            body,
            out_shape=(
                jax.ShapeDtypeStruct((rows, width), jnp.float32),
                jax.ShapeDtypeStruct((1, LANES), jnp.float32),
            ),
            in_specs=[
                pl.BlockSpec(memory_space=pltpu.HBM),
                pl.BlockSpec(memory_space=pltpu.HBM),
                pl.BlockSpec(memory_space=pltpu.HBM),
            ],
            out_specs=(pl.BlockSpec(memory_space=pltpu.VMEM), pl.BlockSpec(memory_space=pltpu.VMEM)),
            scratch_shapes=[
                pltpu.VMEM((rows, feats), hidden.dtype),
                pltpu.VMEM((feats,), jnp.float32),
                *[pltpu.VMEM((SLOTS, feats, CHUNK), jnp.bfloat16) for _ in range(4)],
                pltpu.VMEM((rows, feats), jnp.bfloat16),
                *[pltpu.VMEM(block, jnp.float32) for _ in range(7)],
                pltpu.VMEM((4, 1, LANES), jnp.float32),
                pltpu.VMEM((16, 1, LANES), jnp.float32),
                *[pltpu.VMEM((rows, LANES), jnp.float32) for _ in range(5)],
                *[pltpu.VMEM((rows, (TILES - 1) * LANES), jnp.float32) for _ in range(4)],
                pltpu.VMEM((rows, LANES), jnp.float32),
                dma, dma, pltpu.SemaphoreType.REGULAR((4,)),
                *[dma((SLOTS,)) for _ in range(4)], dma((4,)), dma((4,)),
                dma, dma, dma((len(GROUPS) + 2,)), dma((count,)), dma((count,)), dma((len(GROUPS) + 2,)), dma((16,)), dma((16,)), dma, dma, dma((3,)), dma((3,)), dma, dma, dma,
                dma((3,)), dma((3,)),
            ],
            compiler_params=pltpu.CompilerParams(
                collective_id=0, has_side_effects=True, vmem_limit_bytes=48 * 1024 * 1024
            ),
            name="head",
        )(pltpu.with_memory_space_constraint(hidden, pltpu.HBM), pltpu.with_memory_space_constraint(norm_gain, pltpu.HBM), w_head)
        log_norm = lse[0, :rows]
        return z - log_norm[:, None], log_norm

    return jax.shard_map(
        local_head,
        mesh=mesh,
        in_specs=(P("dp", "row"), P("row"), P("row", "col")),
        out_specs=(P("dp", ("col", "row")), P("dp")),
        check_vma=False,
    )
```

```python
import jax
import jax.numpy as jnp
from jax import lax
from jax.experimental import pallas as pl
from jax.experimental.pallas import tpu as pltpu
from jax.sharding import PartitionSpec as P

EPS = 1e-5
MESH = pl.DeviceIdType.MESH
LANES = 128
TILES = 3
CHUNK = TILES * LANES
SLOTS = 4
GROUPS = ((0,), (1, 2), (3, 6), (8, 17), (18, 22), (23,), (24,))
RELAY = 7
RELAY_AT = 14


def head_kernel(
    count, width, hidden_size,
    h_hbm, g_hbm, w_ref, z_ref, lse_ref,
    h_ref, g_ref, wq, wr, wp, wl, x_ref, qbuf, rbuf, pbuf, lbuf, rin, lin, yin, nst, fst, m_ref, s_ref, carry, edge_out, edge_in, relay_in, relay_mid, rx, qx, first_in,
    h_sem, g_sem, hops, wq_sem, wr_sem, wp_sem, wl_sem, nsend, nrecv, qsend, psend, ysend, rrecv, lrecv, yrecv, fsend, frecv, esend, erecv, relay_send, relay_recv, rx_send, rx_recv, qx_send, first_send, first_recv,
):
    h_copy = pltpu.make_async_copy(h_hbm, h_ref, h_sem)
    g_copy = pltpu.make_async_copy(g_hbm, g_ref, g_sem)
    h_copy.start()
    g_copy.start()
    rows, feats = h_ref.shape
    stride = (width // LANES) * LANES
    rest = width - stride
    col = lax.axis_index("col")
    row = lax.axis_index("row")
    core = lax.rem(row, 2)
    mate = row + 1 - 2 * core
    across = lax.rem(row + 2, 4)
    far = 3 - row
    shift = row * rest

    end = count - 1

    streams = {
        "far": (far, wq, wq_sem), "across": (across, wr, wr_sem), "mate": (mate, wp, wp_sem), "own": (row, wl, wl_sem)
    }

    def chunk_at(t):
        if isinstance(t, int) and t < 2:
            return t * RELAY
        return t - 1 + (t + end - RELAY) // count

    def fetch(name, t):
        part, buf, sem = streams[name]
        chunk = t
        if name in ("far", "across"):
            chunk = chunk_at(t)
        start = pl.multiple_of(stride * part + CHUNK * chunk, LANES)
        slot = lax.rem(t, SLOTS)
        return pltpu.make_async_copy(w_ref.at[:, pl.ds(start, CHUNK)], buf.at[slot], sem.at[slot])

    barrier = pltpu.get_barrier_semaphore()

    def tell_column(sem, step):
        @pl.when((col + step >= 0) & (col + step < 4))
        def _():
            pl.semaphore_signal(sem, inc=1, device_id_type=MESH, device_id={"col": col + step})

    def tell_columns(sem):
        tell_column(sem, -1)
        tell_column(sem, 1)

    for k in (2, 3, 1):
        pl.semaphore_signal(barrier, inc=1, device_id_type=MESH, device_id={"row": lax.rem(row + k, 4)})
    tell_column(barrier, 1)
    below = (col + 2) // 3
    above = (5 - col) // 3
    beside = below + above

    h_copy.wait()
    for name, t in (("far", 0), ("far", 1), ("across", 0)):
        fetch(name, t).start()

    lane = lax.broadcasted_iota(jnp.int32, (rows, LANES), 1)
    sq = jnp.zeros((rows, LANES), jnp.float32)
    for j in range(feats // LANES):
        part = h_ref[:, j * LANES:(j + 1) * LANES].astype(jnp.float32)
        sq = sq + part * part
    sq = jnp.transpose(jnp.concatenate([sq, sq], axis=0))
    nst[row] = jnp.sum(sq, axis=0, keepdims=True)
    pl.semaphore_wait(barrier, 3 + below)

    def norm_copy(k):
        return pltpu.make_async_remote_copy(
            src_ref=nst.at[row], dst_ref=nst.at[row], send_sem=nsend.at[k], recv_sem=nrecv.at[row],
            device_id={"row": lax.rem(row + k, 4)}, device_id_type=MESH,
        )

    for k in (2, 3, 1):
        norm_copy(k).start()
    tell_column(hops.at[0], -1)
    for t in range(1, SLOTS):
        if t > 1:
            fetch("far", t).start()
        fetch("across", t).start()
    for k in range(1, 4):
        peer = lax.rem(row + k, 4)
        pltpu.make_async_remote_copy(
            src_ref=nst.at[peer], dst_ref=nst.at[peer], send_sem=nsend.at[k], recv_sem=nrecv.at[peer],
            device_id={"row": peer}, device_id_type=MESH,
        ).wait_recv()
    g_copy.wait()
    total = nst[0] + nst[1] + nst[2] + nst[3]
    scale = lax.rsqrt(total / hidden_size + EPS)
    scale = jnp.transpose(jnp.broadcast_to(scale, (LANES, LANES)))[:rows]
    for j in range(feats // LANES):
        cols = slice(j * LANES, (j + 1) * LANES)
        x_ref[:, cols] = (h_ref[:, cols].astype(jnp.float32) * scale * g_ref[cols].reshape(1, LANES)).astype(jnp.bfloat16)

    def product(name, t):
        fetch(name, t).wait()
        return jnp.dot(x_ref[...], streams[name][1][lax.rem(t, SLOTS)], preferred_element_type=jnp.float32)

    def refill(name, t):
        @pl.when(t + SLOTS < count)
        def _():
            fetch(name, t + SLOTS).start()

    def mate_copy(src, dst, send, recv, i):
        return pltpu.make_async_remote_copy(
            src_ref=src.at[i], dst_ref=dst.at[i], send_sem=send, recv_sem=recv.at[i],
            device_id={"row": mate}, device_id_type=MESH,
        )

    most = pl.ds(0, (TILES - 1) * LANES)
    final = len(GROUPS) - 1

    def across_copy(k, where):
        return pltpu.make_async_remote_copy(
            src_ref=rbuf.at[where], dst_ref=yin.at[where], send_sem=ysend.at[k], recv_sem=yrecv.at[k],
            device_id={"row": across}, device_id_type=MESH,
        )

    def pieces(k):
        lo, hi = GROUPS[k][0], GROUPS[k][-1]
        if lo <= RELAY <= hi:
            return [(k, pl.ds(lo, RELAY - lo)), (len(GROUPS), pl.ds(RELAY + 1, hi - RELAY))]
        return [(k, pl.ds(lo, hi - lo + 1))]

    rx_copy = pltpu.make_async_remote_copy(
        src_ref=rbuf.at[end, :, most], dst_ref=rx, send_sem=rx_send, recv_sem=rx_recv,
        device_id={"row": mate}, device_id_type=MESH,
    )
    qx_copy = pltpu.make_async_remote_copy(
        src_ref=qx, dst_ref=yin.at[end, :, most], send_sem=qx_send, recv_sem=yrecv.at[final],
        device_id={"row": far}, device_id_type=MESH,
    )

    lead = pl.ds(0, LANES)
    rest_of = pl.ds(LANES, (TILES - 1) * LANES)

    def first_copy(k):
        src, dst, device = (
            (qbuf.at[0, :, lead], first_in, far),
            (rbuf.at[0, :, lead], yin.at[0, :, lead], across),
            (rbuf.at[0, :, rest_of], yin.at[0, :, rest_of], across),
        )[k]
        return pltpu.make_async_remote_copy(
            src_ref=src, dst_ref=dst, send_sem=first_send.at[k], recv_sem=first_recv.at[k],
            device_id={"row": device}, device_id_type=MESH,
        )

    def last_step():
        rbuf[end] = product("across", end)

        @pl.when(core == 0)
        def _():
            rx_copy.start()

        mate_copy(qbuf, rin, qsend, rrecv, end).wait_recv()

        @pl.when(core == 1)
        def _():
            rx_copy.wait_recv()
            qx[...] = qbuf[end, :, most] + rx[...]
            qx_copy.start()
            rbuf[end] = rbuf[end] + rin[end]
            across_copy(final, end).start()

    def each_group(k, act):
        for sem, where in pieces(k):
            act(across_copy(sem, where))

    late = col >= 3 - core
    early = col <= core

    def each_single(act):
        @pl.when(jnp.logical_not(late))
        def _():
            act(across_copy(len(GROUPS) + 1, RELAY))

        @pl.when(late)
        def _():
            act(across_copy(len(GROUPS) + 1, (RELAY, slice(None), pl.ds((TILES - 1) * LANES, LANES))))

    def relay_copy(k):
        src, dst, device = (
            (rbuf.at[RELAY, :, most], relay_in, {"col": core * (col - 2)}),
            (relay_in, relay_mid, {"row": across}),
            (relay_mid, yin.at[RELAY, :, most], {"col": 3 + core * (col - 1)}),
        )[k]
        return pltpu.make_async_remote_copy(
            src_ref=src, dst_ref=dst, send_sem=relay_send.at[k], recv_sem=relay_recv.at[k],
            device_id=device, device_id_type=MESH,
        )

    edge_copy = pltpu.make_async_remote_copy(
        src_ref=edge_out, dst_ref=edge_in, send_sem=esend, recv_sem=erecv,
        device_id={"row": mate}, device_id_type=MESH,
    )

    def far_step(t, i):
        qbuf[i] = product("far", t)
        mate_copy(qbuf, rin, qsend, rrecv, i).start()
        refill("far", t)

    def across_step(t, i):
        term = product("across", t)
        refill("across", t)
        mate_copy(qbuf, rin, qsend, rrecv, i).wait_recv()
        rbuf[i] = term + rin[i]

    def mate_step(i):
        pbuf[i] = product("mate", i)
        mate_copy(pbuf, lin, psend, lrecv, i).start()
        refill("mate", i)

    def own_step(i):
        lbuf[i] = product("own", i)
        refill("own", i)

    turn = lax.rem(LANES - shift, LANES)
    keep = lane < LANES - shift

    def arrive(i, first, last):
        mate_copy(pbuf, lin, psend, lrecv, i).wait_recv()
        if first:
            for k in range(3):
                first_copy(k).wait_recv()
        elif last:
            @pl.when(core == 0)
            def _():
                qx_copy.wait_recv()

            @pl.when(core == 1)
            def _():
                across_copy(final, end).wait_recv()
        else:
            for k in range(1, final):
                for sem, where in pieces(k):
                    @pl.when(i == where.start)
                    def _():
                        across_copy(sem, where).wait_recv()

            @pl.when(i == RELAY)
            def _():
                each_single(lambda copy: copy.wait_recv())

                @pl.when(late)
                def _():
                    relay_copy(2).wait_recv()
        full = lbuf[i] + lin[i] + yin[i]
        parts = [full[:, k * LANES:(k + 1) * LANES] for k in range(TILES)]
        if first:
            parts[0] = parts[0] + first_in[...]
            edge_out[...] = parts[0]

            @pl.when(core == 1)
            def _():
                edge_copy.start()
        if last:
            @pl.when(core == 0)
            def _():
                edge_copy.wait_recv()

            parts[-1] = jnp.where(core == 0, edge_in[...], parts[-1])
        rolled = [pltpu.roll(part, turn, 1) for part in parts]
        tiles = [jnp.where(keep, rolled[k], rolled[k + 1]) for k in range(TILES - 1)]
        at = 0
        if not first:
            tiles = [jnp.where(keep, carry[...], rolled[0])] + tiles
            at = pl.multiple_of(i * CHUNK - LANES, LANES)
        carry[...] = rolled[-1]
        z_ref[:, pl.ds(at, LANES * len(tiles))] = jnp.concatenate(tiles, axis=1)
        top = tiles[0]
        for tile in tiles[1:]:
            top = jnp.maximum(top, tile)
        if not first:
            top = jnp.maximum(top, m_ref[...])
        mass = jnp.exp(tiles[0] - top)
        for tile in tiles[1:]:
            mass = mass + jnp.exp(tile - top)
        if not first:
            mass = mass + s_ref[...] * jnp.exp(m_ref[...] - top)
        m_ref[...] = top
        s_ref[...] = mass

    far_step(0, 0)
    first_copy(0).start()
    rbuf[0] = product("across", 0)
    first_copy(1).start()
    refill("across", 0)

    @pl.when(col < 3)
    def _():
        pl.semaphore_wait(hops.at[0], 1)

    tell_columns(hops.at[1])
    far_step(1, RELAY)
    mate_copy(qbuf, rin, qsend, rrecv, 0).wait_recv()
    rbuf[0, :, LANES:] = rbuf[0, :, LANES:] + rin[0, :, LANES:]
    first_copy(2).start()
    for t in range(SLOTS):
        fetch("mate", t).start()
        fetch("own", t).start()
    far_step(2, 1)
    pl.semaphore_wait(hops.at[1], beside)
    tell_columns(hops.at[2])
    far_step(3, 2)
    across_step(1, RELAY)
    each_single(lambda copy: copy.start())

    @pl.when(late)
    def _():
        pl.semaphore_wait(hops.at[2], beside)
        relay_copy(0).start()

    @pl.loop(2, end)
    def _(t):
        @pl.when(t < end - 1)
        def _():
            far_step(t + 2, chunk_at(t + 2))

        i = chunk_at(t)
        across_step(t, i)
        for k in range(1, final):
            for sem, where in pieces(k):
                @pl.when(i == where.start + where.size - 1)
                def _():
                    across_copy(sem, where).start()

        @pl.when((t == RELAY_AT) & early)
        def _():
            relay_copy(0).wait_recv()
            relay_copy(1).start()

    last_step()

    @pl.when(jnp.logical_not(late))
    def _():
        pl.semaphore_wait(hops.at[2], beside)

    tell_columns(hops.at[3])

    @pl.loop(0, count)
    def _(i):
        mate_step(i)
        own_step(i)

    @pl.when(early)
    def _():
        relay_copy(1).wait_recv()
        relay_copy(2).start()

    pl.semaphore_wait(hops.at[3], beside)
    arrive(0, True, False)

    @pl.loop(1, end)
    def _(i):
        arrive(i, False, False)

    arrive(end, False, True)

    last = carry[...]
    z_ref[:, stride:] = last[:, :rest]
    last = jnp.where(lane < rest, last, -jnp.inf)
    top = jnp.maximum(m_ref[...], last)
    mass = s_ref[...] * jnp.exp(m_ref[...] - top) + jnp.exp(last - top)
    top = jnp.transpose(jnp.concatenate([top, top], axis=0))
    mass = jnp.transpose(jnp.concatenate([mass, mass], axis=0))
    peak = jnp.max(top, axis=0, keepdims=True)
    mass = jnp.sum(mass * jnp.exp(top - peak), axis=0, keepdims=True)
    me = col * 4 + row
    fst[me] = jnp.where(lane[:1] < rows, peak, mass)

    def stat_copy(c, r, slot):
        return pltpu.make_async_remote_copy(
            src_ref=fst.at[slot], dst_ref=fst.at[slot], send_sem=fsend.at[c * 4 + r], recv_sem=frecv.at[slot],
            device_id={"col": c, "row": r}, device_id_type=MESH,
        )

    def each_peer(act):
        for c in range(4):
            for r in range(4):
                @pl.when(me != c * 4 + r)
                def _():
                    act(c, r)

    each_peer(lambda c, r: stat_copy(c, r, me).start())
    for k in range(1, 16):
        peer = lax.rem(me + k, 16)
        stat_copy(col, row, peer).wait_recv()
    stats = fst[...]
    swapped = pltpu.roll(stats, LANES // 2, 2)
    peak = jnp.max(stats, axis=0)
    mass = jnp.sum(swapped * jnp.exp(stats - peak), axis=0)
    lse_ref[...] = peak + jnp.log(mass)

    for k in range(1, 4):
        norm_copy(k).wait_send()
    for src, dst, send, recv in ((qbuf, rin, qsend, rrecv), (pbuf, lin, psend, lrecv)):
        pltpu.make_async_remote_copy(
            src_ref=src, dst_ref=dst, send_sem=send, recv_sem=recv.at[0],
            device_id={"row": mate}, device_id_type=MESH,
        ).wait_send()
    for k in range(3):
        first_copy(k).wait_send()
    for k in range(1, final):
        each_group(k, lambda copy: copy.wait_send())
    each_single(lambda copy: copy.wait_send())

    @pl.when(core == 0)
    def _():
        rx_copy.wait_send()

    @pl.when(core == 1)
    def _():
        qx_copy.wait_send()
        across_copy(final, end).wait_send()

    @pl.when(late)
    def _():
        relay_copy(0).wait_send()

    @pl.when(early)
    def _():
        relay_copy(1).wait_send()
        relay_copy(2).wait_send()

    @pl.when(core == 1)
    def _():
        edge_copy.wait_send()

    each_peer(lambda c, r: stat_copy(c, r, me).wait_send())


def solution(mesh):
    def local_head(hidden, norm_gain, w_head):
        rows, feats = hidden.shape
        width = w_head.shape[1] // 4
        count = (width // LANES + 1) // TILES
        block = (count, rows, CHUNK)
        dma = pltpu.SemaphoreType.DMA

        def body(*refs):
            head_kernel(count, width, feats * 4, *refs)

        z, lse = pl.pallas_call(
            body,
            out_shape=(
                jax.ShapeDtypeStruct((rows, width), jnp.float32),
                jax.ShapeDtypeStruct((1, LANES), jnp.float32),
            ),
            in_specs=[
                pl.BlockSpec(memory_space=pltpu.HBM),
                pl.BlockSpec(memory_space=pltpu.HBM),
                pl.BlockSpec(memory_space=pltpu.HBM),
            ],
            out_specs=(pl.BlockSpec(memory_space=pltpu.VMEM), pl.BlockSpec(memory_space=pltpu.VMEM)),
            scratch_shapes=[
                pltpu.VMEM((rows, feats), hidden.dtype),
                pltpu.VMEM((feats,), jnp.float32),
                *[pltpu.VMEM((SLOTS, feats, CHUNK), jnp.bfloat16) for _ in range(4)],
                pltpu.VMEM((rows, feats), jnp.bfloat16),
                *[pltpu.VMEM(block, jnp.float32) for _ in range(7)],
                pltpu.VMEM((4, 1, LANES), jnp.float32),
                pltpu.VMEM((16, 1, LANES), jnp.float32),
                *[pltpu.VMEM((rows, LANES), jnp.float32) for _ in range(5)],
                *[pltpu.VMEM((rows, (TILES - 1) * LANES), jnp.float32) for _ in range(4)],
                pltpu.VMEM((rows, LANES), jnp.float32),
                dma, dma, pltpu.SemaphoreType.REGULAR((4,)),
                *[dma((SLOTS,)) for _ in range(4)], dma((4,)), dma((4,)),
                dma, dma, dma((len(GROUPS) + 2,)), dma((count,)), dma((count,)), dma((len(GROUPS) + 2,)), dma((16,)), dma((16,)), dma, dma, dma((3,)), dma((3,)), dma, dma, dma,
                dma((3,)), dma((3,)),
            ],
            compiler_params=pltpu.CompilerParams(
                collective_id=0, has_side_effects=True, vmem_limit_bytes=48 * 1024 * 1024
            ),
            name="head",
        )(pltpu.with_memory_space_constraint(hidden, pltpu.HBM), pltpu.with_memory_space_constraint(norm_gain, pltpu.HBM), w_head)
        log_norm = lse[0, :rows]
        return z - log_norm[:, None], log_norm

    return jax.shard_map(
        local_head,
        mesh=mesh,
        in_specs=(P("dp", "row"), P("row"), P("row", "col")),
        out_specs=(P("dp", ("col", "row")), P("dp")),
        check_vma=False,
    )
```
